256 devices in a mesh: gx: 8 (over y_hi, x), gy: 8 (over z), gz: 4 (over y_lo, core).
Axes of the slice: x: 4, y: 4 (y_hi: 2, y_lo: 2; y = y_hi * 2 + y_lo), z: 8, core: 2. Of those that a mesh axis runs over, the one named last changes fastest.
Arguments:
- tokens: bfloat16 [4096, 49, 512], P(('gx', 'gy', 'gz')), may hold values from -6 to 6
- cotangent: bfloat16 [4096, 49, 512], P(('gx', 'gy', 'gz')), may hold values from -6 to 6
- regions: int32 [4096, 49], P(('gx', 'gy', 'gz')), may hold values from 0 to 3
- rel_index: int32 [49, 49], replicated, may hold values from 0 to 168
- w_qkv: bfloat16 [512, 1536], replicated, may hold values from -0.25 to 0.25
- w_proj: bfloat16 [512, 512], replicated, may hold values from -0.25 to 0.25
- bias_table: float32 [169, 16], replicated, may hold values from -4 to 4
- mom_qkv: float32 [786432], P(('gx', 'gy', 'gz')), may hold values from -0.06 to 0.06
- mom_proj: float32 [262144], P(('gx', 'gy', 'gz')), may hold values from -0.06 to 0.06
- mom_table: float32 [169, 16], replicated, may hold values from -0.06 to 0.06
Outputs:
- new_mom_qkv: float32 [786432], P(('gx', 'gy', 'gz'))
- new_mom_proj: float32 [262144], P(('gx', 'gy', 'gz'))
- new_mom_table: float32 [169, 16], replicated
The draws below stay inside these ranges and needn't reach their ends.
All inputs are finite; a program needn't handle non-finite values.
Results may differ from the reference program's by a relative error of at most 0.015.
Values sent between devices are 32-bit elements; how exact they have to be, the bound alone decides.
A program may use at most 128 MiB of HBM per device.

```python
import jax
import jax.numpy as jnp
from jax import lax

D = 512
HEADS = 16
WIN_TOK = 49
TABLE = 169
WIN_DEV = 16
WINDOWS = 4096
N_GX = 8
N_GY = 8
N_GZ = 4


def touch_ends(drawn, own_key, smallest, largest):
    dims = drawn.shape
    index_at = [jax.random.randint(jax.random.fold_in(own_key, axis), (), 0, dims[axis]) for axis in range(len(dims))]
    drawn = drawn.at[tuple(index_at)].set(smallest)
    longest = dims.index(max(dims))
    index_at[longest] = (index_at[longest] + 1) % dims[longest]
    return drawn.at[tuple(index_at)].set(largest)


def block_levels(key, shape, cuts, low, largest):
    def one(dim, shards_of):
        steps = jax.random.uniform(jax.random.fold_in(jax.random.fold_in(key, 6), dim), (shards_of,), jnp.float32, low / len(cuts), largest / len(cuts))
        return jnp.repeat(jnp.exp(steps), shape[dim] // shards_of).reshape((-1,) + (1,) * (len(shape) - dim - 1))

    loudness = one(*cuts[0])
    for cut in cuts[1:]:
        loudness = loudness * one(*cut)
    return loudness


def noise(stream_key, extent, deviation, reach, cuts=(), held_as=jnp.bfloat16):
    drawn = deviation * jax.random.normal(stream_key, extent, jnp.float32)
    if cuts:
        drawn = drawn * block_levels(stream_key, extent, cuts, -0.22, 0.18)
    return jnp.clip(drawn, -reach, reach).astype(held_as)


def setup_inputs(seed: int = 0) -> dict:
    key_list = jax.random.split(jax.random.key(seed), 11)
    return {
        "tokens": noise(key_list[0], (WINDOWS, WIN_TOK, D), 1.0, 6.0, ((0, 256),)),
        "cotangent": noise(key_list[1], (WINDOWS, WIN_TOK, D), 1.0, 6.0, ((0, 256),)),
        "regions": touch_ends(jax.random.randint(key_list[2], (WINDOWS, WIN_TOK), 0, 4), jax.random.fold_in(key_list[2], 1), 0, 3).astype(jnp.int32),
        "rel_index": touch_ends(jax.random.randint(key_list[3], (WIN_TOK, WIN_TOK), 0, 169), jax.random.fold_in(key_list[3], 1), 0, 168).astype(jnp.int32),
        "w_qkv": noise(key_list[4], (D, 3 * D), D ** -0.5, 0.25),
        "w_proj": noise(key_list[5], (D, D), D ** -0.5, 0.25),
        "bias_table": noise(key_list[6], (TABLE, HEADS), 1.0, 4.0, (), jnp.float32),
        "mom_qkv": noise(key_list[7], (3 * D * D,), 0.01, 0.06, ((0, 256),), jnp.float32),
        "mom_proj": noise(key_list[8], (D * D,), 0.01, 0.06, ((0, 256),), jnp.float32),
        "mom_table": noise(key_list[9], (TABLE, HEADS), 0.01, 0.06, (), jnp.float32),
    }


def attend_core(qkv, table, regions, rel_index, heads):
    win, count, width = qkv.shape
    dim = width // 3
    parts = qkv.reshape(win, count, 3, heads, dim // heads).astype(jnp.float32)
    bias = jnp.transpose(table[rel_index], (2, 0, 1))
    scores = jnp.einsum('wihc,wjhc->whij', parts[:, :, 0], parts[:, :, 1]) * (dim // heads) ** (-0.5)
    masked = jnp.where(regions[:, :, None] == regions[:, None, :], 0.0, -100.0).astype(jnp.float32)
    scores = scores + bias[None] + masked[:, None]
    probs = jax.nn.softmax(scores, axis=-1).astype(jnp.bfloat16)
    attended = jnp.einsum('whij,wjhc->wihc', probs.astype(jnp.float32), parts[:, :, 2])
    return attended.astype(jnp.bfloat16).reshape(win, count, dim)

def local_grads(tokens, cotangent, regions, rel_index, w_qkv, w_proj, bias_table, heads):
    win, count, dim = tokens.shape
    flat = tokens.reshape(win * count, dim)
    qkv = jnp.dot(flat, w_qkv, preferred_element_type=jnp.float32).astype(jnp.bfloat16).reshape(win, count, 3 * dim)

    def forward(values, table):
        return attend_core(values, table, regions, rel_index, heads)
    attended, pullback = jax.vjp(forward, qkv, bias_table)
    flat_dy = cotangent.reshape(win * count, dim)
    grad_proj = jnp.dot(attended.reshape(win * count, dim).astype(jnp.float32).T, flat_dy.astype(jnp.float32))
    d_attended = jnp.dot(flat_dy, w_proj.T, preferred_element_type=jnp.float32).astype(jnp.bfloat16)
    d_qkv, grad_table = pullback(d_attended.reshape(win, count, dim))
    grad_qkv = jnp.dot(flat.astype(jnp.float32).T, d_qkv.reshape(win * count, 3 * dim).astype(jnp.float32))
    return (grad_qkv, grad_proj, grad_table)

def reference(tokens, cotangent, regions, rel_index, w_qkv, w_proj, bias_table, mom_qkv, mom_proj, mom_table):
    groups = N_GX * N_GY * N_GZ
    heads = bias_table.shape[1]
    tok_groups = tokens.reshape(groups, WIN_DEV, WIN_TOK, D)
    cot_groups = cotangent.reshape(groups, WIN_DEV, WIN_TOK, D)
    reg_groups = regions.reshape(groups, WIN_DEV, WIN_TOK)

    def step(carry, items):
        g_qkv, g_proj, g_table = local_grads(items[0], items[1], items[2], rel_index, w_qkv, w_proj, bias_table, heads)
        return ((carry[0] + g_qkv, carry[1] + g_proj, carry[2] + g_table), None)
    start = (jnp.zeros(w_qkv.shape, jnp.float32), jnp.zeros(w_proj.shape, jnp.float32), jnp.zeros(bias_table.shape, jnp.float32))
    sums, unused = lax.scan(step, start, (tok_groups, cot_groups, reg_groups))
    scale = 1.0 / (WIN_DEV * groups)
    return (0.9 * mom_qkv + sums[0].reshape(-1) * scale, 0.9 * mom_proj + sums[1].reshape(-1) * scale, 0.9 * mom_table + sums[2] * scale)
```

```python
import functools

import jax
import jax.numpy as jnp
from jax import lax
from jax.experimental import pallas as pl
from jax.experimental.pallas import tpu as pltpu
from jax.sharding import PartitionSpec as P

MESH = pl.DeviceIdType.MESH
BF = jnp.bfloat16
F32 = jnp.float32
WIN = 16
TOK = 49
SEG = 64
TP = 56
D = 512
HEAD_DIM = 32
SCALE = HEAD_DIM ** -0.5
UNITS = 2


def nt(a, b):
    return lax.dot_general(a, b, (((1,), (1,)), ((), ())), preferred_element_type=F32)


def nn(a, b):
    return jnp.dot(a, b, preferred_element_type=F32)


def iota(shape, dim):
    return lax.broadcasted_iota(jnp.int32, shape, dim)


def compute_kernel(
    tok, cot, reg, rel, wqkv, wproj, tab_t, g_out, tab_out,
    xp, cp, qkv, kvt, da, xpt, bias, mask, dk, dv, dqt, at, gb, pad, tabp, relt,
):
    low = iota((TP, 128), 1) < SEG
    pad[...] = jnp.zeros_like(pad)
    pad[0:TOK, 0:TOK] = rel[...].astype(F32)
    flipped = pad[...].T
    both = flipped[0:TP] + pltpu.roll(flipped, SEG, 1)[0:TP]
    index = both.astype(jnp.int32)
    relt[...] = both
    pad[...] = jnp.zeros_like(pad)
    pad[0:WIN, 0:TOK] = reg[...].astype(F32)
    regions = pad[0:WIN, :]
    moved = pltpu.roll(regions, SEG, 1)
    columns = pad[...].T[0:TP]
    for pair in range(WIN // 2):
        w = 2 * pair
        key = jnp.where(
            low,
            jnp.broadcast_to(columns[:, w : w + 1], (TP, 128)),
            jnp.broadcast_to(columns[:, w + 1 : w + 2], (TP, 128)),
        )
        query = jnp.where(low[0:1], regions[w : w + 1], moved[w + 1 : w + 2])
        mask[pair] = jnp.where(key == query, 0.0, -100.0).astype(F32)
    tabp[...] = jnp.zeros_like(tabp)
    tabp[:, 0:169] = tab_t[...]
    first = jnp.bitwise_and(index, 127)
    beyond = index >= 128
    real = iota((TP, 128), 0) < TOK
    for h in range(16):
        lo = jnp.broadcast_to(tabp[h : h + 1, 0:128], (TP, 128))
        hi = jnp.broadcast_to(tabp[h : h + 1, 128:256], (TP, 128))
        lo = jnp.take_along_axis(lo, first, axis=1, mode="promise_in_bounds")
        hi = jnp.take_along_axis(hi, first, axis=1, mode="promise_in_bounds")
        bias[h // 4, :, (h % 4) * 128 : (h % 4 + 1) * 128] = jnp.where(
            real, jnp.where(beyond, hi, lo), -1e30
        )
    gb[...] = jnp.zeros_like(gb)

    row = iota((256, 784), 0)
    wanted = (row % SEG) * WIN + row // SEG
    column = iota((256, 784), 1)
    eye = (iota((128, 128), 0) == iota((128, 128), 1)).astype(BF)
    rho = iota((D, D), 0)
    natural = (
        ((rho >> 7) & 1) * 256
        + ((rho >> 4) & 3) * 64
        + ((rho >> 1) & 7) * 8
        + ((rho >> 6) & 1) * 4
        + ((rho >> 8) & 1) * 2
        + (rho & 1)
    )
    order = (natural == iota((D, D), 1)).astype(F32).astype(BF)

    def project(c, carry):
        rows = pl.ds(pl.multiple_of(c * 256, 256), 256)
        pick = (wanted + 4 * c == column).astype(F32).astype(BF)
        x = nn(pick, tok[...]).astype(BF)
        xp[rows, :] = x
        y = nn(pick, cot[...]).astype(BF)
        cp[rows, :] = y
        da[rows, :] = nt(y, wproj[...]).astype(BF)
        xpt[:, rows] = nt(order, x).astype(BF)
        values = nn(x, wqkv[...]).astype(BF)
        qkv[rows, :] = values
        for b in range(8):
            kvt[b * 128 : (b + 1) * 128, rows] = nt(
                eye, values[:, 512 + b * 128 : 512 + (b + 1) * 128]
            ).astype(BF)
        return carry

    lax.fori_loop(0, 4, project, 0)

    lane = iota((SEG, 128), 1)
    heads = [(lane // HEAD_DIM == h).astype(F32).astype(BF) for h in range(4)]
    zero = jnp.zeros((SEG, 128), BF)
    half = iota((SEG, 512), 1) % 128
    left = (half < SEG).astype(F32).astype(BF)
    right = (half >= SEG).astype(F32).astype(BF)
    tail = jnp.zeros((SEG - TP, 512), F32)

    def spread(a):
        blocks = []
        for h in range(4):
            blocks.append(jnp.concatenate([a[0:SEG] * heads[h], zero], axis=1))
            blocks.append(jnp.concatenate([zero, a[SEG:] * heads[h]], axis=1))
        return jnp.concatenate(blocks, axis=0)

    def side(a):
        return jnp.concatenate([a[0:SEG], a[SEG:]], axis=1)

    def attend(g, pair):
        rows = pl.ds(pl.multiple_of(pair * 128, 128), 128)
        rows0 = pl.ds(pl.multiple_of(pair * 128, 128), SEG)
        rows1 = pl.ds(pl.multiple_of(pair * 128 + SEG, SEG), SEG)

        def cols(start):
            return pl.ds(pl.multiple_of(start + g * 128, 128), 128)

        q_wide = spread(qkv[rows, cols(0)])
        scores = nt(side(qkv[rows, cols(512)]), q_wide)[0:TP] * SCALE + bias[g]
        scores = scores + jnp.concatenate([mask[pair]] * 4, axis=1)
        e = jnp.exp(scores - jnp.max(scores, axis=0, keepdims=True))
        p = e * (1.0 / jnp.sum(e, axis=0, keepdims=True))
        probs = jnp.concatenate([p, tail], axis=0).astype(BF)
        da_wide = spread(da[rows, cols(0)])
        dp = nt(side(qkv[rows, cols(1024)]), da_wide)[0:TP]
        ds = p * (dp - jnp.sum(p * dp, axis=0, keepdims=True))
        gb[g] += ds
        dsb = jnp.concatenate([ds * SCALE, tail], axis=0).astype(BF)
        dv_pair = nn(probs, da_wide).astype(BF)
        dv[rows0, cols(0)] = dv_pair[:, 0:128]
        dv[rows1, cols(0)] = dv_pair[:, 128:256]
        dk_pair = nn(dsb, q_wide).astype(BF)
        dk[rows0, cols(0)] = dk_pair[:, 0:128]
        dk[rows1, cols(0)] = dk_pair[:, 128:256]
        p_bd = jnp.concatenate([probs * left, probs * right], axis=0)
        s_bd = jnp.concatenate([dsb * left, dsb * right], axis=0)
        a_full = nn(kvt[cols(512), rows], p_bd)
        q_full = nn(kvt[cols(0), rows], s_bd)
        for h in range(4):
            strip = pl.ds(pl.multiple_of(g * 128 + 32 * h, 32), 32)
            block = (slice(32 * h, 32 * h + 32), slice(128 * h, 128 * h + 128))
            at[strip, rows] = a_full[block].astype(BF)
            dqt[strip, rows] = q_full[block].astype(BF)

    steps = WIN // 2 // UNITS

    def attention(t, carry):
        for u in range(UNITS):
            attend(t // steps, (t % steps) * UNITS + u)
        return carry

    lax.fori_loop(0, 4 * steps, attention, 0)

    def put(lo, value):
        g_out[:, :, :, :, lo : lo + 512] = value.reshape(2, 4, 4, 16, 512)

    put(0, nt(xpt[...], dqt[...]))
    put(512, nn(xpt[...], dk[...]))
    put(1024, nn(xpt[...], dv[...]))
    put(1536, nn(nn(order, at[...]).astype(BF), cp[...]))

    total = jnp.zeros((32, 256), F32)
    entry = iota((256, 128), 0).astype(F32)
    for j in range(TOK):
        hot = (entry == jnp.broadcast_to(relt[j : j + 1, :], (256, 128))).astype(F32).astype(BF)
        line = jnp.concatenate([gb[g, j : j + 1, h * 128 : (h + 1) * 128] for g in range(4) for h in range(4)], axis=0)
        upper = line.astype(BF)
        lower = (line - upper.astype(F32)).astype(BF)
        total = total + nt(jnp.concatenate([upper, lower], axis=0), hot)
    tab_out[...] = total[0:16] + total[16:32]


def compute(tok, cot, reg, rel, wqkv, wproj, tab_t):
    vm = pl.BlockSpec(memory_space=pltpu.VMEM)
    return pl.pallas_call(
        compute_kernel,
        name="grads",
        out_shape=(
            jax.ShapeDtypeStruct((2, 4, 4, 16, 2048), F32),
            jax.ShapeDtypeStruct((16, 256), F32),
        ),
        in_specs=[vm] * 7,
        out_specs=(vm, vm),
        scratch_shapes=[
            pltpu.VMEM((1024, D), BF),
            pltpu.VMEM((1024, D), BF),
            pltpu.VMEM((1024, 3 * D), BF),
            pltpu.VMEM((1024, 1024), BF),
            pltpu.VMEM((1024, D), BF),
            pltpu.VMEM((D, 1024), BF),
            pltpu.VMEM((4, TP, 512), F32),
            pltpu.VMEM((WIN // 2, TP, 128), F32),
            pltpu.VMEM((1024, D), BF),
            pltpu.VMEM((1024, D), BF),
            pltpu.VMEM((D, 1024), BF),
            pltpu.VMEM((D, 1024), BF),
            pltpu.VMEM((4, TP, 512), F32),
            pltpu.VMEM((128, 128), F32),
            pltpu.VMEM((16, 256), F32),
            pltpu.VMEM((TP, 128), F32),
        ],
        compiler_params=pltpu.CompilerParams(vmem_limit_bytes=60 * 2**20),
    )(tok, cot, reg, rel, wqkv, wproj, tab_t)


def sum_kernel(
    scale, g, tab, mom_qkv, mom_proj, mom_tab, out_qkv, out_proj, out_tab,
    s1, ra, rb, a2, b2, ra2, rb2, zs, rz, tsend, trecv, send, recv,
):
    gx, gy, gz = lax.axis_index("gx"), lax.axis_index("gy"), lax.axis_index("gz")
    x, z, core = lax.rem(gx, 4), gy, lax.rem(gz, 2)
    y = (gx // 4) * 2 + gz // 2

    def device(x, y, z, core):
        return ((y // 2) * 4 + x, z, lax.rem(y, 2) * 2 + core)

    def xor(a, b):
        out = 0
        for bit in (1, 2, 4):
            have = lax.rem(a // bit, 2)
            out = out + bit * ((1 - have) if b & bit else have)
        return out

    partner = device(x, y, z, 1 - core)
    along_x = [(xor(x, d), device(xor(x, d), y, z, core)) for d in (1, 2, 3)]
    along_y = [(xor(y, d), device(x, xor(y, d), z, core)) for d in (1, 2, 3)]
    along_z = [(xor(z, d), device(x, y, xor(z, d), core)) for d in range(1, 8)]
    peers = [partner] + [dev for _, dev in along_x + along_y + along_z]
    barrier = pltpu.get_barrier_semaphore()
    for peer in peers:
        pl.semaphore_signal(barrier, inc=1, device_id=peer, device_id_type=MESH)
    pl.semaphore_wait(barrier, len(peers))

    used = [0]

    def copy(src, dst, dev):
        n = used[0]
        used[0] += 1
        c = pltpu.make_async_remote_copy(
            src_ref=src, dst_ref=dst, send_sem=send.at[n], recv_sem=recv.at[n],
            device_id=dev, device_id_type=MESH,
        )
        c.start()
        return c

    def wait(copies):
        for c in copies:
            c.wait()

    wait([copy(g.at[1 - core], s1, partner), copy(tab, trecv.at[0], partner)])
    for b in range(4):
        s1[b] += g[core, b]
    tsend[0] = tab[...] + trecv[0]

    copies = []
    for n, (to, dev) in enumerate(along_x):
        copies.append(copy(s1.at[:, to, :, pl.ds(0, 1024)], ra.at[n], dev))
        copies.append(copy(tsend.at[0], trecv.at[1 + n], dev))
    for n, (to, dev) in enumerate(along_y):
        copies.append(copy(s1.at[to, :, :, pl.ds(1024, 1024)], rb.at[n], dev))
    wait(copies)
    for b in range(4):
        a2[b] = s1[b, x, :, 0:1024] + ra[0, b] + ra[1, b] + ra[2, b]
        b2[b] = s1[y, b, :, 1024:2048] + rb[0, b] + rb[1, b] + rb[2, b]
    tsend[1] = tsend[0] + trecv[1] + trecv[2] + trecv[3]

    copies = []
    for n, (to, dev) in enumerate(along_y):
        copies.append(copy(a2.at[to], ra2.at[n], dev))
        copies.append(copy(tsend.at[1], trecv.at[4 + n], dev))
    for n, (to, dev) in enumerate(along_x):
        copies.append(copy(b2.at[to], rb2.at[n], dev))
    wait(copies)
    a3 = a2[y] + ra2[0] + ra2[1] + ra2[2]
    b3 = b2[x] + rb2[0] + rb2[1] + rb2[2]
    for k in range(8):
        zs[k, :, 0:1024] = a3[2 * k : 2 * k + 2]
        zs[k, :, 1024:2048] = b3[2 * k : 2 * k + 2]
    tsend[2] = tsend[1] + trecv[4] + trecv[5] + trecv[6]

    copies = []
    for n, (to, dev) in enumerate(along_z):
        copies.append(copy(zs.at[to], rz.at[n], dev))
        copies.append(copy(tsend.at[2], trecv.at[7 + n], dev))
    wait(copies)
    mine = zs[z]
    table = tsend[2]
    for n in range(7):
        mine = mine + rz[n]
        table = table + trecv[7 + n]
    for r in range(2):
        for c in range(12):
            k = r * 12 + c
            out_qkv[k : k + 1, :] = 0.9 * mom_qkv[k : k + 1, :] + mine[r : r + 1, c * 128 : (c + 1) * 128] * scale
        for c in range(4):
            k = r * 4 + c
            out_proj[k : k + 1, :] = 0.9 * mom_proj[k : k + 1, :] + mine[r : r + 1, 1536 + c * 128 : 1536 + (c + 1) * 128] * scale
    out_tab[...] = 0.9 * mom_tab[...] + table[:, 0:169] * scale


def add_up(scale, g, tab, mom_qkv, mom_proj, mom_tab):
    vm = pl.BlockSpec(memory_space=pltpu.VMEM)
    return pl.pallas_call(
        functools.partial(sum_kernel, scale),
        name="add_up",
        out_shape=(
            jax.ShapeDtypeStruct((24, 128), F32),
            jax.ShapeDtypeStruct((8, 128), F32),
            jax.ShapeDtypeStruct((16, 169), F32),
        ),
        in_specs=[vm] * 5,
        out_specs=(vm, vm, vm),
        scratch_shapes=[
            pltpu.VMEM((4, 4, 16, 2048), F32),
            pltpu.VMEM((3, 4, 16, 1024), F32),
            pltpu.VMEM((3, 4, 16, 1024), F32),
            pltpu.VMEM((4, 16, 1024), F32),
            pltpu.VMEM((4, 16, 1024), F32),
            pltpu.VMEM((3, 16, 1024), F32),
            pltpu.VMEM((3, 16, 1024), F32),
            pltpu.VMEM((8, 2, 2048), F32),
            pltpu.VMEM((7, 2, 2048), F32),
            pltpu.VMEM((3, 16, 256), F32),
            pltpu.VMEM((14, 16, 256), F32),
            pltpu.SemaphoreType.DMA((40,)),
            pltpu.SemaphoreType.DMA((40,)),
        ],
        compiler_params=pltpu.CompilerParams(
            collective_id=0, has_side_effects=True, vmem_limit_bytes=40 * 2**20
        ),
    )(g, tab, mom_qkv, mom_proj, mom_tab)


def body(tokens, cotangent, regions, rel_index, w_qkv, w_proj, bias_table, mom_qkv, mom_proj, mom_table):
    win, count, dim = tokens.shape
    devices = lax.axis_size(("gx", "gy", "gz"))
    tok = jnp.transpose(tokens, (1, 0, 2)).reshape(count * win, dim)
    cot = jnp.transpose(cotangent, (1, 0, 2)).reshape(count * win, dim)
    g, tab = compute(tok, cot, regions, rel_index, w_qkv, w_proj, bias_table.T)
    out_qkv, out_proj, out_tab = add_up(
        1.0 / (win * devices), g, tab,
        mom_qkv.reshape(24, 128), mom_proj.reshape(8, 128), mom_table.T,
    )
    return out_qkv.reshape(-1), out_proj.reshape(-1), out_tab.T


def solution(mesh):
    return jax.shard_map(
        body,
        mesh=mesh,
        in_specs=(
            P(("gx", "gy", "gz"), None, None),
            P(("gx", "gy", "gz"), None, None),
            P(("gx", "gy", "gz"), None),
            P(),
            P(),
            P(),
            P(),
            P(("gx", "gy", "gz")),
            P(("gx", "gy", "gz")),
            P(),
        ),
        out_specs=(P(("gx", "gy", "gz")), P(("gx", "gy", "gz")), P()),
        check_vma=False,
    )
```

```python
import functools

import jax
import jax.numpy as jnp
from jax import lax
from jax.experimental import pallas as pl
from jax.experimental.pallas import tpu as pltpu
from jax.sharding import PartitionSpec as P

MESH = pl.DeviceIdType.MESH
BF = jnp.bfloat16
F32 = jnp.float32
WIN = 16
TOK = 49
SEG = 64
TP = 56
D = 512
HEAD_DIM = 32
SCALE = HEAD_DIM ** -0.5
UNITS = 2


def nt(a, b):
    return lax.dot_general(a, b, (((1,), (1,)), ((), ())), preferred_element_type=F32)


def nn(a, b):
    return jnp.dot(a, b, preferred_element_type=F32)


def iota(shape, dim):
    return lax.broadcasted_iota(jnp.int32, shape, dim)


def compute_kernel(
    tok, cot, reg, rel, wqkv, wproj, tab_t, g_out, tab_out,
    xp, cp, qkv, kvt, da, xpt, bias, mask, dk, dv, dqt, at, gb, pad, tabp, relt,
):
    low = iota((TP, 128), 1) < SEG
    pad[...] = jnp.zeros_like(pad)
    pad[0:TOK, 0:TOK] = rel[...].astype(F32)
    flipped = pad[...].T
    both = flipped[0:TP] + pltpu.roll(flipped, SEG, 1)[0:TP]
    index = both.astype(jnp.int32)
    relt[...] = both
    pad[...] = jnp.zeros_like(pad)
    pad[0:WIN, 0:TOK] = reg[...].astype(F32)
    regions = pad[0:WIN, :]
    moved = pltpu.roll(regions, SEG, 1)
    columns = pad[...].T[0:TP]
    for pair in range(WIN // 2):
        w = 2 * pair
        key = jnp.where(
            low,
            jnp.broadcast_to(columns[:, w : w + 1], (TP, 128)),
            jnp.broadcast_to(columns[:, w + 1 : w + 2], (TP, 128)),
        )
        query = jnp.where(low[0:1], regions[w : w + 1], moved[w + 1 : w + 2])
        mask[pair] = jnp.where(key == query, 0.0, -100.0).astype(F32)
    tabp[...] = jnp.zeros_like(tabp)
    tabp[:, 0:169] = tab_t[...]
    first = jnp.bitwise_and(index, 127)
    beyond = index >= 128
    real = iota((TP, 128), 0) < TOK
    for h in range(16):
        lo = jnp.broadcast_to(tabp[h : h + 1, 0:128], (TP, 128))
        hi = jnp.broadcast_to(tabp[h : h + 1, 128:256], (TP, 128))
        lo = jnp.take_along_axis(lo, first, axis=1, mode="promise_in_bounds")
        hi = jnp.take_along_axis(hi, first, axis=1, mode="promise_in_bounds")
        bias[h // 4, :, (h % 4) * 128 : (h % 4 + 1) * 128] = jnp.where(
            real, jnp.where(beyond, hi, lo), -1e30
        )
    gb[...] = jnp.zeros_like(gb)

    row = iota((256, 784), 0)
    wanted = (row % SEG) * WIN + row // SEG
    column = iota((256, 784), 1)
    eye = (iota((128, 128), 0) == iota((128, 128), 1)).astype(BF)
    rho = iota((D, D), 0)
    natural = (
        ((rho >> 7) & 1) * 256
        + ((rho >> 4) & 3) * 64
        + ((rho >> 1) & 7) * 8
        + ((rho >> 6) & 1) * 4
        + ((rho >> 8) & 1) * 2
        + (rho & 1)
    )
    order = (natural == iota((D, D), 1)).astype(F32).astype(BF)

    def project(c, carry):
        rows = pl.ds(pl.multiple_of(c * 256, 256), 256)
        pick = (wanted + 4 * c == column).astype(F32).astype(BF)
        x = nn(pick, tok[...]).astype(BF)
        xp[rows, :] = x
        y = nn(pick, cot[...]).astype(BF)
        cp[rows, :] = y
        da[rows, :] = nt(y, wproj[...]).astype(BF)
        xpt[:, rows] = nt(order, x).astype(BF)
        values = nn(x, wqkv[...]).astype(BF)
        qkv[rows, :] = values
        for b in range(8):
            kvt[b * 128 : (b + 1) * 128, rows] = nt(
                eye, values[:, 512 + b * 128 : 512 + (b + 1) * 128]
            ).astype(BF)
        return carry

    lax.fori_loop(0, 4, project, 0)

    lane = iota((SEG, 128), 1)
    heads = [(lane // HEAD_DIM == h).astype(F32).astype(BF) for h in range(4)]
    zero = jnp.zeros((SEG, 128), BF)
    half = iota((SEG, 512), 1) % 128
    left = (half < SEG).astype(F32).astype(BF)
    right = (half >= SEG).astype(F32).astype(BF)
    tail = jnp.zeros((SEG - TP, 512), F32)

    def spread(a):
        blocks = []
        for h in range(4):
            blocks.append(jnp.concatenate([a[0:SEG] * heads[h], zero], axis=1))
            blocks.append(jnp.concatenate([zero, a[SEG:] * heads[h]], axis=1))
        return jnp.concatenate(blocks, axis=0)

    def side(a):
        return jnp.concatenate([a[0:SEG], a[SEG:]], axis=1)

    def attend(g, pair):
        rows = pl.ds(pl.multiple_of(pair * 128, 128), 128)
        rows0 = pl.ds(pl.multiple_of(pair * 128, 128), SEG)
        rows1 = pl.ds(pl.multiple_of(pair * 128 + SEG, SEG), SEG)

        def cols(start):
            return pl.ds(pl.multiple_of(start + g * 128, 128), 128)

        q_wide = spread(qkv[rows, cols(0)])
        scores = nt(side(qkv[rows, cols(512)]), q_wide)[0:TP] * SCALE + bias[g]
        scores = scores + jnp.concatenate([mask[pair]] * 4, axis=1)
        e = jnp.exp(scores - jnp.max(scores, axis=0, keepdims=True))
        p = e * (1.0 / jnp.sum(e, axis=0, keepdims=True))
        probs = jnp.concatenate([p, tail], axis=0).astype(BF)
        da_wide = spread(da[rows, cols(0)])
        dp = nt(side(qkv[rows, cols(1024)]), da_wide)[0:TP]
        ds = p * (dp - jnp.sum(p * dp, axis=0, keepdims=True))
        gb[g] += ds
        dsb = jnp.concatenate([ds * SCALE, tail], axis=0).astype(BF)
        dv_pair = nn(probs, da_wide).astype(BF)
        dv[rows0, cols(0)] = dv_pair[:, 0:128]
        dv[rows1, cols(0)] = dv_pair[:, 128:256]
        dk_pair = nn(dsb, q_wide).astype(BF)
        dk[rows0, cols(0)] = dk_pair[:, 0:128]
        dk[rows1, cols(0)] = dk_pair[:, 128:256]
        p_bd = jnp.concatenate([probs * left, probs * right], axis=0)
        s_bd = jnp.concatenate([dsb * left, dsb * right], axis=0)
        a_full = nn(kvt[cols(512), rows], p_bd)
        q_full = nn(kvt[cols(0), rows], s_bd)
        for h in range(4):
            strip = pl.ds(pl.multiple_of(g * 128 + 32 * h, 32), 32)
            block = (slice(32 * h, 32 * h + 32), slice(128 * h, 128 * h + 128))
            at[strip, rows] = a_full[block].astype(BF)
            dqt[strip, rows] = q_full[block].astype(BF)

    steps = WIN // 2 // UNITS

    def attention(t, carry):
        for u in range(UNITS):
            attend(t // steps, (t % steps) * UNITS + u)
        return carry

    lax.fori_loop(0, 4 * steps, attention, 0)

    def put(lo, value):
        g_out[:, :, :, :, lo : lo + 512] = value.reshape(2, 4, 4, 16, 512)

    put(0, nt(xpt[...], dqt[...]))
    put(512, nn(xpt[...], dk[...]))
    put(1024, nn(xpt[...], dv[...]))
    put(1536, nn(nn(order, at[...]).astype(BF), cp[...]))

    total = jnp.zeros((32, 256), F32)
    entry = iota((256, 128), 0).astype(F32)
    for j in range(TOK):
        hot = (entry == jnp.broadcast_to(relt[j : j + 1, :], (256, 128))).astype(F32).astype(BF)
        line = jnp.concatenate([gb[g, j : j + 1, h * 128 : (h + 1) * 128] for g in range(4) for h in range(4)], axis=0)
        upper = line.astype(BF)
        lower = (line - upper.astype(F32)).astype(BF)
        total = total + nt(jnp.concatenate([upper, lower], axis=0), hot)
    tab_out[...] = total[0:16] + total[16:32]


def sum_kernel(
    scale, g, tab, mom_qkv, mom_proj, mom_tab, out_qkv, out_proj, out_tab,
    s1, ra, rb, a2, b2, ra2, rb2, zs, rz, tsend, trecv, send, recv,
):
    gx, gy, gz = lax.axis_index("gx"), lax.axis_index("gy"), lax.axis_index("gz")
    x, z, core = lax.rem(gx, 4), gy, lax.rem(gz, 2)
    y = (gx // 4) * 2 + gz // 2

    def device(x, y, z, core):
        return ((y // 2) * 4 + x, z, lax.rem(y, 2) * 2 + core)

    def xor(a, b):
        out = 0
        for bit in (1, 2, 4):
            have = lax.rem(a // bit, 2)
            out = out + bit * ((1 - have) if b & bit else have)
        return out

    partner = device(x, y, z, 1 - core)
    along_x = [(xor(x, d), device(xor(x, d), y, z, core)) for d in (1, 2, 3)]
    along_y = [(xor(y, d), device(x, xor(y, d), z, core)) for d in (1, 2, 3)]
    along_z = [(xor(z, d), device(x, y, xor(z, d), core)) for d in range(1, 8)]
    peers = [partner] + [dev for _, dev in along_x + along_y + along_z]
    barrier = pltpu.get_barrier_semaphore()
    for peer in peers:
        pl.semaphore_signal(barrier, inc=1, device_id=peer, device_id_type=MESH)
    pl.semaphore_wait(barrier, len(peers))

    used = [0]

    def copy(src, dst, dev):
        n = used[0]
        used[0] += 1
        c = pltpu.make_async_remote_copy(
            src_ref=src, dst_ref=dst, send_sem=send.at[n], recv_sem=recv.at[n],
            device_id=dev, device_id_type=MESH,
        )
        c.start()
        return c

    def wait(copies):
        for c in copies:
            c.wait()

    wait([copy(g.at[1 - core], s1, partner), copy(tab, trecv.at[0], partner)])
    for b in range(4):
        s1[b] += g[core, b]
    tsend[0] = tab[...] + trecv[0]

    copies = []
    for n, (to, dev) in enumerate(along_x):
        copies.append(copy(s1.at[:, to, :, pl.ds(0, 1024)], ra.at[n], dev))
        copies.append(copy(tsend.at[0], trecv.at[1 + n], dev))
    for n, (to, dev) in enumerate(along_y):
        copies.append(copy(s1.at[to, :, :, pl.ds(1024, 1024)], rb.at[n], dev))
    wait(copies)
    for b in range(4):
        a2[b] = s1[b, x, :, 0:1024] + ra[0, b] + ra[1, b] + ra[2, b]
        b2[b] = s1[y, b, :, 1024:2048] + rb[0, b] + rb[1, b] + rb[2, b]
    tsend[1] = tsend[0] + trecv[1] + trecv[2] + trecv[3]

    copies = []
    for n, (to, dev) in enumerate(along_y):
        copies.append(copy(a2.at[to], ra2.at[n], dev))
        copies.append(copy(tsend.at[1], trecv.at[4 + n], dev))
    for n, (to, dev) in enumerate(along_x):
        copies.append(copy(b2.at[to], rb2.at[n], dev))
    wait(copies)
    a3 = a2[y] + ra2[0] + ra2[1] + ra2[2]
    b3 = b2[x] + rb2[0] + rb2[1] + rb2[2]
    for k in range(8):
        zs[k, :, 0:1024] = a3[2 * k : 2 * k + 2]
        zs[k, :, 1024:2048] = b3[2 * k : 2 * k + 2]
    tsend[2] = tsend[1] + trecv[4] + trecv[5] + trecv[6]

    copies = []
    for n, (to, dev) in enumerate(along_z):
        copies.append(copy(zs.at[to], rz.at[n], dev))
        copies.append(copy(tsend.at[2], trecv.at[7 + n], dev))
    wait(copies)
    mine = zs[z]
    table = tsend[2]
    for n in range(7):
        mine = mine + rz[n]
        table = table + trecv[7 + n]
    for r in range(2):
        for c in range(12):
            k = r * 12 + c
            out_qkv[k : k + 1, :] = 0.9 * mom_qkv[k : k + 1, :] + mine[r : r + 1, c * 128 : (c + 1) * 128] * scale
        for c in range(4):
            k = r * 4 + c
            out_proj[k : k + 1, :] = 0.9 * mom_proj[k : k + 1, :] + mine[r : r + 1, 1536 + c * 128 : 1536 + (c + 1) * 128] * scale
    out_tab[...] = 0.9 * mom_tab[...] + table[:, 0:169] * scale


LOCAL = [
    pltpu.VMEM((1024, D), BF),
    pltpu.VMEM((1024, D), BF),
    pltpu.VMEM((1024, 3 * D), BF),
    pltpu.VMEM((1024, 1024), BF),
    pltpu.VMEM((1024, D), BF),
    pltpu.VMEM((D, 1024), BF),
    pltpu.VMEM((4, TP, 512), F32),
    pltpu.VMEM((WIN // 2, TP, 128), F32),
    pltpu.VMEM((1024, D), BF),
    pltpu.VMEM((1024, D), BF),
    pltpu.VMEM((D, 1024), BF),
    pltpu.VMEM((D, 1024), BF),
    pltpu.VMEM((4, TP, 512), F32),
    pltpu.VMEM((128, 128), F32),
    pltpu.VMEM((16, 256), F32),
    pltpu.VMEM((TP, 128), F32),
]
SHARED = [
    pltpu.VMEM((4, 4, 16, 2048), F32),
    pltpu.VMEM((3, 4, 16, 1024), F32),
    pltpu.VMEM((3, 4, 16, 1024), F32),
    pltpu.VMEM((4, 16, 1024), F32),
    pltpu.VMEM((4, 16, 1024), F32),
    pltpu.VMEM((3, 16, 1024), F32),
    pltpu.VMEM((3, 16, 1024), F32),
    pltpu.VMEM((8, 2, 2048), F32),
    pltpu.VMEM((7, 2, 2048), F32),
    pltpu.VMEM((3, 16, 256), F32),
    pltpu.VMEM((14, 16, 256), F32),
    pltpu.SemaphoreType.DMA((40,)),
    pltpu.SemaphoreType.DMA((40,)),
]


def kernel(scale, *refs):
    inputs, refs = refs[:7], refs[7:]
    moms, refs = refs[:3], refs[3:]
    outs, refs = refs[:3], refs[3:]
    g, tab, refs = refs[0], refs[1], refs[2:]
    local, shared = refs[: len(LOCAL)], refs[len(LOCAL) :]
    compute_kernel(*inputs, g, tab, *local)
    sum_kernel(scale, g, tab, *moms, *outs, *shared)


def step(scale, *operands):
    vm = pl.BlockSpec(memory_space=pltpu.VMEM)
    return pl.pallas_call(
        functools.partial(kernel, scale),
        name="step",
        out_shape=(
            jax.ShapeDtypeStruct((24, 128), F32),
            jax.ShapeDtypeStruct((8, 128), F32),
            jax.ShapeDtypeStruct((16, 169), F32),
        ),
        in_specs=[vm] * 10,
        out_specs=(vm, vm, vm),
        scratch_shapes=[
            pltpu.VMEM((2, 4, 4, 16, 2048), F32),
            pltpu.VMEM((16, 256), F32),
            *LOCAL,
            *SHARED,
        ],
        compiler_params=pltpu.CompilerParams(
            collective_id=0, has_side_effects=True, vmem_limit_bytes=60 * 2**20
        ),
    )(*operands)


def body(tokens, cotangent, regions, rel_index, w_qkv, w_proj, bias_table, mom_qkv, mom_proj, mom_table):
    win, count, dim = tokens.shape
    devices = lax.axis_size(("gx", "gy", "gz"))
    tok = jnp.transpose(tokens, (1, 0, 2)).reshape(count * win, dim)
    cot = jnp.transpose(cotangent, (1, 0, 2)).reshape(count * win, dim)
    out_qkv, out_proj, out_tab = step(
        1.0 / (win * devices), tok, cot, regions, rel_index, w_qkv, w_proj, bias_table.T,
        mom_qkv.reshape(24, 128), mom_proj.reshape(8, 128), mom_table.T,
    )
    return out_qkv.reshape(-1), out_proj.reshape(-1), out_tab.T


def solution(mesh):
    return jax.shard_map(
        body,
        mesh=mesh,
        in_specs=(
            P(("gx", "gy", "gz"), None, None),
            P(("gx", "gy", "gz"), None, None),
            P(("gx", "gy", "gz"), None),
            P(),
            P(),
            P(),
            P(),
            P(("gx", "gy", "gz")),
            P(("gx", "gy", "gz")),
            P(),
        ),
        out_specs=(P(("gx", "gy", "gz")), P(("gx", "gy", "gz")), P()),
        check_vma=False,
    )
```

```python
import functools

import jax
import jax.numpy as jnp
from jax import lax
from jax.experimental import pallas as pl
from jax.experimental.pallas import tpu as pltpu
from jax.sharding import PartitionSpec as P

MESH = pl.DeviceIdType.MESH
BF = jnp.bfloat16
F32 = jnp.float32
WIN = 16
TOK = 49
SEG = 64
TP = 56
D = 512
HEAD_DIM = 32
SCALE = HEAD_DIM ** -0.5
UNITS = 2
CH = 256
CHUNKS = 8


def nt(a, b):
    return lax.dot_general(a, b, (((1,), (1,)), ((), ())), preferred_element_type=F32)


def nn(a, b):
    return jnp.dot(a, b, preferred_element_type=F32)


def iota(shape, dim):
    return lax.broadcasted_iota(jnp.int32, shape, dim)


def onehot(condition):
    return condition.astype(F32).astype(BF)


def aligned(start, size, to=128):
    return pl.ds(pl.multiple_of(start, to), size)


def small_tables(reg, rel, tab_t, bias, mask, pad, tabp, relt):
    low = iota((TP, 128), 1) < SEG
    pad[...] = jnp.zeros_like(pad)
    pad[0:TOK, 0:TOK] = rel[...].astype(F32)
    flipped = pad[...].T
    both = flipped[0:TP] + pltpu.roll(flipped, SEG, 1)[0:TP]
    index = both.astype(jnp.int32)
    relt[...] = both
    pad[...] = jnp.zeros_like(pad)
    pad[0:WIN, 0:TOK] = reg[...].astype(F32)
    regions = pad[0:WIN, :]
    regions = regions + pltpu.roll(regions, SEG, 1)
    columns = pad[...].T[0:TP]
    for w in range(WIN):
        key = jnp.broadcast_to(columns[:, w : w + 1], (TP, 128))
        mask[w] = jnp.where(key == regions[w : w + 1], 0.0, -100.0).astype(F32)
    tabp[...] = jnp.zeros_like(tabp)
    tabp[:, 0:169] = tab_t[...]
    first = jnp.bitwise_and(index, 127)
    beyond = index >= 128
    real = iota((TP, 128), 0) < TOK

    def looked(h):
        lo = jnp.broadcast_to(tabp[h : h + 1, 0:128], (TP, 128))
        hi = jnp.broadcast_to(tabp[h : h + 1, 128:256], (TP, 128))
        lo = jnp.take_along_axis(lo, first, axis=1, mode="promise_in_bounds")
        hi = jnp.take_along_axis(hi, first, axis=1, mode="promise_in_bounds")
        return jnp.where(beyond, hi, lo)

    for k in range(8):
        value = jnp.where(low, looked(2 * k), looked(2 * k + 1))
        bias[k // 2, :, (k % 2) * 128 : (k % 2 + 1) * 128] = jnp.where(real, value, -1e30)


def gather_windows(src, dst):
    row, col = iota((256, 256), 0), iota((256, 256), 1)
    pick = onehot((row % 16) * 16 + row // 16 == col)
    for part in range(3):
        out = nn(pick, src[part * 256 : (part + 1) * 256, :]).astype(BF)
        dst[:, part * 16 : (part + 1) * 16, :] = out.reshape(WIN, 16, D)
    out = nn(pick[:, 0:16], src[768:784, :]).astype(BF)
    dst[:, 48:64, :] = out.reshape(WIN, 16, D)


def project(wqkv, wproj, xp, cp, qkv, kvt, da, xpt):
    eye = onehot(iota((128, 128), 0) == iota((128, 128), 1))
    s = iota((128, 128), 0)
    wanted = (
        (s // 32) * 32
        + ((s // 4) % 2) * 16
        + ((s // 2) % 2) * 8
        + ((s // 8) % 2) * 4
        + ((s // 16) % 2) * 2
        + s % 2
    )
    strips = onehot(wanted == iota((128, 128), 1))

    def four_windows(c, carry):
        rows = aligned(c * 256, 256, 256)
        x = xp[pl.ds(c * 4, 4)].reshape(256, D)
        y = cp[pl.ds(c * 4, 4)].reshape(256, D)
        values = nn(x, wqkv[...]).astype(BF)
        qkv[rows, :] = values
        da[rows, :] = nt(y, wproj[...]).astype(BF)
        for b in range(4):
            xpt[b * 128 : (b + 1) * 128, rows] = nt(strips, x[:, b * 128 : (b + 1) * 128]).astype(BF)
            k = values[:, 512 + b * 128 : 512 + (b + 1) * 128]
            kvt[b * 128 : (b + 1) * 128, rows] = nt(eye, k).astype(BF)
            v = values[:, 1024 + b * 128 : 1024 + (b + 1) * 128]
            kvt[512 + b * 128 : 512 + (b + 1) * 128, rows] = nt(strips, v).astype(BF)
        return carry

    lax.fori_loop(0, 4, four_windows, 0)


class Attention:
    def __init__(self, qkv, kvt, da, bias, mask, keep, dk, dv, dqt, at, gb):
        self.refs = qkv, kvt, da, bias, mask, keep, dk, dv, dqt, at, gb
        lane = iota((SEG, 256), 1) % 128
        self.heads = [onehot(lane // HEAD_DIM == h) for h in range(4)]
        self.zero = jnp.zeros((SEG, 128), BF)
        self.tail = jnp.zeros((SEG - TP, 256), F32)
        half = iota((128, 128), 1)
        self.left = onehot(half < SEG)
        self.right = onehot(half >= SEG)
        self.low = iota((32, 128), 1) < SEG

    def spread(self, a):
        a = jnp.concatenate([a[0:SEG], a[SEG:]], axis=1)
        return jnp.concatenate([a * head for head in self.heads], axis=0)

    def diagonal(self, a):
        upper = jnp.concatenate([a[0:SEG], self.zero], axis=1)
        lower = jnp.concatenate([self.zero, a[SEG:]], axis=1)
        return jnp.concatenate([upper, lower], axis=0)

    def stack(self, a, b):
        return jnp.concatenate([a, self.tail, b, self.tail], axis=0).astype(BF)

    def own(self, dst, pair, g, value):
        dst[aligned(pair * 128, SEG), aligned(g * 128, 128)] = value[0:SEG, 0:128].astype(BF)
        dst[aligned(pair * 128 + SEG, SEG, SEG), aligned(g * 128, 128)] = value[SEG:, 128:256].astype(BF)

    def across(self, dst, pair, g, turned, wide):
        lhs = jnp.concatenate([turned * self.left, turned * self.right], axis=0)
        full = nn(lhs, wide)
        for h in range(4):
            lanes = slice((h // 2) * 128, (h // 2 + 1) * 128)
            one = full[32 * h : 32 * h + 32, lanes]
            two = full[128 + 32 * h : 128 + 32 * h + 32, lanes]
            if h % 2:
                one = pltpu.roll(one, SEG, 1)
            else:
                two = pltpu.roll(two, SEG, 1)
            value = jnp.where(self.low, one, two).astype(BF)
            dst[aligned(g * 128 + 32 * h, 32, 32), aligned(pair * 128, 128)] = value

    def forward(self, g, pair):
        qkv, kvt, da, bias, mask, keep, dk, dv, dqt, at, gb = self.refs
        rows = aligned(pair * 128, 128)
        q_wide = self.spread(qkv[rows, aligned(g * 128, 128)])
        both = nt(self.diagonal(qkv[rows, aligned(512 + g * 128, 128)]), q_wide)
        probs = []
        for i in range(2):
            scores = both[i * SEG : i * SEG + TP] * SCALE + bias[g]
            scores = scores + jnp.concatenate([mask[2 * pair + i]] * 2, axis=1)
            e = jnp.exp(scores - jnp.max(scores, axis=0, keepdims=True))
            p = e * (1.0 / jnp.sum(e, axis=0, keepdims=True))
            keep[2 * pair + i, :, aligned(g * 256, 256, 256)] = p
            probs.append(p)
        probs = self.stack(*probs)
        da_wide = self.spread(da[rows, aligned(g * 128, 128)])
        self.own(dv, pair, g, nn(probs, da_wide))
        self.across(at, pair, g, kvt[aligned(512 + g * 128, 128), rows], probs)

    def backward(self, g, pair):
        qkv, kvt, da, bias, mask, keep, dk, dv, dqt, at, gb = self.refs
        rows = aligned(pair * 128, 128)
        da_wide = self.spread(da[rows, aligned(g * 128, 128)])
        both = nt(self.diagonal(qkv[rows, aligned(1024 + g * 128, 128)]), da_wide)
        parts = []
        for i in range(2):
            p = keep[2 * pair + i, :, aligned(g * 256, 256, 256)]
            dp = both[i * SEG : i * SEG + TP]
            ds = p * (dp - jnp.sum(p * dp, axis=0, keepdims=True))
            parts.append(ds)
        total = parts[0] + parts[1]
        for k in range(2):
            block = aligned((2 * g + k) * TP, TP, 8)
            gb[block, :] = gb[block, :] + total[:, k * 128 : (k + 1) * 128]
        wide = self.stack(parts[0] * SCALE, parts[1] * SCALE)
        q_wide = self.spread(qkv[rows, aligned(g * 128, 128)])
        self.own(dk, pair, g, nn(wide, q_wide))
        self.across(dqt, pair, g, kvt[aligned(g * 128, 128), rows], wide)

    def run(self, pass_, g):
        def one(t, carry):
            for u in range(UNITS):
                pass_(g, t * UNITS + u)
            return carry

        lax.fori_loop(0, WIN // 2 // UNITS, one, 0)


def table_gradient(gb, relt):
    low = iota((8, 128), 1) < SEG
    entry = iota((256, 128), 0).astype(F32)
    total = jnp.zeros((32, 256), F32)

    def line(j):
        if j >= TOK:
            return jnp.zeros((32, 128), BF), jnp.zeros((256, 128), BF)
        hot = onehot(entry == jnp.broadcast_to(relt[j : j + 1, :], (256, 128)))
        pairs = gb[pl.ds(j, 8, stride=TP), :]
        split = jnp.concatenate([jnp.where(low, pairs, 0.0), jnp.where(low, 0.0, pairs)], axis=0)
        upper = split.astype(BF)
        lower = (split - upper.astype(F32)).astype(BF)
        return jnp.concatenate([upper, lower], axis=0), hot

    for j in range(0, TOK, 2):
        a, b = line(j), line(j + 1)
        total = total + nt(
            jnp.concatenate([a[0], b[0]], axis=1), jnp.concatenate([a[1], b[1]], axis=1)
        )
    return total[0:16] + total[16:32]


class Exchange:
    def __init__(self, g, s1, ra, rb, a2, b2, ra2, rb2, zs, rz, tt, tr, send, recv):
        self.g, self.s1, self.ra, self.rb, self.a2, self.b2 = g, s1, ra, rb, a2, b2
        self.ra2, self.rb2, self.zs, self.rz, self.tt, self.tr = ra2, rb2, zs, rz, tt, tr
        self.send, self.recv, self.used = send, recv, 0
        gx, gy, gz = lax.axis_index("gx"), lax.axis_index("gy"), lax.axis_index("gz")
        x, z, core = lax.rem(gx, 4), gy, lax.rem(gz, 2)
        y = (gx // 4) * 2 + gz // 2

        def device(x, y, z, core):
            return ((y // 2) * 4 + x, z, lax.rem(y, 2) * 2 + core)

        def xor(a, b):
            out = 0
            for bit in (1, 2, 4):
                have = lax.rem(a // bit, 2)
                out = out + bit * ((1 - have) if b & bit else have)
            return out

        self.x, self.y, self.z, self.core = x, y, z, core
        self.partner = device(x, y, z, 1 - core)
        self.along_x = [(xor(x, d), device(xor(x, d), y, z, core)) for d in (1, 2, 3)]
        self.along_y = [(xor(y, d), device(x, xor(y, d), z, core)) for d in (1, 2, 3)]
        self.along_z = [(xor(z, d), device(x, y, xor(z, d), core)) for d in range(1, 8)]
        self.flight = {}

    def greet(self):
        self.peers = [self.partner] + [dev for _, dev in self.along_x + self.along_y + self.along_z]
        barrier = pltpu.get_barrier_semaphore()
        for peer in self.peers:
            pl.semaphore_signal(barrier, inc=1, device_id=peer, device_id_type=MESH)

    def greeted(self):
        pl.semaphore_wait(pltpu.get_barrier_semaphore(), len(self.peers))

    def start(self, key, src, dst, dev):
        n = self.used
        self.used += 1
        c = pltpu.make_async_remote_copy(
            src_ref=src, dst_ref=dst, send_sem=self.send.at[n], recv_sem=self.recv.at[n],
            device_id=dev, device_id_type=MESH,
        )
        c.start()
        self.flight.setdefault(key, []).append(c)

    def finish(self, key):
        for c in self.flight.pop(key):
            c.wait()

    def put(self, c, lo, value):
        lanes = slice(lo, lo + value.shape[1])
        for strip in range(16):
            y1, x, z2 = strip // 8, (strip // 2) % 4, strip % 2
            for core in range(2):
                for y0 in range(2):
                    r = strip * 32 + core * 16 + y0 * 8
                    self.g[c, core, z2, y1 * 2 + y0, x, :, lanes] = value[r : r + 8]

    def cores(self, c):
        self.start(("p0", c), self.g.at[c, 1 - self.core], self.s1.at[c], self.partner)

    def first(self, c):
        self.finish(("p0", c))
        for half in range(2):
            self.s1[c, half] = self.s1[c, half] + self.g[c, self.core, half]
        for n, (to, dev) in enumerate(self.along_x):
            self.start(("p1", c), self.s1.at[c, 0, :, to], self.ra.at[c, n], dev)
        for n, (to, dev) in enumerate(self.along_y):
            self.start(("p1", c), self.s1.at[c, 1, to], self.rb.at[c, n], dev)

    def second(self, lo, hi):
        for c in range(lo, hi):
            self.finish(("p1", c))
            self.a2[c] = self.s1[c, 0, :, self.x] + self.ra[c, 0] + self.ra[c, 1] + self.ra[c, 2]
            self.b2[c] = self.s1[c, 1, self.y] + self.rb[c, 0] + self.rb[c, 1] + self.rb[c, 2]
        span = pl.ds(lo, hi - lo)
        for n, (to, dev) in enumerate(self.along_y):
            self.start(("p2", lo), self.a2.at[span, to], self.ra2.at[n, span], dev)
        for n, (to, dev) in enumerate(self.along_x):
            self.start(("p2", lo), self.b2.at[span, to], self.rb2.at[n, span], dev)

    def third(self, lo, hi):
        self.finish(("p2", lo))
        for c in range(lo, hi):
            a = self.a2[c, self.y] + self.ra2[0, c] + self.ra2[1, c] + self.ra2[2, c]
            b = self.b2[c, self.x] + self.rb2[0, c] + self.rb2[1, c] + self.rb2[2, c]
            for k in range(4):
                self.zs[c, k] = a[2 * k : 2 * k + 2]
                self.zs[c, 4 + k] = b[2 * k : 2 * k + 2]
        span = pl.ds(lo, hi - lo)
        for n, (to, dev) in enumerate(self.along_z):
            self.start(("p3", lo), self.zs.at[span, to], self.rz.at[n, span], dev)

    def last(self, lo, hi):
        self.finish(("p3", lo))
        out = []
        for c in range(lo, hi):
            mine = self.zs[c, self.z]
            for n in range(7):
                mine = mine + self.rz[n, c]
            out.append(mine)
        return out

    def table_cores(self, value):
        self.tt[0, 0] = value[0:8]
        self.tt[0, 1] = value[8:16]
        self.start("t0", self.tt.at[0, 1 - self.core], self.tr.at[0], self.partner)

    def table_axis(self, key, stage, first, count, own, peers):
        total = own
        if key is not None:
            self.finish(key)
            for n in range(count):
                total = total + self.tr[first + n]
        self.tt[stage, 0] = total
        for n, (_, dev) in enumerate(peers):
            self.start("t%d" % stage, self.tt.at[stage, 0], self.tr.at[first + count + n], dev)


def kernel(scale, *refs):
    refs = list(refs)

    def take(n):
        out = refs[:n]
        del refs[:n]
        return out

    tok_hbm, cot_hbm, reg, rel, wqkv_hbm, wproj_hbm, tab_t = take(7)
    mom_qkv, mom_proj, mom_tab = take(3)
    out_qkv, out_proj, out_tab = take(3)
    tok, cot, wqkv, wproj, fetched = take(5)
    xp, cp, qkv, kvt, da, xpt = take(6)
    bias, mask, keep, dk, dv, dqt, at, gb, pad, tabp, relt = take(11)
    ex = Exchange(*refs)

    fetches = []
    for n, (src, dst) in enumerate(((tok_hbm, tok), (cot_hbm, cot), (wqkv_hbm, wqkv), (wproj_hbm, wproj))):
        fetch = pltpu.make_async_copy(src, dst, fetched.at[n])
        fetch.start()
        fetches.append(fetch)
    ex.greet()
    small_tables(reg, rel, tab_t, bias, mask, pad, tabp, relt)
    gb[...] = jnp.zeros_like(gb)
    fetches[0].wait()
    gather_windows(tok, xp)
    fetches[1].wait()
    gather_windows(cot, cp)
    fetches[2].wait()
    fetches[3].wait()
    project(wqkv, wproj, xp, cp, qkv, kvt, da, xpt)

    att = Attention(qkv, kvt, da, bias, mask, keep, dk, dv, dqt, at, gb)

    def v_chunk(c):
        ex.put(c, 0, nn(xpt[...], dv[:, c * 256 : (c + 1) * 256]))
        ex.cores(c)

    def proj_chunk(c):
        y = cp[:, :, c * 256 : (c + 1) * 256].reshape(WIN * SEG, 256)
        ex.put(2 + c, 0, nn(at[...], y))
        ex.cores(2 + c)

    def qk_chunk(g):
        ex.put(4 + g, 0, nt(xpt[...], dqt[g * 128 : (g + 1) * 128, :]))
        ex.put(4 + g, 128, nn(xpt[...], dk[:, g * 128 : (g + 1) * 128]))
        ex.cores(4 + g)

    att.run(att.forward, 0)
    att.run(att.forward, 1)
    ex.greeted()
    v_chunk(0)
    att.run(att.forward, 2)
    ex.first(0)
    att.run(att.forward, 3)
    v_chunk(1)
    proj_chunk(0)
    ex.first(1)
    proj_chunk(1)
    ex.first(2)
    att.run(att.backward, 0)
    ex.first(3)
    qk_chunk(0)
    att.run(att.backward, 1)
    ex.first(4)
    ex.second(0, 4)
    qk_chunk(1)
    att.run(att.backward, 2)
    ex.first(5)
    ex.third(0, 4)
    qk_chunk(2)
    att.run(att.backward, 3)
    ex.first(6)
    qk_chunk(3)
    ex.second(4, 6)
    ex.table_cores(table_gradient(gb, relt))
    ex.first(7)
    own = ex.tt[0, ex.core]
    ex.finish("t0")
    ex.table_axis(None, 1, 0, 1, own + ex.tr[0], ex.along_x)
    ex.third(4, 6)
    ex.second(6, 8)
    ex.table_axis("t1", 2, 1, 3, ex.tt[1, 0], ex.along_y)
    ex.third(6, 8)
    ex.table_axis("t2", 3, 4, 3, ex.tt[2, 0], ex.along_z)

    def finish(lo, hi):
        for c, mine in zip(range(lo, hi), ex.last(lo, hi)):
            for r in range(2):
                for part in range(2):
                    value = mine[r : r + 1, part * 128 : (part + 1) * 128] * scale
                    if 2 <= c < 4:
                        k = r * 4 + (c - 2) * 2 + part
                        out_proj[k : k + 1, :] = 0.9 * mom_proj[k : k + 1, :] + value
                    else:
                        col = 8 + c * 2 + part if c < 2 else part * 4 + c - 4
                        k = r * 12 + col
                        out_qkv[k : k + 1, :] = 0.9 * mom_qkv[k : k + 1, :] + value

    finish(0, 4)
    finish(4, 6)
    finish(6, 8)
    ex.finish("t3")
    table = ex.tt[3, 0]
    for n in range(7):
        table = table + ex.tr[7 + n]
    ex.tt[4, 0] = table
    ex.start("t4", ex.tt.at[4, 0], ex.tr.at[14], ex.partner)
    ex.finish("t4")
    core = ex.core.astype(F32)
    other = ex.tr[14]
    even = table * (1.0 - core) + other * core
    odd = table * core + other * (1.0 - core)
    for k in range(8):
        out_tab[2 * k : 2 * k + 1, :] = 0.9 * mom_tab[2 * k : 2 * k + 1, :] + even[k : k + 1, 0:169] * scale
        out_tab[2 * k + 1 : 2 * k + 2, :] = (
            0.9 * mom_tab[2 * k + 1 : 2 * k + 2, :] + odd[k : k + 1, 0:169] * scale
        )


SCRATCH = [
    pltpu.VMEM((784, D), BF),
    pltpu.VMEM((784, D), BF),
    pltpu.VMEM((D, 3 * D), BF),
    pltpu.VMEM((D, D), BF),
    pltpu.SemaphoreType.DMA((4,)),
    pltpu.VMEM((WIN, SEG, D), BF),
    pltpu.VMEM((WIN, SEG, D), BF),
    pltpu.VMEM((1024, 3 * D), BF),
    pltpu.VMEM((1024, 1024), BF),
    pltpu.VMEM((1024, D), BF),
    pltpu.VMEM((D, 1024), BF),
    pltpu.VMEM((4, TP, 256), F32),
    pltpu.VMEM((WIN, TP, 128), F32),
    pltpu.VMEM((WIN, TP, 1024), F32),
    pltpu.VMEM((1024, D), BF),
    pltpu.VMEM((1024, D), BF),
    pltpu.VMEM((D, 1024), BF),
    pltpu.VMEM((D, 1024), BF),
    pltpu.VMEM((8 * TP, 128), F32),
    pltpu.VMEM((128, 128), F32),
    pltpu.VMEM((16, 256), F32),
    pltpu.VMEM((TP, 128), F32),
    pltpu.VMEM((CHUNKS, 2, 2, 4, 4, 8, CH), F32),
    pltpu.VMEM((CHUNKS, 2, 4, 4, 8, CH), F32),
    pltpu.VMEM((CHUNKS, 3, 4, 8, CH), F32),
    pltpu.VMEM((CHUNKS, 3, 4, 8, CH), F32),
    pltpu.VMEM((CHUNKS, 4, 8, CH), F32),
    pltpu.VMEM((CHUNKS, 4, 8, CH), F32),
    pltpu.VMEM((3, CHUNKS, 8, CH), F32),
    pltpu.VMEM((3, CHUNKS, 8, CH), F32),
    pltpu.VMEM((CHUNKS, 8, 2, CH), F32),
    pltpu.VMEM((7, CHUNKS, 2, CH), F32),
    pltpu.VMEM((5, 2, 8, CH), F32),
    pltpu.VMEM((15, 8, CH), F32),
    pltpu.SemaphoreType.DMA((120,)),
    pltpu.SemaphoreType.DMA((120,)),
]


def step(scale, *operands):
    vm = pl.BlockSpec(memory_space=pltpu.VMEM)
    hbm = pl.BlockSpec(memory_space=pl.ANY)
    return pl.pallas_call(
        functools.partial(kernel, scale),
        name="step",
        out_shape=(
            jax.ShapeDtypeStruct((24, 128), F32),
            jax.ShapeDtypeStruct((8, 128), F32),
            jax.ShapeDtypeStruct((16, 169), F32),
        ),
        in_specs=[hbm, hbm, vm, vm, hbm, hbm, vm, vm, vm, vm],
        out_specs=(vm, vm, vm),
        scratch_shapes=SCRATCH,
        compiler_params=pltpu.CompilerParams(
            collective_id=0, has_side_effects=True, vmem_limit_bytes=60 * 2**20
        ),
    )(*operands)


def body(tokens, cotangent, regions, rel_index, w_qkv, w_proj, bias_table, mom_qkv, mom_proj, mom_table):
    win, count, dim = tokens.shape
    devices = lax.axis_size(("gx", "gy", "gz"))
    tok = jnp.transpose(tokens, (1, 0, 2)).reshape(count * win, dim)
    cot = jnp.transpose(cotangent, (1, 0, 2)).reshape(count * win, dim)
    out_qkv, out_proj, out_tab = step(
        1.0 / (win * devices), tok, cot, regions, rel_index, w_qkv, w_proj, bias_table.T,
        mom_qkv.reshape(24, 128), mom_proj.reshape(8, 128), mom_table.T,
    )
    return out_qkv.reshape(-1), out_proj.reshape(-1), out_tab.T


def solution(mesh):
    rows = P(("gx", "gy", "gz"))
    wide = P(("gx", "gy", "gz"), None, None)
    return jax.shard_map(
        body,
        mesh=mesh,
        in_specs=(wide, wide, P(("gx", "gy", "gz"), None), P(), P(), P(), P(), rows, rows, P()),
        out_specs=(rows, rows, P()),
        check_vma=False,
    )
```

```python
import functools

import jax
import jax.numpy as jnp
from jax import lax
from jax.experimental import pallas as pl
from jax.experimental.pallas import tpu as pltpu
from jax.sharding import PartitionSpec as P

MESH = pl.DeviceIdType.MESH
BF = jnp.bfloat16
F32 = jnp.float32
WIN = 16
TOK = 49
SEG = 64
TP = 56
D = 512
HEAD_DIM = 32
SCALE = HEAD_DIM ** -0.5
UNITS = 4
STEPS = 4 * WIN // 2 // UNITS
GROUP = STEPS // 4
CH = 256
CHUNKS = 8


def nt(a, b):
    return lax.dot_general(a, b, (((1,), (1,)), ((), ())), preferred_element_type=F32)


def nn(a, b):
    return jnp.dot(a, b, preferred_element_type=F32)


def iota(shape, dim):
    return lax.broadcasted_iota(jnp.int32, shape, dim)


def onehot(condition):
    return condition.astype(F32).astype(BF)


def aligned(start, size, to=128):
    return pl.ds(pl.multiple_of(start, to), size)


def small_tables(reg, rel, tab_t, bias, mask, pad, tabp, relt):
    low = iota((TP, 128), 1) < SEG
    pad[...] = jnp.zeros_like(pad)
    pad[0:TOK, 0:TOK] = rel[...].astype(F32)
    flipped = pad[...].T
    both = flipped[0:TP] + pltpu.roll(flipped, SEG, 1)[0:TP]
    index = both.astype(jnp.int32)
    relt[...] = both
    pad[...] = jnp.zeros_like(pad)
    pad[0:WIN, 0:TOK] = reg[...].astype(F32)
    regions = pad[0:WIN, :]
    regions = regions + pltpu.roll(regions, SEG, 1)
    columns = pad[...].T[0:TP]
    for w in range(WIN):
        key = jnp.broadcast_to(columns[:, w : w + 1], (TP, 128))
        mask[w] = jnp.where(key == regions[w : w + 1], 0.0, -100.0).astype(F32)
    tabp[...] = jnp.zeros_like(tabp)
    tabp[:, 0:169] = tab_t[...]
    first = jnp.bitwise_and(index, 127)
    beyond = index >= 128
    real = iota((TP, 128), 0) < TOK

    def looked(h):
        lo = jnp.broadcast_to(tabp[h : h + 1, 0:128], (TP, 128))
        hi = jnp.broadcast_to(tabp[h : h + 1, 128:256], (TP, 128))
        lo = jnp.take_along_axis(lo, first, axis=1, mode="promise_in_bounds")
        hi = jnp.take_along_axis(hi, first, axis=1, mode="promise_in_bounds")
        return jnp.where(beyond, hi, lo)

    for k in range(8):
        value = jnp.where(low, looked(2 * k), looked(2 * k + 1))
        bias[k // 2, :, (k % 2) * 128 : (k % 2 + 1) * 128] = jnp.where(real, value, -1e30)


def gather_windows(src, dst):
    row, col = iota((256, 256), 0), iota((256, 256), 1)
    pick = onehot((row % 16) * 16 + row // 16 == col)
    for part in range(3):
        out = nn(pick, src[part * 256 : (part + 1) * 256, :]).astype(BF)
        dst[:, part * 16 : (part + 1) * 16, :] = out.reshape(WIN, 16, D)
    out = nn(pick[:, 0:16], src[768:784, :]).astype(BF)
    dst[:, 48:64, :] = out.reshape(WIN, 16, D)


def project(wqkv, wproj, xp, cp, qkv, kvt, da, xpt):
    eye = onehot(iota((128, 128), 0) == iota((128, 128), 1))
    s = iota((128, 128), 0)
    wanted = (
        (s // 32) * 32
        + ((s // 4) % 2) * 16
        + ((s // 2) % 2) * 8
        + ((s // 8) % 2) * 4
        + ((s // 16) % 2) * 2
        + s % 2
    )
    strips = onehot(wanted == iota((128, 128), 1))

    def four_windows(c, carry):
        rows = aligned(c * 256, 256, 256)
        x = xp[pl.ds(c * 4, 4)].reshape(256, D)
        y = cp[pl.ds(c * 4, 4)].reshape(256, D)
        values = nn(x, wqkv[...]).astype(BF)
        qkv[rows, :] = values
        da[rows, :] = nt(y, wproj[...]).astype(BF)
        for b in range(4):
            xpt[b * 128 : (b + 1) * 128, rows] = nt(strips, x[:, b * 128 : (b + 1) * 128]).astype(BF)
            k = values[:, 512 + b * 128 : 512 + (b + 1) * 128]
            kvt[b * 128 : (b + 1) * 128, rows] = nt(eye, k).astype(BF)
            v = values[:, 1024 + b * 128 : 1024 + (b + 1) * 128]
            kvt[512 + b * 128 : 512 + (b + 1) * 128, rows] = nt(strips, v).astype(BF)
        return carry

    lax.fori_loop(0, 4, four_windows, 0)


class Attention:
    def __init__(self, qkv, kvt, da, bias, mask, keep, dk, dv, dqt, at, gb, raw, wide):
        self.qkv, self.kvt, self.da, self.bias, self.mask = qkv, kvt, da, bias, mask
        self.keep, self.dk, self.dv, self.dqt, self.at = keep, dk, dv, dqt, at
        self.gb, self.raw, self.wide = gb, raw, wide
        lane = iota((SEG, 256), 1) % 128
        self.heads = [onehot(lane // HEAD_DIM == h) for h in range(4)]
        self.zero = jnp.zeros((SEG, 128), BF)
        self.tail = jnp.zeros((SEG - TP, 256), F32)
        half = iota((128, 128), 1)
        self.left = onehot(half < SEG)
        self.right = onehot(half >= SEG)
        self.low = iota((32, 128), 1) < SEG

    def spread(self, a):
        a = jnp.concatenate([a[0:SEG], a[SEG:]], axis=1)
        return jnp.concatenate([a * head for head in self.heads], axis=0)

    def diagonal(self, a):
        upper = jnp.concatenate([a[0:SEG], self.zero], axis=1)
        lower = jnp.concatenate([self.zero, a[SEG:]], axis=1)
        return jnp.concatenate([upper, lower], axis=0)

    def stack(self, a, b):
        return jnp.concatenate([a, self.tail, b, self.tail], axis=0).astype(BF)

    def own(self, dst, pair, g, value):
        dst[aligned(pair * 128, SEG), aligned(g * 128, 128)] = value[0:SEG, 0:128].astype(BF)
        dst[aligned(pair * 128 + SEG, SEG, SEG), aligned(g * 128, 128)] = value[SEG:, 128:256].astype(BF)

    def across(self, dst, pair, g, turned, wide):
        lhs = jnp.concatenate([turned * self.left, turned * self.right], axis=0)
        full = nn(lhs, wide)
        for h in range(4):
            lanes = slice((h // 2) * 128, (h // 2 + 1) * 128)
            one = full[32 * h : 32 * h + 32, lanes]
            two = full[128 + 32 * h : 128 + 32 * h + 32, lanes]
            if h % 2:
                one = pltpu.roll(one, SEG, 1)
            else:
                two = pltpu.roll(two, SEG, 1)
            value = jnp.where(self.low, one, two).astype(BF)
            dst[aligned(g * 128 + 32 * h, 32, 32), aligned(pair * 128, 128)] = value

    def place(self, unit):
        return unit // (WIN // 2), unit % (WIN // 2)

    def forward1(self, u, unit):
        g, pair = self.place(unit)
        rows = aligned(pair * 128, 128)
        q_wide = self.spread(self.qkv[rows, aligned(g * 128, 128)])
        self.raw[u] = nt(self.diagonal(self.qkv[rows, aligned(512 + g * 128, 128)]), q_wide)

    def forward2(self, u, unit):
        g, pair = self.place(unit)
        probs = []
        for i in range(2):
            scores = self.raw[u, i * SEG : i * SEG + TP, :] * SCALE + self.bias[g]
            scores = scores + jnp.concatenate([self.mask[2 * pair + i]] * 2, axis=1)
            e = jnp.exp(scores - jnp.max(scores, axis=0, keepdims=True))
            p = e * (1.0 / jnp.sum(e, axis=0, keepdims=True))
            self.keep[2 * unit + i] = p
            probs.append(p)
        self.wide[u] = self.stack(*probs)

    def forward3(self, u, unit):
        g, pair = self.place(unit)
        rows = aligned(pair * 128, 128)
        probs = self.wide[u]
        da_wide = self.spread(self.da[rows, aligned(g * 128, 128)])
        self.own(self.dv, pair, g, nn(probs, da_wide))
        self.across(self.at, pair, g, self.kvt[aligned(512 + g * 128, 128), rows], probs)

    def backward1(self, u, unit):
        g, pair = self.place(unit)
        rows = aligned(pair * 128, 128)
        da_wide = self.spread(self.da[rows, aligned(g * 128, 128)])
        self.raw[u] = nt(self.diagonal(self.qkv[rows, aligned(1024 + g * 128, 128)]), da_wide)

    def backward2(self, u, unit):
        g, pair = self.place(unit)
        parts = []
        for i in range(2):
            p = self.keep[2 * unit + i]
            dp = self.raw[u, i * SEG : i * SEG + TP, :]
            parts.append(p * (dp - jnp.sum(p * dp, axis=0, keepdims=True)))
        total = parts[0] + parts[1]
        for k in range(2):
            block = aligned((2 * g + k) * TP, TP, 8)
            self.gb[block, :] = self.gb[block, :] + total[:, k * 128 : (k + 1) * 128]
        self.wide[u] = self.stack(parts[0] * SCALE, parts[1] * SCALE)

    def backward3(self, u, unit):
        g, pair = self.place(unit)
        rows = aligned(pair * 128, 128)
        wide = self.wide[u]
        q_wide = self.spread(self.qkv[rows, aligned(g * 128, 128)])
        self.own(self.dk, pair, g, nn(wide, q_wide))
        self.across(self.dqt, pair, g, self.kvt[aligned(g * 128, 128), rows], wide)

    def stages(self, stages, t, which):
        for n in (2, 1, 0):
            if n in which:
                for u in range(UNITS):
                    stages[n](u, (t - n) * UNITS + u)

    def run(self, stages, lo, hi):
        if lo == 0:
            self.stages(stages, 0, (0,))
            self.stages(stages, 1, (0, 1))
        end = STEPS if hi == STEPS else hi + 2

        def one(t, carry):
            self.stages(stages, t, (0, 1, 2))
            return carry

        lax.fori_loop(lo + 2, end, one, 0)
        if hi == STEPS:
            self.stages(stages, STEPS, (1, 2))
            self.stages(stages, STEPS + 1, (2,))


def table_gradient(gb, relt):
    low = iota((8, 128), 1) < SEG
    entry = iota((256, 128), 0).astype(F32)
    total = jnp.zeros((32, 256), F32)

    def line(j):
        if j >= TOK:
            return jnp.zeros((32, 128), BF), jnp.zeros((256, 128), BF)
        hot = onehot(entry == jnp.broadcast_to(relt[j : j + 1, :], (256, 128)))
        pairs = gb[pl.ds(j, 8, stride=TP), :]
        split = jnp.concatenate([jnp.where(low, pairs, 0.0), jnp.where(low, 0.0, pairs)], axis=0)
        upper = split.astype(BF)
        lower = (split - upper.astype(F32)).astype(BF)
        return jnp.concatenate([upper, lower], axis=0), hot

    for j in range(0, TOK, 2):
        a, b = line(j), line(j + 1)
        total = total + nt(
            jnp.concatenate([a[0], b[0]], axis=1), jnp.concatenate([a[1], b[1]], axis=1)
        )
    return total[0:16] + total[16:32]


class Exchange:
    def __init__(self, g, s1, ra, rb, a2, b2, ra2, rb2, zs, rz, tt, tr, send, recv):
        self.g, self.s1, self.ra, self.rb, self.a2, self.b2 = g, s1, ra, rb, a2, b2
        self.ra2, self.rb2, self.zs, self.rz, self.tt, self.tr = ra2, rb2, zs, rz, tt, tr
        self.send, self.recv, self.used = send, recv, 0
        gx, gy, gz = lax.axis_index("gx"), lax.axis_index("gy"), lax.axis_index("gz")
        x, z, core = lax.rem(gx, 4), gy, lax.rem(gz, 2)
        y = (gx // 4) * 2 + gz // 2

        def device(x, y, z, core):
            return ((y // 2) * 4 + x, z, lax.rem(y, 2) * 2 + core)

        def xor(a, b):
            out = 0
            for bit in (1, 2, 4):
                have = lax.rem(a // bit, 2)
                out = out + bit * ((1 - have) if b & bit else have)
            return out

        self.x, self.y, self.z, self.core = x, y, z, core
        self.partner = device(x, y, z, 1 - core)
        self.along_x = [(xor(x, d), device(xor(x, d), y, z, core)) for d in (1, 2, 3)]
        self.along_y = [(xor(y, d), device(x, xor(y, d), z, core)) for d in (1, 2, 3)]
        self.along_z = [(xor(z, d), device(x, y, xor(z, d), core)) for d in range(1, 8)]
        self.flight = {}

    def greet(self):
        self.peers = [self.partner] + [dev for _, dev in self.along_x + self.along_y + self.along_z]
        barrier = pltpu.get_barrier_semaphore()
        for peer in self.peers:
            pl.semaphore_signal(barrier, inc=1, device_id=peer, device_id_type=MESH)

    def greeted(self):
        pl.semaphore_wait(pltpu.get_barrier_semaphore(), len(self.peers))

    def start(self, key, src, dst, dev):
        n = self.used
        self.used += 1
        c = pltpu.make_async_remote_copy(
            src_ref=src, dst_ref=dst, send_sem=self.send.at[n], recv_sem=self.recv.at[n],
            device_id=dev, device_id_type=MESH,
        )
        c.start()
        self.flight.setdefault(key, []).append(c)

    def finish(self, key):
        for c in self.flight.pop(key):
            c.wait()

    def put(self, c, lo, value):
        lanes = slice(lo, lo + value.shape[1])
        for strip in range(16):
            y1, x, z2 = strip // 8, (strip // 2) % 4, strip % 2
            for core in range(2):
                for y0 in range(2):
                    r = strip * 32 + core * 16 + y0 * 8
                    self.g[c, core, z2, y1 * 2 + y0, x, :, lanes] = value[r : r + 8]

    def cores(self, c):
        self.start(("p0", c), self.g.at[c, 1 - self.core], self.s1.at[c], self.partner)

    def first(self, c):
        self.finish(("p0", c))
        for half in range(2):
            self.s1[c, half] = self.s1[c, half] + self.g[c, self.core, half]
        for n, (to, dev) in enumerate(self.along_x):
            self.start(("p1", c), self.s1.at[c, 0, :, to], self.ra.at[c, n], dev)
        for n, (to, dev) in enumerate(self.along_y):
            self.start(("p1", c), self.s1.at[c, 1, to], self.rb.at[c, n], dev)

    def second(self, lo, hi):
        for c in range(lo, hi):
            self.finish(("p1", c))
            self.a2[c] = self.s1[c, 0, :, self.x] + self.ra[c, 0] + self.ra[c, 1] + self.ra[c, 2]
            self.b2[c] = self.s1[c, 1, self.y] + self.rb[c, 0] + self.rb[c, 1] + self.rb[c, 2]
        span = pl.ds(lo, hi - lo)
        for n, (to, dev) in enumerate(self.along_y):
            self.start(("p2", lo), self.a2.at[span, to], self.ra2.at[n, span], dev)
        for n, (to, dev) in enumerate(self.along_x):
            self.start(("p2", lo), self.b2.at[span, to], self.rb2.at[n, span], dev)

    def third(self, lo, hi):
        self.finish(("p2", lo))
        for c in range(lo, hi):
            a = self.a2[c, self.y] + self.ra2[0, c] + self.ra2[1, c] + self.ra2[2, c]
            b = self.b2[c, self.x] + self.rb2[0, c] + self.rb2[1, c] + self.rb2[2, c]
            for k in range(4):
                self.zs[c, k] = a[2 * k : 2 * k + 2]
                self.zs[c, 4 + k] = b[2 * k : 2 * k + 2]
        span = pl.ds(lo, hi - lo)
        for n, (to, dev) in enumerate(self.along_z):
            self.start(("p3", lo), self.zs.at[span, to], self.rz.at[n, span], dev)

    def last(self, lo, hi):
        self.finish(("p3", lo))
        out = []
        for c in range(lo, hi):
            mine = self.zs[c, self.z]
            for n in range(7):
                mine = mine + self.rz[n, c]
            out.append(mine)
        return out

    def table_cores(self, value):
        self.tt[0, 0] = value[0:8]
        self.tt[0, 1] = value[8:16]
        self.start("t0", self.tt.at[0, 1 - self.core], self.tr.at[0], self.partner)

    def table_axis(self, key, stage, first, count, own, peers):
        total = own
        if key is not None:
            self.finish(key)
            for n in range(count):
                total = total + self.tr[first + n]
        self.tt[stage, 0] = total
        for n, (_, dev) in enumerate(peers):
            self.start("t%d" % stage, self.tt.at[stage, 0], self.tr.at[first + count + n], dev)


def kernel(*refs):
    refs = list(refs)

    def take(n):
        out = refs[:n]
        del refs[:n]
        return out

    tok_hbm, cot_hbm, reg, rel, wqkv_hbm, wproj_hbm, tab_t = take(7)
    out_qkv, out_proj, out_tab = take(3)
    tok, cot, wqkv, wproj, fetched = take(5)
    xp, cp, qkv, kvt, da, xpt = take(6)
    bias, mask, keep, dk, dv, dqt, at, gb, pad, tabp, relt, raw, wide = take(13)
    ex = Exchange(*refs)

    fetches = []
    for n, (src, dst) in enumerate(((tok_hbm, tok), (cot_hbm, cot), (wqkv_hbm, wqkv), (wproj_hbm, wproj))):
        fetch = pltpu.make_async_copy(src, dst, fetched.at[n])
        fetch.start()
        fetches.append(fetch)
    ex.greet()
    small_tables(reg, rel, tab_t, bias, mask, pad, tabp, relt)
    gb[...] = jnp.zeros_like(gb)
    fetches[0].wait()
    gather_windows(tok, xp)
    fetches[1].wait()
    gather_windows(cot, cp)
    fetches[2].wait()
    fetches[3].wait()
    project(wqkv, wproj, xp, cp, qkv, kvt, da, xpt)

    att = Attention(qkv, kvt, da, bias, mask, keep, dk, dv, dqt, at, gb, raw, wide)
    forward = att.forward1, att.forward2, att.forward3
    backward = att.backward1, att.backward2, att.backward3

    def v_chunk(c):
        ex.put(c, 0, nn(xpt[...], dv[:, c * 256 : (c + 1) * 256]))
        ex.cores(c)

    def proj_chunk(c):
        y = cp[:, :, c * 256 : (c + 1) * 256].reshape(WIN * SEG, 256)
        ex.put(2 + c, 0, nn(at[...], y))
        ex.cores(2 + c)

    def qk_chunk(g):
        ex.put(4 + g, 0, nt(xpt[...], dqt[g * 128 : (g + 1) * 128, :]))
        ex.put(4 + g, 128, nn(xpt[...], dk[:, g * 128 : (g + 1) * 128]))
        ex.cores(4 + g)

    att.run(forward, 0, 2 * GROUP)
    ex.greeted()
    v_chunk(0)
    att.run(forward, 2 * GROUP, 4 * GROUP)
    ex.first(0)
    v_chunk(1)
    proj_chunk(0)
    ex.first(1)
    proj_chunk(1)
    ex.first(2)
    att.run(backward, 0, GROUP)
    ex.first(3)
    qk_chunk(0)
    att.run(backward, GROUP, 2 * GROUP)
    ex.first(4)
    ex.second(0, 4)
    qk_chunk(1)
    att.run(backward, 2 * GROUP, 3 * GROUP)
    ex.first(5)
    ex.third(0, 4)
    qk_chunk(2)
    att.run(backward, 3 * GROUP, 4 * GROUP)
    ex.first(6)
    qk_chunk(3)
    ex.second(4, 6)
    ex.table_cores(table_gradient(gb, relt))
    ex.first(7)
    own = ex.tt[0, ex.core]
    ex.finish("t0")
    ex.table_axis(None, 1, 0, 1, own + ex.tr[0], ex.along_x)
    ex.third(4, 6)
    ex.table_axis("t1", 2, 1, 3, ex.tt[1, 0], ex.along_y)
    ex.second(6, 8)
    ex.table_axis("t2", 3, 4, 3, ex.tt[2, 0], ex.along_z)
    ex.third(6, 8)

    def finish(lo, hi):
        for c, mine in zip(range(lo, hi), ex.last(lo, hi)):
            for r in range(2):
                for part in range(2):
                    value = mine[r : r + 1, part * 128 : (part + 1) * 128]
                    if 2 <= c < 4:
                        k = r * 4 + (c - 2) * 2 + part
                        out_proj[k : k + 1, :] = value
                    else:
                        col = 8 + c * 2 + part if c < 2 else part * 4 + c - 4
                        k = r * 12 + col
                        out_qkv[k : k + 1, :] = value

    finish(0, 4)
    finish(4, 6)
    finish(6, 8)
    ex.finish("t3")
    table = ex.tt[3, 0]
    for n in range(7):
        table = table + ex.tr[7 + n]
    ex.tt[4, 0] = table
    ex.start("t4", ex.tt.at[4, 0], ex.tr.at[14], ex.partner)
    ex.finish("t4")
    core = ex.core.astype(F32)
    other = ex.tr[14]
    even = table * (1.0 - core) + other * core
    odd = table * core + other * (1.0 - core)
    for k in range(8):
        out_tab[2 * k : 2 * k + 1, :] = even[k : k + 1, 0:169]
        out_tab[2 * k + 1 : 2 * k + 2, :] = odd[k : k + 1, 0:169]


def apply_kernel(scale, *refs):
    for total, momentum, out in zip(refs[0:3], refs[3:6], refs[6:9]):
        out[...] = 0.9 * momentum[...] + total[...] * scale


SCRATCH = [
    pltpu.VMEM((784, D), BF),
    pltpu.VMEM((784, D), BF),
    pltpu.VMEM((D, 3 * D), BF),
    pltpu.VMEM((D, D), BF),
    pltpu.SemaphoreType.DMA((4,)),
    pltpu.VMEM((WIN, SEG, D), BF),
    pltpu.VMEM((WIN, SEG, D), BF),
    pltpu.VMEM((1024, 3 * D), BF),
    pltpu.VMEM((1024, 1024), BF),
    pltpu.VMEM((1024, D), BF),
    pltpu.VMEM((D, 1024), BF),
    pltpu.VMEM((4, TP, 256), F32),
    pltpu.VMEM((WIN, TP, 128), F32),
    pltpu.VMEM((4 * WIN, TP, 256), F32),
    pltpu.VMEM((1024, D), BF),
    pltpu.VMEM((1024, D), BF),
    pltpu.VMEM((D, 1024), BF),
    pltpu.VMEM((D, 1024), BF),
    pltpu.VMEM((8 * TP, 128), F32),
    pltpu.VMEM((128, 128), F32),
    pltpu.VMEM((16, 256), F32),
    pltpu.VMEM((TP, 128), F32),
    pltpu.VMEM((UNITS, 128, 256), F32),
    pltpu.VMEM((UNITS, 128, 256), BF),
    pltpu.VMEM((CHUNKS, 2, 2, 4, 4, 8, CH), F32),
    pltpu.VMEM((CHUNKS, 2, 4, 4, 8, CH), F32),
    pltpu.VMEM((CHUNKS, 3, 4, 8, CH), F32),
    pltpu.VMEM((CHUNKS, 3, 4, 8, CH), F32),
    pltpu.VMEM((CHUNKS, 4, 8, CH), F32),
    pltpu.VMEM((CHUNKS, 4, 8, CH), F32),
    pltpu.VMEM((3, CHUNKS, 8, CH), F32),
    pltpu.VMEM((3, CHUNKS, 8, CH), F32),
    pltpu.VMEM((CHUNKS, 8, 2, CH), F32),
    pltpu.VMEM((7, CHUNKS, 2, CH), F32),
    pltpu.VMEM((5, 2, 8, CH), F32),
    pltpu.VMEM((15, 8, CH), F32),
    pltpu.SemaphoreType.DMA((120,)),
    pltpu.SemaphoreType.DMA((120,)),
]


OUT = (
    jax.ShapeDtypeStruct((24, 128), F32),
    jax.ShapeDtypeStruct((8, 128), F32),
    jax.ShapeDtypeStruct((16, 169), F32),
)


def step(*operands):
    vm = pl.BlockSpec(memory_space=pltpu.VMEM)
    hbm = pl.BlockSpec(memory_space=pl.ANY)
    return pl.pallas_call(
        kernel,
        name="step",
        out_shape=OUT,
        in_specs=[hbm, hbm, vm, vm, hbm, hbm, vm],
        out_specs=(vm, vm, vm),
        scratch_shapes=SCRATCH,
        compiler_params=pltpu.CompilerParams(
            collective_id=0, has_side_effects=True, vmem_limit_bytes=60 * 2**20
        ),
    )(*operands)


def apply(scale, *operands):
    vm = pl.BlockSpec(memory_space=pltpu.VMEM)
    return pl.pallas_call(
        functools.partial(apply_kernel, scale),
        name="apply",
        out_shape=OUT,
        in_specs=[vm] * 6,
        out_specs=(vm, vm, vm),
        compiler_params=pltpu.CompilerParams(vmem_limit_bytes=60 * 2**20),
    )(*operands)


def body(tokens, cotangent, regions, rel_index, w_qkv, w_proj, bias_table, mom_qkv, mom_proj, mom_table):
    win, count, dim = tokens.shape
    devices = lax.axis_size(("gx", "gy", "gz"))
    tok = jnp.transpose(tokens, (1, 0, 2)).reshape(count * win, dim)
    cot = jnp.transpose(cotangent, (1, 0, 2)).reshape(count * win, dim)
    sums = step(tok, cot, regions, rel_index, w_qkv, w_proj, bias_table.T)
    out_qkv, out_proj, out_tab = apply(
        1.0 / (win * devices), *sums, mom_qkv.reshape(24, 128), mom_proj.reshape(8, 128), mom_table.T
    )
    return out_qkv.reshape(-1), out_proj.reshape(-1), out_tab.T


def solution(mesh):
    rows = P(("gx", "gy", "gz"))
    wide = P(("gx", "gy", "gz"), None, None)
    return jax.shard_map(
        body,
        mesh=mesh,
        in_specs=(wide, wide, P(("gx", "gy", "gz"), None), P(), P(), P(), P(), rows, rows, P()),
        out_specs=(rows, rows, P()),
        check_vma=False,
    )
```

```python
import functools

import jax
import jax.numpy as jnp
from jax import lax
from jax.experimental import pallas as pl
from jax.experimental.pallas import tpu as pltpu
from jax.sharding import PartitionSpec as P

MESH = pl.DeviceIdType.MESH
BF = jnp.bfloat16
F32 = jnp.float32
WIN = 16
TOK = 49
SEG = 64
TP = 56
D = 512
HEAD_DIM = 32
SCALE = HEAD_DIM ** -0.5
UNITS = 4
STEPS = 4 * WIN // 2 // UNITS
GROUP = STEPS // 4
CH = 256
CHUNKS = 8


def nt(a, b):
    return lax.dot_general(a, b, (((1,), (1,)), ((), ())), preferred_element_type=F32)


def nn(a, b):
    return jnp.dot(a, b, preferred_element_type=F32)


def iota(shape, dim):
    return lax.broadcasted_iota(jnp.int32, shape, dim)


def onehot(condition):
    return condition.astype(F32).astype(BF)


def aligned(start, size, to=128):
    return pl.ds(pl.multiple_of(start, to), size)


def small_tables(reg, rel, tab_t, bias, mask, pad, tabp, relt):
    low = iota((TP, 128), 1) < SEG
    pad[...] = jnp.zeros_like(pad)
    pad[0:TOK, 0:TOK] = rel[...].astype(F32)
    flipped = pad[...].T
    both = flipped[0:TP] + pltpu.roll(flipped, SEG, 1)[0:TP]
    index = both.astype(jnp.int32)
    relt[...] = both
    pad[...] = jnp.zeros_like(pad)
    pad[0:WIN, 0:TOK] = reg[...].astype(F32)
    regions = pad[0:WIN, :]
    regions = regions + pltpu.roll(regions, SEG, 1)
    columns = pad[...].T[0:TP]
    for w in range(WIN):
        key = jnp.broadcast_to(columns[:, w : w + 1], (TP, 128))
        mask[w] = jnp.where(key == regions[w : w + 1], 0.0, -100.0).astype(F32)
    tabp[...] = jnp.zeros_like(tabp)
    tabp[:, 0:169] = tab_t[...]
    first = jnp.bitwise_and(index, 127)
    beyond = index >= 128
    real = iota((TP, 128), 0) < TOK

    def looked(h):
        lo = jnp.broadcast_to(tabp[h : h + 1, 0:128], (TP, 128))
        hi = jnp.broadcast_to(tabp[h : h + 1, 128:256], (TP, 128))
        lo = jnp.take_along_axis(lo, first, axis=1, mode="promise_in_bounds")
        hi = jnp.take_along_axis(hi, first, axis=1, mode="promise_in_bounds")
        return jnp.where(beyond, hi, lo)

    for k in range(8):
        value = jnp.where(low, looked(2 * k), looked(2 * k + 1))
        bias[k // 2, :, (k % 2) * 128 : (k % 2 + 1) * 128] = jnp.where(real, value, -1e30)


def gather_windows(src, dst):
    row, col = iota((256, 256), 0), iota((256, 256), 1)
    pick = onehot((row % 16) * 16 + row // 16 == col)
    for part in range(3):
        out = nn(pick, src[part * 256 : (part + 1) * 256, :]).astype(BF)
        dst[:, part * 16 : (part + 1) * 16, :] = out.reshape(WIN, 16, D)
    out = nn(pick[:, 0:16], src[768:784, :]).astype(BF)
    dst[:, 48:64, :] = out.reshape(WIN, 16, D)


def project(wqkv, wproj, xp, cp, qkv, kvt, da, xpt):
    eye = onehot(iota((128, 128), 0) == iota((128, 128), 1))
    s = iota((128, 128), 0)
    wanted = (
        (s // 32) * 32
        + ((s // 4) % 2) * 16
        + ((s // 2) % 2) * 8
        + ((s // 8) % 2) * 4
        + ((s // 16) % 2) * 2
        + s % 2
    )
    strips = onehot(wanted == iota((128, 128), 1))

    def four_windows(c, carry):
        rows = aligned(c * 256, 256, 256)
        x = xp[pl.ds(c * 4, 4)].reshape(256, D)
        y = cp[pl.ds(c * 4, 4)].reshape(256, D)
        values = nn(x, wqkv[...]).astype(BF)
        qkv[rows, :] = values
        da[rows, :] = nt(y, wproj[...]).astype(BF)
        for b in range(4):
            xpt[b * 128 : (b + 1) * 128, rows] = nt(strips, x[:, b * 128 : (b + 1) * 128]).astype(BF)
            k = values[:, 512 + b * 128 : 512 + (b + 1) * 128]
            kvt[b * 128 : (b + 1) * 128, rows] = nt(eye, k).astype(BF)
            v = values[:, 1024 + b * 128 : 1024 + (b + 1) * 128]
            kvt[512 + b * 128 : 512 + (b + 1) * 128, rows] = nt(strips, v).astype(BF)
        return carry

    lax.fori_loop(0, 4, four_windows, 0)


class Attention:
    def __init__(self, qkv, kvt, da, bias, mask, keep, dk, dv, dqt, at, gb, raw, wide, grads):
        self.qkv, self.kvt, self.da, self.bias, self.mask = qkv, kvt, da, bias, mask
        self.keep, self.dk, self.dv, self.dqt, self.at = keep, dk, dv, dqt, at
        self.gb, self.raw, self.wide, self.grads = gb, raw, wide, grads
        lane = iota((SEG, 256), 1) % 128
        self.heads = [onehot(lane // HEAD_DIM == h) for h in range(4)]
        self.zero = jnp.zeros((SEG, 128), BF)
        self.tail = jnp.zeros((SEG - TP, 256), F32)
        half = iota((128, 128), 1)
        self.left = onehot(half < SEG)
        self.right = onehot(half >= SEG)
        self.low = iota((32, 128), 1) < SEG

    def spread(self, a):
        a = jnp.concatenate([a[0:SEG], a[SEG:]], axis=1)
        return jnp.concatenate([a * head for head in self.heads], axis=0)

    def diagonal(self, a):
        upper = jnp.concatenate([a[0:SEG], self.zero], axis=1)
        lower = jnp.concatenate([self.zero, a[SEG:]], axis=1)
        return jnp.concatenate([upper, lower], axis=0)

    def stack(self, a, b):
        return jnp.concatenate([a, self.tail, b, self.tail], axis=0).astype(BF)

    def own(self, dst, pair, g, value):
        dst[aligned(pair * 128, SEG), aligned(g * 128, 128)] = value[0:SEG, 0:128].astype(BF)
        dst[aligned(pair * 128 + SEG, SEG, SEG), aligned(g * 128, 128)] = value[SEG:, 128:256].astype(BF)

    def across(self, dst, pair, g, turned, wide):
        lhs = jnp.concatenate([turned * self.left, turned * self.right], axis=0)
        full = nn(lhs, wide)
        for h in range(4):
            lanes = slice((h // 2) * 128, (h // 2 + 1) * 128)
            one = full[32 * h : 32 * h + 32, lanes]
            two = full[128 + 32 * h : 128 + 32 * h + 32, lanes]
            if h % 2:
                one = pltpu.roll(one, SEG, 1)
            else:
                two = pltpu.roll(two, SEG, 1)
            value = jnp.where(self.low, one, two).astype(BF)
            dst[aligned(g * 128 + 32 * h, 32, 32), aligned(pair * 128, 128)] = value

    def place(self, unit):
        return unit // (WIN // 2), unit % (WIN // 2)

    def forward1(self, u, unit):
        g, pair = self.place(unit)
        rows = aligned(pair * 128, 128)
        q_wide = self.spread(self.qkv[rows, aligned(g * 128, 128)])
        self.raw[u] = nt(self.diagonal(self.qkv[rows, aligned(512 + g * 128, 128)]), q_wide)

    def forward2(self, u, unit):
        g, pair = self.place(unit)
        probs = []
        for i in range(2):
            scores = self.raw[u, i * SEG : i * SEG + TP, :] * SCALE + self.bias[g]
            scores = scores + jnp.concatenate([self.mask[2 * pair + i]] * 2, axis=1)
            e = jnp.exp(scores - jnp.max(scores, axis=0, keepdims=True))
            p = e * (1.0 / jnp.sum(e, axis=0, keepdims=True))
            self.keep[2 * unit + i] = p
            probs.append(p)
        self.wide[u] = self.stack(*probs)

    def forward3(self, u, unit):
        g, pair = self.place(unit)
        rows = aligned(pair * 128, 128)
        probs = self.wide[u]
        da_wide = self.spread(self.da[rows, aligned(g * 128, 128)])
        self.own(self.dv, pair, g, nn(probs, da_wide))
        self.across(self.at, pair, g, self.kvt[aligned(512 + g * 128, 128), rows], probs)

    def backward1(self, u, unit):
        g, pair = self.place(unit)
        rows = aligned(pair * 128, 128)
        da_wide = self.spread(self.da[rows, aligned(g * 128, 128)])
        self.raw[u] = nt(self.diagonal(self.qkv[rows, aligned(1024 + g * 128, 128)]), da_wide)

    def backward2(self, u, unit):
        g, pair = self.place(unit)
        parts = []
        for i in range(2):
            p = self.keep[2 * unit + i]
            dp = self.raw[u, i * SEG : i * SEG + TP, :]
            parts.append(p * (dp - jnp.sum(p * dp, axis=0, keepdims=True)))
        total = parts[0] + parts[1]
        for k in range(2):
            block = aligned((2 * g + k) * TP, TP, 8)
            self.gb[block, :] = self.gb[block, :] + total[:, k * 128 : (k + 1) * 128]
        self.grads[unit] = self.stack(parts[0] * SCALE, parts[1] * SCALE)

    def backward_k(self, u, unit):
        g, pair = self.place(unit)
        rows = aligned(pair * 128, 128)
        q_wide = self.spread(self.qkv[rows, aligned(g * 128, 128)])
        self.own(self.dk, pair, g, nn(self.grads[unit], q_wide))

    def backward_q(self, u, unit):
        g, pair = self.place(unit)
        rows = aligned(pair * 128, 128)
        self.across(self.dqt, pair, g, self.kvt[aligned(g * 128, 128), rows], self.grads[unit])

    def stages(self, stages, t, which):
        for n in reversed(which):
            for u in range(UNITS):
                stages[n](u, (t - n) * UNITS + u)

    def run(self, stages, lo, hi):
        ahead = len(stages) - 1
        whole = tuple(range(len(stages)))
        if lo == 0:
            for t in range(ahead):
                self.stages(stages, t, whole[: t + 1])
        end = STEPS if hi == STEPS else hi + ahead

        def one(t, carry):
            self.stages(stages, t, whole)
            return carry

        lax.fori_loop(lo + ahead, end, one, 0)
        if hi == STEPS:
            for t in range(ahead):
                self.stages(stages, STEPS + t, whole[t + 1 :])


def table_gradient(gb, relt):
    low = iota((8, 128), 1) < SEG
    entry = iota((256, 128), 0).astype(F32)
    total = jnp.zeros((32, 256), F32)

    def line(j):
        if j >= TOK:
            return jnp.zeros((32, 128), BF), jnp.zeros((256, 128), BF)
        hot = onehot(entry == jnp.broadcast_to(relt[j : j + 1, :], (256, 128)))
        pairs = gb[pl.ds(j, 8, stride=TP), :]
        split = jnp.concatenate([jnp.where(low, pairs, 0.0), jnp.where(low, 0.0, pairs)], axis=0)
        upper = split.astype(BF)
        lower = (split - upper.astype(F32)).astype(BF)
        return jnp.concatenate([upper, lower], axis=0), hot

    for j in range(0, TOK, 2):
        a, b = line(j), line(j + 1)
        total = total + nt(
            jnp.concatenate([a[0], b[0]], axis=1), jnp.concatenate([a[1], b[1]], axis=1)
        )
    return total[0:16] + total[16:32]


class Exchange:
    def __init__(self, g, s1, ra, rb, a2, b2, ra2, rb2, zs, rz, tt, tr, send, recv):
        self.g, self.s1, self.ra, self.rb, self.a2, self.b2 = g, s1, ra, rb, a2, b2
        self.ra2, self.rb2, self.zs, self.rz, self.tt, self.tr = ra2, rb2, zs, rz, tt, tr
        self.send, self.recv, self.used = send, recv, 0
        gx, gy, gz = lax.axis_index("gx"), lax.axis_index("gy"), lax.axis_index("gz")
        x, z, core = lax.rem(gx, 4), gy, lax.rem(gz, 2)
        y = (gx // 4) * 2 + gz // 2

        def device(x, y, z, core):
            return ((y // 2) * 4 + x, z, lax.rem(y, 2) * 2 + core)

        def xor(a, b):
            out = 0
            for bit in (1, 2, 4):
                have = lax.rem(a // bit, 2)
                out = out + bit * ((1 - have) if b & bit else have)
            return out

        self.x, self.y, self.z, self.core = x, y, z, core
        self.partner = device(x, y, z, 1 - core)
        self.along_x = [(xor(x, d), device(xor(x, d), y, z, core)) for d in (1, 2, 3)]
        self.along_y = [(xor(y, d), device(x, xor(y, d), z, core)) for d in (1, 2, 3)]
        self.along_z = [(xor(z, d), device(x, y, xor(z, d), core)) for d in range(1, 8)]
        self.flight = {}

    def greet(self):
        self.peers = [self.partner] + [dev for _, dev in self.along_x + self.along_y + self.along_z]
        barrier = pltpu.get_barrier_semaphore()
        for peer in self.peers:
            pl.semaphore_signal(barrier, inc=1, device_id=peer, device_id_type=MESH)

    def greeted(self):
        pl.semaphore_wait(pltpu.get_barrier_semaphore(), len(self.peers))

    def start(self, key, src, dst, dev):
        n = self.used
        self.used += 1
        c = pltpu.make_async_remote_copy(
            src_ref=src, dst_ref=dst, send_sem=self.send.at[n], recv_sem=self.recv.at[n],
            device_id=dev, device_id_type=MESH,
        )
        c.start()
        self.flight.setdefault(key, []).append(c)

    def finish(self, key):
        for c in self.flight.pop(key):
            c.wait()

    def put(self, c, lo, value):
        lanes = slice(lo, lo + value.shape[1])
        for strip in range(16):
            y1, x, z2 = strip // 8, (strip // 2) % 4, strip % 2
            for core in range(2):
                for y0 in range(2):
                    r = strip * 32 + core * 16 + y0 * 8
                    self.g[c, core, z2, y1 * 2 + y0, x, :, lanes] = value[r : r + 8]

    def cores(self, c):
        self.start(("p0", c), self.g.at[c, 1 - self.core], self.s1.at[c], self.partner)

    def first(self, c):
        self.finish(("p0", c))
        for half in range(2):
            self.s1[c, half] = self.s1[c, half] + self.g[c, self.core, half]
        for n, (to, dev) in enumerate(self.along_x):
            self.start(("p1", c), self.s1.at[c, 0, :, to], self.ra.at[c, n], dev)
        for n, (to, dev) in enumerate(self.along_y):
            self.start(("p1", c), self.s1.at[c, 1, to], self.rb.at[c, n], dev)

    def second(self, lo, hi):
        for c in range(lo, hi):
            self.finish(("p1", c))
            self.a2[c] = self.s1[c, 0, :, self.x] + self.ra[c, 0] + self.ra[c, 1] + self.ra[c, 2]
            self.b2[c] = self.s1[c, 1, self.y] + self.rb[c, 0] + self.rb[c, 1] + self.rb[c, 2]
        span = pl.ds(lo, hi - lo)
        for n, (to, dev) in enumerate(self.along_y):
            self.start(("p2", lo), self.a2.at[span, to], self.ra2.at[n, span], dev)
        for n, (to, dev) in enumerate(self.along_x):
            self.start(("p2", lo), self.b2.at[span, to], self.rb2.at[n, span], dev)

    def third(self, lo, hi):
        self.finish(("p2", lo))
        for c in range(lo, hi):
            a = self.a2[c, self.y] + self.ra2[0, c] + self.ra2[1, c] + self.ra2[2, c]
            b = self.b2[c, self.x] + self.rb2[0, c] + self.rb2[1, c] + self.rb2[2, c]
            for k in range(4):
                self.zs[c, k] = a[2 * k : 2 * k + 2]
                self.zs[c, 4 + k] = b[2 * k : 2 * k + 2]
        span = pl.ds(lo, hi - lo)
        for n, (to, dev) in enumerate(self.along_z):
            self.start(("p3", lo), self.zs.at[span, to], self.rz.at[n, span], dev)

    def last(self, lo, hi):
        self.finish(("p3", lo))
        out = []
        for c in range(lo, hi):
            mine = self.zs[c, self.z]
            for n in range(7):
                mine = mine + self.rz[n, c]
            out.append(mine)
        return out

    def table_cores(self, value):
        self.tt[0, 0] = value[0:8]
        self.tt[0, 1] = value[8:16]
        self.start("t0", self.tt.at[0, 1 - self.core], self.tr.at[0], self.partner)

    def table_axis(self, key, stage, first, count, own, peers):
        total = own
        if key is not None:
            self.finish(key)
            for n in range(count):
                total = total + self.tr[first + n]
        self.tt[stage, 0] = total
        for n, (_, dev) in enumerate(peers):
            self.start("t%d" % stage, self.tt.at[stage, 0], self.tr.at[first + count + n], dev)


def kernel(*refs):
    refs = list(refs)

    def take(n):
        out = refs[:n]
        del refs[:n]
        return out

    tok_hbm, cot_hbm, reg, rel, wqkv_hbm, wproj_hbm, tab_t = take(7)
    out_qkv, out_proj, out_tab = take(3)
    tok, cot, wqkv, wproj, fetched = take(5)
    xp, cp, qkv, kvt, da, xpt = take(6)
    bias, mask, keep, dk, dv, dqt, at, gb, pad, tabp, relt, raw, wide, grads = take(14)
    ex = Exchange(*refs)

    fetches = []
    for n, (src, dst) in enumerate(((tok_hbm, tok), (cot_hbm, cot), (wqkv_hbm, wqkv), (wproj_hbm, wproj))):
        fetch = pltpu.make_async_copy(src, dst, fetched.at[n])
        fetch.start()
        fetches.append(fetch)
    ex.greet()
    small_tables(reg, rel, tab_t, bias, mask, pad, tabp, relt)
    gb[...] = jnp.zeros_like(gb)
    fetches[0].wait()
    gather_windows(tok, xp)
    fetches[1].wait()
    gather_windows(cot, cp)
    fetches[2].wait()
    fetches[3].wait()
    project(wqkv, wproj, xp, cp, qkv, kvt, da, xpt)

    att = Attention(qkv, kvt, da, bias, mask, keep, dk, dv, dqt, at, gb, raw, wide, grads)
    forward = att.forward1, att.forward2, att.forward3
    backward = att.backward1, att.backward2

    def v_chunk(c):
        ex.put(c, 0, nn(xpt[...], dv[:, c * 256 : (c + 1) * 256]))
        ex.cores(c)

    def proj_chunk(c):
        y = cp[:, :, c * 256 : (c + 1) * 256].reshape(WIN * SEG, 256)
        ex.put(2 + c, 0, nn(at[...], y))
        ex.cores(2 + c)

    def k_chunk(c):
        ex.put(4 + 2 * c, 0, nn(xpt[...], dk[:, c * 256 : (c + 1) * 256]))
        ex.cores(4 + 2 * c)

    def q_chunk(c):
        ex.put(5 + 2 * c, 0, nt(xpt[...], dqt[c * 256 : (c + 1) * 256, :]))
        ex.cores(5 + 2 * c)

    half = 2 * GROUP
    att.run(forward, 0, half)
    ex.greeted()
    v_chunk(0)
    att.run(forward, half, STEPS)
    ex.first(0)
    v_chunk(1)
    proj_chunk(0)
    ex.first(1)
    proj_chunk(1)
    ex.first(2)
    att.run(backward, 0, half)
    ex.first(3)
    att.run((att.backward_k,), 0, half)
    k_chunk(0)
    att.run((att.backward_q,), 0, half)
    ex.first(4)
    q_chunk(0)
    ex.second(0, 4)
    att.run(backward, half, STEPS)
    ex.first(5)
    att.run((att.backward_k,), half, STEPS)
    k_chunk(1)
    ex.table_cores(table_gradient(gb, relt))
    ex.first(6)
    ex.third(0, 4)
    att.run((att.backward_q,), half, STEPS)
    own = ex.tt[0, ex.core]
    ex.finish("t0")
    ex.table_axis(None, 1, 0, 1, own + ex.tr[0], ex.along_x)
    q_chunk(1)
    ex.second(4, 6)
    ex.table_axis("t1", 2, 1, 3, ex.tt[1, 0], ex.along_y)
    ex.first(7)
    ex.third(4, 6)
    ex.table_axis("t2", 3, 4, 3, ex.tt[2, 0], ex.along_z)
    ex.second(6, 8)
    ex.third(6, 8)

    def finish(lo, hi):
        for c, mine in zip(range(lo, hi), ex.last(lo, hi)):
            for r in range(2):
                for part in range(2):
                    value = mine[r : r + 1, part * 128 : (part + 1) * 128]
                    if 2 <= c < 4:
                        k = r * 4 + (c - 2) * 2 + part
                        out_proj[k : k + 1, :] = value
                    else:
                        col = (8, 10, 0, 0, 4, 0, 6, 2)[c] + part
                        k = r * 12 + col
                        out_qkv[k : k + 1, :] = value

    finish(0, 4)
    finish(4, 6)
    finish(6, 8)
    ex.finish("t3")
    table = ex.tt[3, 0]
    for n in range(7):
        table = table + ex.tr[7 + n]
    ex.tt[4, 0] = table
    ex.start("t4", ex.tt.at[4, 0], ex.tr.at[14], ex.partner)
    ex.finish("t4")
    core = ex.core.astype(F32)
    other = ex.tr[14]
    even = table * (1.0 - core) + other * core
    odd = table * core + other * (1.0 - core)
    for k in range(8):
        out_tab[2 * k : 2 * k + 1, :] = even[k : k + 1, 0:169]
        out_tab[2 * k + 1 : 2 * k + 2, :] = odd[k : k + 1, 0:169]


def apply_kernel(scale, *refs):
    for total, momentum, out in zip(refs[0:3], refs[3:6], refs[6:9]):
        out[...] = 0.9 * momentum[...] + total[...] * scale


SCRATCH = [
    pltpu.VMEM((784, D), BF),
    pltpu.VMEM((784, D), BF),
    pltpu.VMEM((D, 3 * D), BF),
    pltpu.VMEM((D, D), BF),
    pltpu.SemaphoreType.DMA((4,)),
    pltpu.VMEM((WIN, SEG, D), BF),
    pltpu.VMEM((WIN, SEG, D), BF),
    pltpu.VMEM((1024, 3 * D), BF),
    pltpu.VMEM((1024, 1024), BF),
    pltpu.VMEM((1024, D), BF),
    pltpu.VMEM((D, 1024), BF),
    pltpu.VMEM((4, TP, 256), F32),
    pltpu.VMEM((WIN, TP, 128), F32),
    pltpu.VMEM((4 * WIN, TP, 256), F32),
    pltpu.VMEM((1024, D), BF),
    pltpu.VMEM((1024, D), BF),
    pltpu.VMEM((D, 1024), BF),
    pltpu.VMEM((D, 1024), BF),
    pltpu.VMEM((8 * TP, 128), F32),
    pltpu.VMEM((128, 128), F32),
    pltpu.VMEM((16, 256), F32),
    pltpu.VMEM((TP, 128), F32),
    pltpu.VMEM((UNITS, 128, 256), F32),
    pltpu.VMEM((UNITS, 128, 256), BF),
    pltpu.VMEM((2 * WIN, 128, 256), BF),
    pltpu.VMEM((CHUNKS, 2, 2, 4, 4, 8, CH), F32),
    pltpu.VMEM((CHUNKS, 2, 4, 4, 8, CH), F32),
    pltpu.VMEM((CHUNKS, 3, 4, 8, CH), F32),
    pltpu.VMEM((CHUNKS, 3, 4, 8, CH), F32),
    pltpu.VMEM((CHUNKS, 4, 8, CH), F32),
    pltpu.VMEM((CHUNKS, 4, 8, CH), F32),
    pltpu.VMEM((3, CHUNKS, 8, CH), F32),
    pltpu.VMEM((3, CHUNKS, 8, CH), F32),
    pltpu.VMEM((CHUNKS, 8, 2, CH), F32),
    pltpu.VMEM((7, CHUNKS, 2, CH), F32),
    pltpu.VMEM((5, 2, 8, CH), F32),
    pltpu.VMEM((15, 8, CH), F32),
    pltpu.SemaphoreType.DMA((120,)),
    pltpu.SemaphoreType.DMA((120,)),
]


OUT = (
    jax.ShapeDtypeStruct((24, 128), F32),
    jax.ShapeDtypeStruct((8, 128), F32),
    jax.ShapeDtypeStruct((16, 169), F32),
)


def step(*operands):
    vm = pl.BlockSpec(memory_space=pltpu.VMEM)
    hbm = pl.BlockSpec(memory_space=pl.ANY)
    return pl.pallas_call(
        kernel,
        name="step",
        out_shape=OUT,
        in_specs=[hbm, hbm, vm, vm, hbm, hbm, vm],
        out_specs=(vm, vm, vm),
        scratch_shapes=SCRATCH,
        compiler_params=pltpu.CompilerParams(
            collective_id=0, has_side_effects=True, vmem_limit_bytes=60 * 2**20
        ),
    )(*operands)


def apply(scale, *operands):
    vm = pl.BlockSpec(memory_space=pltpu.VMEM)
    return pl.pallas_call(
        functools.partial(apply_kernel, scale),
        name="apply",
        out_shape=OUT,
        in_specs=[vm] * 6,
        out_specs=(vm, vm, vm),
        compiler_params=pltpu.CompilerParams(vmem_limit_bytes=60 * 2**20),
    )(*operands)


def body(tokens, cotangent, regions, rel_index, w_qkv, w_proj, bias_table, mom_qkv, mom_proj, mom_table):
    win, count, dim = tokens.shape
    devices = lax.axis_size(("gx", "gy", "gz"))
    tok = jnp.transpose(tokens, (1, 0, 2)).reshape(count * win, dim)
    cot = jnp.transpose(cotangent, (1, 0, 2)).reshape(count * win, dim)
    sums = step(tok, cot, regions, rel_index, w_qkv, w_proj, bias_table.T)
    out_qkv, out_proj, out_tab = apply(
        1.0 / (win * devices), *sums, mom_qkv.reshape(24, 128), mom_proj.reshape(8, 128), mom_table.T
    )
    return out_qkv.reshape(-1), out_proj.reshape(-1), out_tab.T


def solution(mesh):
    rows = P(("gx", "gy", "gz"))
    wide = P(("gx", "gy", "gz"), None, None)
    return jax.shard_map(
        body,
        mesh=mesh,
        in_specs=(wide, wide, P(("gx", "gy", "gz"), None), P(), P(), P(), P(), rows, rows, P()),
        out_specs=(rows, rows, P()),
        check_vma=False,
    )
```

```python
import functools

import jax
import jax.numpy as jnp
from jax import lax
from jax.experimental import pallas as pl
from jax.experimental.pallas import tpu as pltpu
from jax.sharding import PartitionSpec as P

MESH = pl.DeviceIdType.MESH
BF = jnp.bfloat16
F32 = jnp.float32
WIN = 16
TOK = 49
SEG = 64
TP = 56
D = 512
HEAD_DIM = 32
SCALE = HEAD_DIM ** -0.5
UNITS = 4
STEPS = 4 * WIN // 2 // UNITS
GROUP = STEPS // 4
CH = 256
CHUNKS = 8


def nt(a, b):
    return lax.dot_general(a, b, (((1,), (1,)), ((), ())), preferred_element_type=F32)


def nn(a, b):
    return jnp.dot(a, b, preferred_element_type=F32)


def iota(shape, dim):
    return lax.broadcasted_iota(jnp.int32, shape, dim)


def onehot(condition):
    return condition.astype(F32).astype(BF)


def aligned(start, size, to=128):
    return pl.ds(pl.multiple_of(start, to), size)


def small_tables(reg, rel, tab_t, bias, mask, pad, tabp, relt):
    low = iota((TP, 128), 1) < SEG
    pad[...] = jnp.zeros_like(pad)
    pad[0:TOK, 0:TOK] = rel[...].astype(F32)
    flipped = pad[...].T
    both = flipped[0:TP] + pltpu.roll(flipped, SEG, 1)[0:TP]
    index = both.astype(jnp.int32)
    relt[...] = both
    pad[...] = jnp.zeros_like(pad)
    pad[0:WIN, 0:TOK] = reg[...].astype(F32)
    regions = pad[0:WIN, :]
    regions = regions + pltpu.roll(regions, SEG, 1)
    columns = pad[...].T[0:TP]
    for w in range(WIN):
        key = jnp.broadcast_to(columns[:, w : w + 1], (TP, 128))
        mask[w] = jnp.where(key == regions[w : w + 1], 0.0, -100.0).astype(F32)
    tabp[...] = jnp.zeros_like(tabp)
    tabp[:, 0:169] = tab_t[...]
    first = jnp.bitwise_and(index, 127)
    beyond = index >= 128
    real = iota((TP, 128), 0) < TOK

    def looked(h):
        lo = jnp.broadcast_to(tabp[h : h + 1, 0:128], (TP, 128))
        hi = jnp.broadcast_to(tabp[h : h + 1, 128:256], (TP, 128))
        lo = jnp.take_along_axis(lo, first, axis=1, mode="promise_in_bounds")
        hi = jnp.take_along_axis(hi, first, axis=1, mode="promise_in_bounds")
        return jnp.where(beyond, hi, lo)

    for k in range(8):
        value = jnp.where(low, looked(2 * k), looked(2 * k + 1))
        bias[k // 2, :, (k % 2) * 128 : (k % 2 + 1) * 128] = jnp.where(real, value, -1e30)


def gather_windows(src, dst):
    row, col = iota((256, 256), 0), iota((256, 256), 1)
    pick = onehot((row % 16) * 16 + row // 16 == col)
    for part in range(3):
        out = nn(pick, src[part * 256 : (part + 1) * 256, :]).astype(BF)
        dst[:, part * 16 : (part + 1) * 16, :] = out.reshape(WIN, 16, D)
    out = nn(pick[:, 0:16], src[768:784, :]).astype(BF)
    dst[:, 48:64, :] = out.reshape(WIN, 16, D)


def project(wqkv, wproj, xp, cp, qkv, kvt, da, xpt):
    eye = onehot(iota((128, 128), 0) == iota((128, 128), 1))
    s = iota((128, 128), 0)
    wanted = (
        (s // 32) * 32
        + ((s // 4) % 2) * 16
        + ((s // 2) % 2) * 8
        + ((s // 8) % 2) * 4
        + ((s // 16) % 2) * 2
        + s % 2
    )
    strips = onehot(wanted == iota((128, 128), 1))

    def four_windows(c, carry):
        rows = aligned(c * 256, 256, 256)
        x = xp[pl.ds(c * 4, 4)].reshape(256, D)
        y = cp[pl.ds(c * 4, 4)].reshape(256, D)
        values = nn(x, wqkv[...]).astype(BF)
        qkv[rows, :] = values
        da[rows, :] = nt(y, wproj[...]).astype(BF)
        for b in range(4):
            xpt[b * 128 : (b + 1) * 128, rows] = nt(strips, x[:, b * 128 : (b + 1) * 128]).astype(BF)
            k = values[:, 512 + b * 128 : 512 + (b + 1) * 128]
            kvt[b * 128 : (b + 1) * 128, rows] = nt(eye, k).astype(BF)
            v = values[:, 1024 + b * 128 : 1024 + (b + 1) * 128]
            kvt[512 + b * 128 : 512 + (b + 1) * 128, rows] = nt(strips, v).astype(BF)
        return carry

    lax.fori_loop(0, 4, four_windows, 0)


class Attention:
    def __init__(self, qkv, kvt, da, bias, mask, keep, dk, dv, dqt, at, gb, raw, wide, grads):
        self.qkv, self.kvt, self.da, self.bias, self.mask = qkv, kvt, da, bias, mask
        self.keep, self.dk, self.dv, self.dqt, self.at = keep, dk, dv, dqt, at
        self.gb, self.raw, self.wide, self.grads = gb, raw, wide, grads
        lane = iota((SEG, 256), 1) % 128
        self.heads = [onehot(lane // HEAD_DIM == h) for h in range(4)]
        self.zero = jnp.zeros((SEG, 128), BF)
        self.tail = jnp.zeros((SEG - TP, 256), F32)
        half = iota((128, 128), 1)
        self.left = onehot(half < SEG)
        self.right = onehot(half >= SEG)
        self.low = iota((32, 128), 1) < SEG

    def spread(self, a):
        a = jnp.concatenate([a[0:SEG], a[SEG:]], axis=1)
        return jnp.concatenate([a * head for head in self.heads], axis=0)

    def diagonal(self, a):
        upper = jnp.concatenate([a[0:SEG], self.zero], axis=1)
        lower = jnp.concatenate([self.zero, a[SEG:]], axis=1)
        return jnp.concatenate([upper, lower], axis=0)

    def stack(self, a, b):
        return jnp.concatenate([a, self.tail, b, self.tail], axis=0).astype(BF)

    def own(self, dst, pair, g, value):
        dst[aligned(pair * 128, SEG), aligned(g * 128, 128)] = value[0:SEG, 0:128].astype(BF)
        dst[aligned(pair * 128 + SEG, SEG, SEG), aligned(g * 128, 128)] = value[SEG:, 128:256].astype(BF)

    def across(self, dst, pair, g, turned, wide):
        lhs = jnp.concatenate([turned * self.left, turned * self.right], axis=0)
        full = nn(lhs, wide)
        for h in range(4):
            lanes = slice((h // 2) * 128, (h // 2 + 1) * 128)
            one = full[32 * h : 32 * h + 32, lanes]
            two = full[128 + 32 * h : 128 + 32 * h + 32, lanes]
            if h % 2:
                one = pltpu.roll(one, SEG, 1)
            else:
                two = pltpu.roll(two, SEG, 1)
            value = jnp.where(self.low, one, two).astype(BF)
            dst[aligned(g * 128 + 32 * h, 32, 32), aligned(pair * 128, 128)] = value

    def place(self, unit):
        return unit // (WIN // 2), unit % (WIN // 2)

    def forward1(self, u, unit):
        g, pair = self.place(unit)
        rows = aligned(pair * 128, 128)
        q_wide = self.spread(self.qkv[rows, aligned(g * 128, 128)])
        self.raw[u] = nt(self.diagonal(self.qkv[rows, aligned(512 + g * 128, 128)]), q_wide)

    def forward2(self, u, unit):
        g, pair = self.place(unit)
        probs = []
        for i in range(2):
            scores = self.raw[u, i * SEG : i * SEG + TP, :] * SCALE + self.bias[g]
            scores = scores + jnp.concatenate([self.mask[2 * pair + i]] * 2, axis=1)
            e = jnp.exp(scores - jnp.max(scores, axis=0, keepdims=True))
            p = e * (1.0 / jnp.sum(e, axis=0, keepdims=True))
            self.keep[2 * unit + i] = p
            probs.append(p)
        self.wide[u] = self.stack(*probs)

    def forward3(self, u, unit):
        g, pair = self.place(unit)
        rows = aligned(pair * 128, 128)
        probs = self.wide[u]
        da_wide = self.spread(self.da[rows, aligned(g * 128, 128)])
        self.own(self.dv, pair, g, nn(probs, da_wide))
        self.across(self.at, pair, g, self.kvt[aligned(512 + g * 128, 128), rows], probs)

    def backward1(self, u, unit):
        g, pair = self.place(unit)
        rows = aligned(pair * 128, 128)
        da_wide = self.spread(self.da[rows, aligned(g * 128, 128)])
        self.raw[u] = nt(self.diagonal(self.qkv[rows, aligned(1024 + g * 128, 128)]), da_wide)

    def backward2(self, u, unit):
        g, pair = self.place(unit)
        parts = []
        for i in range(2):
            p = self.keep[2 * unit + i]
            dp = self.raw[u, i * SEG : i * SEG + TP, :]
            parts.append(p * (dp - jnp.sum(p * dp, axis=0, keepdims=True)))
        total = parts[0] + parts[1]
        for k in range(2):
            block = aligned((2 * g + k) * TP, TP, 8)
            self.gb[block, :] = self.gb[block, :] + total[:, k * 128 : (k + 1) * 128]
        self.grads[unit] = self.stack(parts[0] * SCALE, parts[1] * SCALE)

    def backward_k(self, u, unit):
        g, pair = self.place(unit)
        rows = aligned(pair * 128, 128)
        q_wide = self.spread(self.qkv[rows, aligned(g * 128, 128)])
        self.own(self.dk, pair, g, nn(self.grads[unit], q_wide))

    def backward_q(self, u, unit):
        g, pair = self.place(unit)
        rows = aligned(pair * 128, 128)
        self.across(self.dqt, pair, g, self.kvt[aligned(g * 128, 128), rows], self.grads[unit])

    def stages(self, stages, t, which):
        for n in reversed(which):
            for u in range(UNITS):
                stages[n](u, (t - n) * UNITS + u)

    def run(self, stages, lo, hi):
        ahead = len(stages) - 1
        whole = tuple(range(len(stages)))
        if lo == 0:
            for t in range(ahead):
                self.stages(stages, t, whole[: t + 1])
        end = STEPS if hi == STEPS else hi + ahead

        def one(t, carry):
            self.stages(stages, t, whole)
            return carry

        lax.fori_loop(lo + ahead, end, one, 0)
        if hi == STEPS:
            for t in range(ahead):
                self.stages(stages, STEPS + t, whole[t + 1 :])


def table_gradient(gb, relt):
    low = iota((8, 128), 1) < SEG
    entry = iota((256, 128), 0).astype(F32)
    total = jnp.zeros((32, 256), F32)

    def line(j):
        if j >= TOK:
            return jnp.zeros((32, 128), BF), jnp.zeros((256, 128), BF)
        hot = onehot(entry == jnp.broadcast_to(relt[j : j + 1, :], (256, 128)))
        pairs = gb[pl.ds(j, 8, stride=TP), :]
        split = jnp.concatenate([jnp.where(low, pairs, 0.0), jnp.where(low, 0.0, pairs)], axis=0)
        upper = split.astype(BF)
        lower = (split - upper.astype(F32)).astype(BF)
        return jnp.concatenate([upper, lower], axis=0), hot

    for j in range(0, TOK, 2):
        a, b = line(j), line(j + 1)
        total = total + nt(
            jnp.concatenate([a[0], b[0]], axis=1), jnp.concatenate([a[1], b[1]], axis=1)
        )
    return total[0:16] + total[16:32]


class Exchange:
    def __init__(self, g, s1, ra, rb, a2, b2, ra2, rb2, zs, rz, tt, tr, send, recv):
        self.g, self.s1, self.ra, self.rb, self.a2, self.b2 = g, s1, ra, rb, a2, b2
        self.ra2, self.rb2, self.zs, self.rz, self.tt, self.tr = ra2, rb2, zs, rz, tt, tr
        self.send, self.recv, self.used = send, recv, 0
        gx, gy, gz = lax.axis_index("gx"), lax.axis_index("gy"), lax.axis_index("gz")
        x, z, core = lax.rem(gx, 4), gy, lax.rem(gz, 2)
        y = (gx // 4) * 2 + gz // 2

        def device(x, y, z, core):
            return ((y // 2) * 4 + x, z, lax.rem(y, 2) * 2 + core)

        def xor(a, b):
            out = 0
            for bit in (1, 2, 4):
                have = lax.rem(a // bit, 2)
                out = out + bit * ((1 - have) if b & bit else have)
            return out

        self.x, self.y, self.z, self.core = x, y, z, core
        self.partner = device(x, y, z, 1 - core)
        self.along_x = [(xor(x, d), device(xor(x, d), y, z, core)) for d in (1, 2, 3)]
        self.along_y = [(xor(y, d), device(x, xor(y, d), z, core)) for d in (1, 2, 3)]
        self.along_z = [(xor(z, d), device(x, y, xor(z, d), core)) for d in range(1, 8)]
        self.flight = {}

    def greet(self):
        self.peers = [self.partner] + [dev for _, dev in self.along_x + self.along_y + self.along_z]
        barrier = pltpu.get_barrier_semaphore()
        for peer in self.peers:
            pl.semaphore_signal(barrier, inc=1, device_id=peer, device_id_type=MESH)

    def greeted(self):
        pl.semaphore_wait(pltpu.get_barrier_semaphore(), len(self.peers))

    def start(self, key, src, dst, dev):
        n = self.used
        self.used += 1
        c = pltpu.make_async_remote_copy(
            src_ref=src, dst_ref=dst, send_sem=self.send.at[n], recv_sem=self.recv.at[n],
            device_id=dev, device_id_type=MESH,
        )
        c.start()
        self.flight.setdefault(key, []).append(c)

    def finish(self, key):
        for c in self.flight.pop(key):
            c.wait()

    def put(self, c, lo, value):
        lanes = slice(lo, lo + value.shape[1])
        for strip in range(16):
            y1, x, z2 = strip // 8, (strip // 2) % 4, strip % 2
            for core in range(2):
                for y0 in range(2):
                    r = strip * 32 + core * 16 + y0 * 8
                    self.g[c, core, z2, y1 * 2 + y0, x, :, lanes] = value[r : r + 8]

    def cores(self, c):
        self.start(("p0", c), self.g.at[c, 1 - self.core], self.s1.at[c], self.partner)

    def first(self, c):
        self.finish(("p0", c))
        for half in range(2):
            self.s1[c, half] = self.s1[c, half] + self.g[c, self.core, half]
        for n, (to, dev) in enumerate(self.along_x):
            self.start(("p1", c), self.s1.at[c, 0, :, to], self.ra.at[c, n], dev)
        for n, (to, dev) in enumerate(self.along_y):
            self.start(("p1", c), self.s1.at[c, 1, to], self.rb.at[c, n], dev)

    def second(self, lo, hi):
        for c in range(lo, hi):
            self.finish(("p1", c))
            self.a2[c] = self.s1[c, 0, :, self.x] + self.ra[c, 0] + self.ra[c, 1] + self.ra[c, 2]
            self.b2[c] = self.s1[c, 1, self.y] + self.rb[c, 0] + self.rb[c, 1] + self.rb[c, 2]
        span = pl.ds(lo, hi - lo)
        for n, (to, dev) in enumerate(self.along_y):
            self.start(("p2", lo), self.a2.at[span, to], self.ra2.at[n, span], dev)
        for n, (to, dev) in enumerate(self.along_x):
            self.start(("p2", lo), self.b2.at[span, to], self.rb2.at[n, span], dev)

    def third(self, lo, hi):
        self.finish(("p2", lo))
        for c in range(lo, hi):
            a = self.a2[c, self.y] + self.ra2[0, c] + self.ra2[1, c] + self.ra2[2, c]
            b = self.b2[c, self.x] + self.rb2[0, c] + self.rb2[1, c] + self.rb2[2, c]
            for k in range(4):
                self.zs[c, k] = a[2 * k : 2 * k + 2]
                self.zs[c, 4 + k] = b[2 * k : 2 * k + 2]
        span = pl.ds(lo, hi - lo)
        for n, (to, dev) in enumerate(self.along_z):
            self.start(("p3", lo), self.zs.at[span, to], self.rz.at[n, span], dev)

    def last(self, lo, hi):
        self.finish(("p3", lo))
        out = []
        for c in range(lo, hi):
            mine = self.zs[c, self.z]
            for n in range(7):
                mine = mine + self.rz[n, c]
            out.append(mine)
        return out

    def table_cores(self, value):
        self.tt[0, 0] = value[0:8]
        self.tt[0, 1] = value[8:16]
        self.start("t0", self.tt.at[0, 1 - self.core], self.tr.at[0], self.partner)

    def table_axis(self, key, stage, first, count, own, peers):
        total = own
        if key is not None:
            self.finish(key)
            for n in range(count):
                total = total + self.tr[first + n]
        self.tt[stage, 0] = total
        for n, (_, dev) in enumerate(peers):
            self.start("t%d" % stage, self.tt.at[stage, 0], self.tr.at[first + count + n], dev)


def kernel(*refs):
    refs = list(refs)

    def take(n):
        out = refs[:n]
        del refs[:n]
        return out

    tok_hbm, cot_hbm, reg_hbm, rel_hbm, wqkv_hbm, wproj_hbm, tab_hbm = take(7)
    out_qkv, out_proj, out_tab = take(3)
    rel, reg, tab_t, tok, cot, wqkv, wproj, fetched = take(8)
    xp, cp, qkv, kvt, da, xpt = take(6)
    bias, mask, keep, dk, dv, dqt, at, gb, pad, tabp, relt, raw, wide, grads = take(14)
    ex = Exchange(*refs)

    fetches = []
    moves = (
        (rel_hbm, rel), (reg_hbm, reg), (tab_hbm, tab_t),
        (tok_hbm, tok), (cot_hbm, cot), (wqkv_hbm, wqkv), (wproj_hbm, wproj),
    )
    for n, (src, dst) in enumerate(moves):
        fetch = pltpu.make_async_copy(src, dst, fetched.at[n])
        fetch.start()
        fetches.append(fetch)
    ex.greet()
    for fetch in fetches[:3]:
        fetch.wait()
    small_tables(reg, rel, tab_t, bias, mask, pad, tabp, relt)
    gb[...] = jnp.zeros_like(gb)
    fetches[3].wait()
    gather_windows(tok, xp)
    fetches[4].wait()
    gather_windows(cot, cp)
    fetches[5].wait()
    fetches[6].wait()
    project(wqkv, wproj, xp, cp, qkv, kvt, da, xpt)

    att = Attention(qkv, kvt, da, bias, mask, keep, dk, dv, dqt, at, gb, raw, wide, grads)
    forward = att.forward1, att.forward2, att.forward3
    backward = att.backward1, att.backward2

    def v_chunk(c):
        ex.put(c, 0, nn(xpt[...], dv[:, c * 256 : (c + 1) * 256]))
        ex.cores(c)

    def proj_chunk(c):
        y = cp[:, :, c * 256 : (c + 1) * 256].reshape(WIN * SEG, 256)
        ex.put(2 + c, 0, nn(at[...], y))
        ex.cores(2 + c)

    def k_chunk(c):
        ex.put(4 + 2 * c, 0, nn(xpt[...], dk[:, c * 256 : (c + 1) * 256]))
        ex.cores(4 + 2 * c)

    def q_chunk(c):
        ex.put(5 + 2 * c, 0, nt(xpt[...], dqt[c * 256 : (c + 1) * 256, :]))
        ex.cores(5 + 2 * c)

    half = 2 * GROUP
    def finish(lo, hi):
        for c, mine in zip(range(lo, hi), ex.last(lo, hi)):
            for r in range(2):
                for part in range(2):
                    value = mine[r : r + 1, part * 128 : (part + 1) * 128]
                    if 2 <= c < 4:
                        k = r * 4 + (c - 2) * 2 + part
                        out_proj[k : k + 1, :] = value
                    else:
                        col = (8, 10, 0, 0, 4, 0, 6, 2)[c] + part
                        k = r * 12 + col
                        out_qkv[k : k + 1, :] = value

    quarter = GROUP
    att.run(forward, 0, half)
    ex.greeted()
    v_chunk(0)
    att.run(forward, half, STEPS)
    ex.first(0)
    v_chunk(1)
    proj_chunk(0)
    proj_chunk(1)
    att.run(backward, 0, quarter)
    ex.first(1)
    ex.first(2)
    att.run(backward, quarter, half)
    ex.first(3)
    att.run((att.backward_k,), 0, half)
    k_chunk(0)
    att.run((att.backward_q,), 0, half)
    q_chunk(0)
    att.run(backward, half, half + quarter)
    ex.first(4)
    att.run(backward, half + quarter, STEPS)
    ex.first(5)
    ex.second(0, 4)
    att.run((att.backward_k,), half, STEPS)
    k_chunk(1)
    ex.table_cores(table_gradient(gb, relt))
    att.run((att.backward_q,), half, half + quarter)
    ex.first(6)
    own = ex.tt[0, ex.core]
    ex.finish("t0")
    ex.table_axis(None, 1, 0, 1, own + ex.tr[0], ex.along_x)
    ex.third(0, 4)
    att.run((att.backward_q,), half + quarter, STEPS)
    q_chunk(1)
    ex.second(4, 6)
    ex.first(7)
    ex.table_axis("t1", 2, 1, 3, ex.tt[1, 0], ex.along_y)
    ex.third(4, 6)
    ex.second(6, 8)
    ex.table_axis("t2", 3, 4, 3, ex.tt[2, 0], ex.along_z)
    finish(0, 4)
    ex.third(6, 8)
    finish(4, 6)
    finish(6, 8)
    ex.finish("t3")
    table = ex.tt[3, 0]
    for n in range(7):
        table = table + ex.tr[7 + n]
    ex.tt[4, 0] = table
    ex.start("t4", ex.tt.at[4, 0], ex.tr.at[14], ex.partner)
    ex.finish("t4")
    core = ex.core.astype(F32)
    other = ex.tr[14]
    even = table * (1.0 - core) + other * core
    odd = table * core + other * (1.0 - core)
    for k in range(8):
        out_tab[2 * k : 2 * k + 1, :] = even[k : k + 1, 0:169]
        out_tab[2 * k + 1 : 2 * k + 2, :] = odd[k : k + 1, 0:169]


def apply_kernel(scale, *refs):
    for total, momentum, out in zip(refs[0:3], refs[3:6], refs[6:9]):
        out[...] = 0.9 * momentum[...] + total[...] * scale


SCRATCH = [
    pltpu.VMEM((TOK, TOK), jnp.int32),
    pltpu.VMEM((WIN, TOK), jnp.int32),
    pltpu.VMEM((16, 169), F32),
    pltpu.VMEM((784, D), BF),
    pltpu.VMEM((784, D), BF),
    pltpu.VMEM((D, 3 * D), BF),
    pltpu.VMEM((D, D), BF),
    pltpu.SemaphoreType.DMA((7,)),
    pltpu.VMEM((WIN, SEG, D), BF),
    pltpu.VMEM((WIN, SEG, D), BF),
    pltpu.VMEM((1024, 3 * D), BF),
    pltpu.VMEM((1024, 1024), BF),
    pltpu.VMEM((1024, D), BF),
    pltpu.VMEM((D, 1024), BF),
    pltpu.VMEM((4, TP, 256), F32),
    pltpu.VMEM((WIN, TP, 128), F32),
    pltpu.VMEM((4 * WIN, TP, 256), F32),
    pltpu.VMEM((1024, D), BF),
    pltpu.VMEM((1024, D), BF),
    pltpu.VMEM((D, 1024), BF),
    pltpu.VMEM((D, 1024), BF),
    pltpu.VMEM((8 * TP, 128), F32),
    pltpu.VMEM((128, 128), F32),
    pltpu.VMEM((16, 256), F32),
    pltpu.VMEM((TP, 128), F32),
    pltpu.VMEM((UNITS, 128, 256), F32),
    pltpu.VMEM((UNITS, 128, 256), BF),
    pltpu.VMEM((2 * WIN, 128, 256), BF),
    pltpu.VMEM((CHUNKS, 2, 2, 4, 4, 8, CH), F32),
    pltpu.VMEM((CHUNKS, 2, 4, 4, 8, CH), F32),
    pltpu.VMEM((CHUNKS, 3, 4, 8, CH), F32),
    pltpu.VMEM((CHUNKS, 3, 4, 8, CH), F32),
    pltpu.VMEM((CHUNKS, 4, 8, CH), F32),
    pltpu.VMEM((CHUNKS, 4, 8, CH), F32),
    pltpu.VMEM((3, CHUNKS, 8, CH), F32),
    pltpu.VMEM((3, CHUNKS, 8, CH), F32),
    pltpu.VMEM((CHUNKS, 8, 2, CH), F32),
    pltpu.VMEM((7, CHUNKS, 2, CH), F32),
    pltpu.VMEM((5, 2, 8, CH), F32),
    pltpu.VMEM((15, 8, CH), F32),
    pltpu.SemaphoreType.DMA((120,)),
    pltpu.SemaphoreType.DMA((120,)),
]


OUT = (
    jax.ShapeDtypeStruct((24, 128), F32),
    jax.ShapeDtypeStruct((8, 128), F32),
    jax.ShapeDtypeStruct((16, 169), F32),
)


def step(*operands):
    vm = pl.BlockSpec(memory_space=pltpu.VMEM)
    hbm = pl.BlockSpec(memory_space=pl.ANY)
    return pl.pallas_call(
        kernel,
        name="step",
        out_shape=OUT,
        in_specs=[hbm] * 7,
        out_specs=(vm, vm, vm),
        scratch_shapes=SCRATCH,
        compiler_params=pltpu.CompilerParams(
            collective_id=0, has_side_effects=True, vmem_limit_bytes=60 * 2**20
        ),
    )(*operands)


def apply(scale, *operands):
    vm = pl.BlockSpec(memory_space=pltpu.VMEM)
    return pl.pallas_call(
        functools.partial(apply_kernel, scale),
        name="apply",
        out_shape=OUT,
        in_specs=[vm] * 6,
        out_specs=(vm, vm, vm),
        compiler_params=pltpu.CompilerParams(vmem_limit_bytes=60 * 2**20),
    )(*operands)


def body(tokens, cotangent, regions, rel_index, w_qkv, w_proj, bias_table, mom_qkv, mom_proj, mom_table):
    win, count, dim = tokens.shape
    devices = lax.axis_size(("gx", "gy", "gz"))
    tok = jnp.transpose(tokens, (1, 0, 2)).reshape(count * win, dim)
    cot = jnp.transpose(cotangent, (1, 0, 2)).reshape(count * win, dim)
    sums = step(tok, cot, regions, rel_index, w_qkv, w_proj, bias_table.T)
    out_qkv, out_proj, out_tab = apply(
        1.0 / (win * devices), *sums, mom_qkv.reshape(24, 128), mom_proj.reshape(8, 128), mom_table.T
    )
    return out_qkv.reshape(-1), out_proj.reshape(-1), out_tab.T


def solution(mesh):
    rows = P(("gx", "gy", "gz"))
    wide = P(("gx", "gy", "gz"), None, None)
    return jax.shard_map(
        body,
        mesh=mesh,
        in_specs=(wide, wide, P(("gx", "gy", "gz"), None), P(), P(), P(), P(), rows, rows, P()),
        out_specs=(rows, rows, P()),
        check_vma=False,
    )
```

```python
import functools

import jax
import jax.numpy as jnp
from jax import lax
from jax.experimental import pallas as pl
from jax.experimental.pallas import tpu as pltpu
from jax.sharding import PartitionSpec as P

MESH = pl.DeviceIdType.MESH
BF = jnp.bfloat16
F32 = jnp.float32
WIN = 16
TOK = 49
SEG = 64
TP = 56
D = 512
HEAD_DIM = 32
SCALE = HEAD_DIM ** -0.5
UNITS = 8
ALL = 4 * WIN // 2
GROUP = ALL // 4
CH = 256
CHUNKS = 8


def nt(a, b):
    return lax.dot_general(a, b, (((1,), (1,)), ((), ())), preferred_element_type=F32)


def nn(a, b):
    return jnp.dot(a, b, preferred_element_type=F32)


def iota(shape, dim):
    return lax.broadcasted_iota(jnp.int32, shape, dim)


def onehot(condition):
    return condition.astype(F32).astype(BF)


def aligned(start, size, to=128):
    return pl.ds(pl.multiple_of(start, to), size)


def small_tables(reg, rel, tab_t, bias, mask, pad, tabp, relt):
    low = iota((TP, 128), 1) < SEG
    pad[...] = jnp.zeros_like(pad)
    pad[0:TOK, 0:TOK] = rel[...].astype(F32)
    flipped = pad[...].T
    both = flipped[0:TP] + pltpu.roll(flipped, SEG, 1)[0:TP]
    index = both.astype(jnp.int32)
    relt[...] = both
    pad[...] = jnp.zeros_like(pad)
    pad[0:WIN, 0:TOK] = reg[...].astype(F32)
    regions = pad[0:WIN, :]
    regions = regions + pltpu.roll(regions, SEG, 1)
    columns = pad[...].T[0:TP]
    for w in range(WIN):
        key = jnp.broadcast_to(columns[:, w : w + 1], (TP, 128))
        mask[w] = jnp.where(key == regions[w : w + 1], 0.0, -100.0).astype(F32)
    tabp[...] = jnp.zeros_like(tabp)
    tabp[:, 0:169] = tab_t[...]
    first = jnp.bitwise_and(index, 127)
    beyond = index >= 128
    real = iota((TP, 128), 0) < TOK

    def looked(h):
        lo = jnp.broadcast_to(tabp[h : h + 1, 0:128], (TP, 128))
        hi = jnp.broadcast_to(tabp[h : h + 1, 128:256], (TP, 128))
        lo = jnp.take_along_axis(lo, first, axis=1, mode="promise_in_bounds")
        hi = jnp.take_along_axis(hi, first, axis=1, mode="promise_in_bounds")
        return jnp.where(beyond, hi, lo)

    for k in range(8):
        value = jnp.where(low, looked(2 * k), looked(2 * k + 1))
        bias[k // 2, :, (k % 2) * 128 : (k % 2 + 1) * 128] = jnp.where(real, value, -1e30)


def gather_windows(src, dst):
    row, col = iota((256, 256), 0), iota((256, 256), 1)
    pick = onehot((row % 16) * 16 + row // 16 == col)
    for part in range(3):
        out = nn(pick, src[part * 256 : (part + 1) * 256, :]).astype(BF)
        dst[:, part * 16 : (part + 1) * 16, :] = out.reshape(WIN, 16, D)
    out = nn(pick[:, 0:16], src[768:784, :]).astype(BF)
    dst[:, 48:64, :] = out.reshape(WIN, 16, D)


def project(wqkv, wproj, xp, cp, qkv, kvt, da, xpt):
    eye = onehot(iota((128, 128), 0) == iota((128, 128), 1))
    s = iota((128, 128), 0)
    wanted = (
        (s // 32) * 32
        + ((s // 4) % 2) * 16
        + ((s // 2) % 2) * 8
        + ((s // 8) % 2) * 4
        + ((s // 16) % 2) * 2
        + s % 2
    )
    strips = onehot(wanted == iota((128, 128), 1))

    def four_windows(c, carry):
        rows = aligned(c * 256, 256, 256)
        x = xp[pl.ds(c * 4, 4)].reshape(256, D)
        y = cp[pl.ds(c * 4, 4)].reshape(256, D)
        values = nn(x, wqkv[...]).astype(BF)
        qkv[rows, :] = values
        da[rows, :] = nt(y, wproj[...]).astype(BF)
        for b in range(4):
            xpt[b * 128 : (b + 1) * 128, rows] = nt(strips, x[:, b * 128 : (b + 1) * 128]).astype(BF)
            k = values[:, 512 + b * 128 : 512 + (b + 1) * 128]
            kvt[b * 128 : (b + 1) * 128, rows] = nt(eye, k).astype(BF)
            v = values[:, 1024 + b * 128 : 1024 + (b + 1) * 128]
            kvt[512 + b * 128 : 512 + (b + 1) * 128, rows] = nt(strips, v).astype(BF)
        return carry

    lax.fori_loop(0, 4, four_windows, 0)


class Attention:
    def __init__(self, qkv, kvt, da, bias, mask, keep, dk, dv, dqt, at, gb, wide, grads):
        self.qkv, self.kvt, self.da, self.bias, self.mask = qkv, kvt, da, bias, mask
        self.keep, self.dk, self.dv, self.dqt, self.at = keep, dk, dv, dqt, at
        self.gb, self.wide, self.grads = gb, wide, grads
        lane = iota((SEG, 256), 1) % 128
        self.heads = [onehot(lane // HEAD_DIM == h) for h in range(4)]
        self.zero = jnp.zeros((SEG, 128), BF)
        self.tail = jnp.zeros((SEG - TP, 256), F32)
        half = iota((128, 128), 1)
        self.left = onehot(half < SEG)
        self.right = onehot(half >= SEG)
        self.low = iota((32, 128), 1) < SEG

    def spread(self, a):
        a = jnp.concatenate([a[0:SEG], a[SEG:]], axis=1)
        return jnp.concatenate([a * head for head in self.heads], axis=0)

    def diagonal(self, a):
        upper = jnp.concatenate([a[0:SEG], self.zero], axis=1)
        lower = jnp.concatenate([self.zero, a[SEG:]], axis=1)
        return jnp.concatenate([upper, lower], axis=0)

    def stack(self, a, b):
        return jnp.concatenate([a, self.tail, b, self.tail], axis=0).astype(BF)

    def own(self, dst, pair, g, value):
        dst[aligned(pair * 128, SEG), aligned(g * 128, 128)] = value[0:SEG, 0:128].astype(BF)
        dst[aligned(pair * 128 + SEG, SEG, SEG), aligned(g * 128, 128)] = value[SEG:, 128:256].astype(BF)

    def across(self, dst, pair, g, turned, wide):
        lhs = jnp.concatenate([turned * self.left, turned * self.right], axis=0)
        full = nn(lhs, wide)
        for h in range(4):
            lanes = slice((h // 2) * 128, (h // 2 + 1) * 128)
            one = full[32 * h : 32 * h + 32, lanes]
            two = full[128 + 32 * h : 128 + 32 * h + 32, lanes]
            if h % 2:
                one = pltpu.roll(one, SEG, 1)
            else:
                two = pltpu.roll(two, SEG, 1)
            value = jnp.where(self.low, one, two).astype(BF)
            dst[aligned(g * 128 + 32 * h, 32, 32), aligned(pair * 128, 128)] = value

    def place(self, unit):
        return unit // (WIN // 2), unit % (WIN // 2)

    def forward12(self, u, unit):
        g, pair = self.place(unit)
        rows = aligned(pair * 128, 128)
        q_wide = self.spread(self.qkv[rows, aligned(g * 128, 128)])
        raw = nt(self.diagonal(self.qkv[rows, aligned(512 + g * 128, 128)]), q_wide)
        probs = []
        for i in range(2):
            scores = raw[i * SEG : i * SEG + TP] * SCALE + self.bias[g]
            scores = scores + jnp.concatenate([self.mask[2 * pair + i]] * 2, axis=1)
            e = jnp.exp(scores - jnp.max(scores, axis=0, keepdims=True))
            p = e * (1.0 / jnp.sum(e, axis=0, keepdims=True))
            self.keep[2 * unit + i] = p
            probs.append(p)
        self.wide[u] = self.stack(*probs)

    def forward3(self, u, unit):
        g, pair = self.place(unit)
        rows = aligned(pair * 128, 128)
        probs = self.wide[u]
        da_wide = self.spread(self.da[rows, aligned(g * 128, 128)])
        self.own(self.dv, pair, g, nn(probs, da_wide))
        self.across(self.at, pair, g, self.kvt[aligned(512 + g * 128, 128), rows], probs)

    def backward12(self, u, unit):
        g, pair = self.place(unit)
        rows = aligned(pair * 128, 128)
        da_wide = self.spread(self.da[rows, aligned(g * 128, 128)])
        raw = nt(self.diagonal(self.qkv[rows, aligned(1024 + g * 128, 128)]), da_wide)
        parts = []
        for i in range(2):
            p = self.keep[2 * unit + i]
            dp = raw[i * SEG : i * SEG + TP]
            parts.append(p * (dp - jnp.sum(p * dp, axis=0, keepdims=True)))
        total = parts[0] + parts[1]
        for k in range(2):
            block = aligned((2 * g + k) * TP, TP, 8)
            self.gb[block, :] = self.gb[block, :] + total[:, k * 128 : (k + 1) * 128]
        self.grads[unit] = self.stack(parts[0] * SCALE, parts[1] * SCALE)

    def backward_k(self, u, unit):
        g, pair = self.place(unit)
        rows = aligned(pair * 128, 128)
        q_wide = self.spread(self.qkv[rows, aligned(g * 128, 128)])
        self.own(self.dk, pair, g, nn(self.grads[unit], q_wide))

    def backward_q(self, u, unit):
        g, pair = self.place(unit)
        rows = aligned(pair * 128, 128)
        self.across(self.dqt, pair, g, self.kvt[aligned(g * 128, 128), rows], self.grads[unit])

    def stages(self, stages, units, t, which):
        for n in reversed(which):
            for u in range(units):
                stages[n](u, (t - n) * units + u)

    def run(self, stages, units, lo, hi):
        ahead = len(stages) - 1
        whole = tuple(range(len(stages)))
        lo, hi, steps = lo // units, hi // units, ALL // units
        if lo == 0:
            for t in range(ahead):
                self.stages(stages, units, t, whole[: t + 1])
        end = steps if hi == steps else hi + ahead

        def one(t, carry):
            self.stages(stages, units, t, whole)
            return carry

        if end - lo - ahead == 1:
            one(lo + ahead, 0)
        else:
            lax.fori_loop(lo + ahead, end, one, 0)
        if hi == steps:
            for t in range(ahead):
                self.stages(stages, units, steps + t, whole[t + 1 :])


def table_gradient(gb, relt):
    low = iota((8, 128), 1) < SEG
    entry = iota((256, 128), 0).astype(F32)
    total = jnp.zeros((32, 256), F32)

    def line(j):
        if j >= TOK:
            return jnp.zeros((32, 128), BF), jnp.zeros((256, 128), BF)
        hot = onehot(entry == jnp.broadcast_to(relt[j : j + 1, :], (256, 128)))
        pairs = gb[pl.ds(j, 8, stride=TP), :]
        split = jnp.concatenate([jnp.where(low, pairs, 0.0), jnp.where(low, 0.0, pairs)], axis=0)
        upper = split.astype(BF)
        lower = (split - upper.astype(F32)).astype(BF)
        return jnp.concatenate([upper, lower], axis=0), hot

    for j in range(0, TOK, 2):
        a, b = line(j), line(j + 1)
        total = total + nt(
            jnp.concatenate([a[0], b[0]], axis=1), jnp.concatenate([a[1], b[1]], axis=1)
        )
    return total[0:16] + total[16:32]


class Exchange:
    def __init__(self, g, s1, ra, rb, a2, b2, ra2, rb2, zs, rz, tt, tr, send, recv):
        self.g, self.s1, self.ra, self.rb, self.a2, self.b2 = g, s1, ra, rb, a2, b2
        self.ra2, self.rb2, self.zs, self.rz, self.tt, self.tr = ra2, rb2, zs, rz, tt, tr
        self.send, self.recv, self.used = send, recv, 0
        gx, gy, gz = lax.axis_index("gx"), lax.axis_index("gy"), lax.axis_index("gz")
        x, z, core = lax.rem(gx, 4), gy, lax.rem(gz, 2)
        y = (gx // 4) * 2 + gz // 2

        def device(x, y, z, core):
            return ((y // 2) * 4 + x, z, lax.rem(y, 2) * 2 + core)

        def xor(a, b):
            out = 0
            for bit in (1, 2, 4):
                have = lax.rem(a // bit, 2)
                out = out + bit * ((1 - have) if b & bit else have)
            return out

        self.x, self.y, self.z, self.core = x, y, z, core
        self.partner = device(x, y, z, 1 - core)
        self.along_x = [(xor(x, d), device(xor(x, d), y, z, core)) for d in (1, 2, 3)]
        self.along_y = [(xor(y, d), device(x, xor(y, d), z, core)) for d in (1, 2, 3)]
        self.along_z = [(xor(z, d), device(x, y, xor(z, d), core)) for d in range(1, 8)]
        self.flight = {}

    def greet(self):
        self.peers = [self.partner] + [dev for _, dev in self.along_x + self.along_y + self.along_z]
        barrier = pltpu.get_barrier_semaphore()
        for peer in self.peers:
            pl.semaphore_signal(barrier, inc=1, device_id=peer, device_id_type=MESH)

    def greeted(self):
        pl.semaphore_wait(pltpu.get_barrier_semaphore(), len(self.peers))

    def start(self, key, src, dst, dev):
        n = self.used
        self.used += 1
        c = pltpu.make_async_remote_copy(
            src_ref=src, dst_ref=dst, send_sem=self.send.at[n], recv_sem=self.recv.at[n],
            device_id=dev, device_id_type=MESH,
        )
        c.start()
        self.flight.setdefault(key, []).append(c)

    def finish(self, key):
        for c in self.flight.pop(key):
            c.wait()

    def put(self, c, lo, value):
        lanes = slice(lo, lo + value.shape[1])
        for strip in range(16):
            y1, x, z2 = strip // 8, (strip // 2) % 4, strip % 2
            for core in range(2):
                for y0 in range(2):
                    r = strip * 32 + core * 16 + y0 * 8
                    self.g[c, core, z2, y1 * 2 + y0, x, :, lanes] = value[r : r + 8]

    def cores(self, c):
        self.start(("p0", c), self.g.at[c, 1 - self.core], self.s1.at[c], self.partner)

    def first(self, c):
        self.finish(("p0", c))
        for half in range(2):
            self.s1[c, half] = self.s1[c, half] + self.g[c, self.core, half]
        for n, (to, dev) in enumerate(self.along_x):
            self.start(("p1", c), self.s1.at[c, 0, :, to], self.ra.at[c, n], dev)
        for n, (to, dev) in enumerate(self.along_y):
            self.start(("p1", c), self.s1.at[c, 1, to], self.rb.at[c, n], dev)

    def second(self, lo, hi):
        for c in range(lo, hi):
            self.finish(("p1", c))
            self.a2[c] = self.s1[c, 0, :, self.x] + self.ra[c, 0] + self.ra[c, 1] + self.ra[c, 2]
            self.b2[c] = self.s1[c, 1, self.y] + self.rb[c, 0] + self.rb[c, 1] + self.rb[c, 2]
        span = pl.ds(lo, hi - lo)
        for n, (to, dev) in enumerate(self.along_y):
            self.start(("p2", lo), self.a2.at[span, to], self.ra2.at[n, span], dev)
        for n, (to, dev) in enumerate(self.along_x):
            self.start(("p2", lo), self.b2.at[span, to], self.rb2.at[n, span], dev)

    def third(self, lo, hi):
        self.finish(("p2", lo))
        for c in range(lo, hi):
            a = self.a2[c, self.y] + self.ra2[0, c] + self.ra2[1, c] + self.ra2[2, c]
            b = self.b2[c, self.x] + self.rb2[0, c] + self.rb2[1, c] + self.rb2[2, c]
            for k in range(4):
                self.zs[c, k] = a[2 * k : 2 * k + 2]
                self.zs[c, 4 + k] = b[2 * k : 2 * k + 2]
        span = pl.ds(lo, hi - lo)
        for n, (to, dev) in enumerate(self.along_z):
            self.start(("p3", lo), self.zs.at[span, to], self.rz.at[n, span], dev)

    def last(self, lo, hi):
        self.finish(("p3", lo))
        out = []
        for c in range(lo, hi):
            mine = self.zs[c, self.z]
            for n in range(7):
                mine = mine + self.rz[n, c]
            out.append(mine)
        return out

    def table_cores(self, value):
        self.tt[0, 0] = value[0:8]
        self.tt[0, 1] = value[8:16]
        self.start("t0", self.tt.at[0, 1 - self.core], self.tr.at[0], self.partner)

    def table_axis(self, key, stage, first, count, own, peers):
        total = own
        if key is not None:
            self.finish(key)
            for n in range(count):
                total = total + self.tr[first + n]
        self.tt[stage, 0] = total
        for n, (_, dev) in enumerate(peers):
            self.start("t%d" % stage, self.tt.at[stage, 0], self.tr.at[first + count + n], dev)


def kernel(*refs):
    refs = list(refs)

    def take(n):
        out = refs[:n]
        del refs[:n]
        return out

    tok_hbm, cot_hbm, reg_hbm, rel_hbm, wqkv_hbm, wproj_hbm, tab_hbm = take(7)
    out_qkv, out_proj, out_tab = take(3)
    rel, reg, tab_t, tok, cot, wqkv, wproj, fetched = take(8)
    xp, cp, qkv, kvt, da, xpt = take(6)
    bias, mask, keep, dk, dv, dqt, at, gb, pad, tabp, relt, wide, grads = take(13)
    ex = Exchange(*refs)

    fetches = []
    moves = (
        (rel_hbm, rel), (reg_hbm, reg), (tab_hbm, tab_t),
        (tok_hbm, tok), (cot_hbm, cot), (wqkv_hbm, wqkv), (wproj_hbm, wproj),
    )
    for n, (src, dst) in enumerate(moves):
        fetch = pltpu.make_async_copy(src, dst, fetched.at[n])
        fetch.start()
        fetches.append(fetch)
    ex.greet()
    for fetch in fetches[:3]:
        fetch.wait()
    small_tables(reg, rel, tab_t, bias, mask, pad, tabp, relt)
    gb[...] = jnp.zeros_like(gb)
    fetches[3].wait()
    gather_windows(tok, xp)
    fetches[4].wait()
    gather_windows(cot, cp)
    fetches[5].wait()
    fetches[6].wait()
    project(wqkv, wproj, xp, cp, qkv, kvt, da, xpt)

    att = Attention(qkv, kvt, da, bias, mask, keep, dk, dv, dqt, at, gb, wide, grads)
    forward = (att.forward12, att.forward3), 4
    backward = (att.backward12,), 8
    to_keys = (att.backward_k,), 8
    to_queries = (att.backward_q,), 8

    def v_chunk(c):
        ex.put(c, 0, nn(xpt[...], dv[:, c * 256 : (c + 1) * 256]))
        ex.cores(c)

    def proj_chunk(c):
        y = cp[:, :, c * 256 : (c + 1) * 256].reshape(WIN * SEG, 256)
        ex.put(2 + c, 0, nn(at[...], y))
        ex.cores(2 + c)

    def k_chunk(c):
        ex.put(4 + 2 * c, 0, nn(xpt[...], dk[:, c * 256 : (c + 1) * 256]))
        ex.cores(4 + 2 * c)

    def q_chunk(c):
        ex.put(5 + 2 * c, 0, nt(xpt[...], dqt[c * 256 : (c + 1) * 256, :]))
        ex.cores(5 + 2 * c)

    half = 2 * GROUP
    def finish(lo, hi):
        for c, mine in zip(range(lo, hi), ex.last(lo, hi)):
            for r in range(2):
                for part in range(2):
                    value = mine[r : r + 1, part * 128 : (part + 1) * 128]
                    if 2 <= c < 4:
                        k = r * 4 + (c - 2) * 2 + part
                        out_proj[k : k + 1, :] = value
                    else:
                        col = (8, 10, 0, 0, 4, 0, 6, 2)[c] + part
                        k = r * 12 + col
                        out_qkv[k : k + 1, :] = value

    quarter = GROUP
    att.run(*forward, 0, half)
    ex.greeted()
    v_chunk(0)
    att.run(*forward, half, ALL)
    ex.first(0)
    v_chunk(1)
    proj_chunk(0)
    proj_chunk(1)
    att.run(*backward, 0, quarter)
    ex.first(1)
    ex.first(2)
    att.run(*backward, quarter, half)
    ex.first(3)
    att.run(*to_keys, 0, half)
    k_chunk(0)
    att.run(*to_queries, 0, half)
    q_chunk(0)
    att.run(*backward, half, half + quarter)
    ex.first(4)
    att.run(*backward, half + quarter, ALL)
    ex.first(5)
    ex.table_cores(table_gradient(gb, relt))
    ex.second(0, 3)
    att.run(*to_keys, half, ALL)
    own = ex.tt[0, ex.core]
    ex.finish("t0")
    ex.table_axis(None, 1, 0, 1, own + ex.tr[0], ex.along_x)
    k_chunk(1)
    att.run(*to_queries, half, half + quarter)
    ex.first(6)
    att.run(*to_queries, half + quarter, ALL)
    ex.table_axis("t1", 2, 1, 3, ex.tt[1, 0], ex.along_y)
    ex.third(0, 3)
    q_chunk(1)
    ex.second(3, 6)
    ex.first(7)
    ex.table_axis("t2", 3, 4, 3, ex.tt[2, 0], ex.along_z)
    ex.third(3, 6)
    finish(0, 3)
    ex.second(6, 8)
    ex.third(6, 8)
    finish(3, 6)
    ex.finish("t3")
    table = ex.tt[3, 0]
    for n in range(7):
        table = table + ex.tr[7 + n]
    ex.tt[4, 0] = table
    ex.start("t4", ex.tt.at[4, 0], ex.tr.at[14], ex.partner)
    ex.finish("t4")
    finish(6, 8)
    core = ex.core.astype(F32)
    other = ex.tr[14]
    even = table * (1.0 - core) + other * core
    odd = table * core + other * (1.0 - core)
    for k in range(8):
        out_tab[2 * k : 2 * k + 1, :] = even[k : k + 1, 0:169]
        out_tab[2 * k + 1 : 2 * k + 2, :] = odd[k : k + 1, 0:169]


def apply_kernel(scale, *refs):
    for total, momentum, out in zip(refs[0:3], refs[3:6], refs[6:9]):
        out[...] = 0.9 * momentum[...] + total[...] * scale


SCRATCH = [
    pltpu.VMEM((TOK, TOK), jnp.int32),
    pltpu.VMEM((WIN, TOK), jnp.int32),
    pltpu.VMEM((16, 169), F32),
    pltpu.VMEM((784, D), BF),
    pltpu.VMEM((784, D), BF),
    pltpu.VMEM((D, 3 * D), BF),
    pltpu.VMEM((D, D), BF),
    pltpu.SemaphoreType.DMA((7,)),
    pltpu.VMEM((WIN, SEG, D), BF),
    pltpu.VMEM((WIN, SEG, D), BF),
    pltpu.VMEM((1024, 3 * D), BF),
    pltpu.VMEM((1024, 1024), BF),
    pltpu.VMEM((1024, D), BF),
    pltpu.VMEM((D, 1024), BF),
    pltpu.VMEM((4, TP, 256), F32),
    pltpu.VMEM((WIN, TP, 128), F32),
    pltpu.VMEM((4 * WIN, TP, 256), F32),
    pltpu.VMEM((1024, D), BF),
    pltpu.VMEM((1024, D), BF),
    pltpu.VMEM((D, 1024), BF),
    pltpu.VMEM((D, 1024), BF),
    pltpu.VMEM((8 * TP, 128), F32),
    pltpu.VMEM((128, 128), F32),
    pltpu.VMEM((16, 256), F32),
    pltpu.VMEM((TP, 128), F32),
    pltpu.VMEM((UNITS, 128, 256), BF),
    pltpu.VMEM((2 * WIN, 128, 256), BF),
    pltpu.VMEM((CHUNKS, 2, 2, 4, 4, 8, CH), F32),
    pltpu.VMEM((CHUNKS, 2, 4, 4, 8, CH), F32),
    pltpu.VMEM((CHUNKS, 3, 4, 8, CH), F32),
    pltpu.VMEM((CHUNKS, 3, 4, 8, CH), F32),
    pltpu.VMEM((CHUNKS, 4, 8, CH), F32),
    pltpu.VMEM((CHUNKS, 4, 8, CH), F32),
    pltpu.VMEM((3, CHUNKS, 8, CH), F32),
    pltpu.VMEM((3, CHUNKS, 8, CH), F32),
    pltpu.VMEM((CHUNKS, 8, 2, CH), F32),
    pltpu.VMEM((7, CHUNKS, 2, CH), F32),
    pltpu.VMEM((5, 2, 8, CH), F32),
    pltpu.VMEM((15, 8, CH), F32),
    pltpu.SemaphoreType.DMA((120,)),
    pltpu.SemaphoreType.DMA((120,)),
]


OUT = (
    jax.ShapeDtypeStruct((24, 128), F32),
    jax.ShapeDtypeStruct((8, 128), F32),
    jax.ShapeDtypeStruct((16, 169), F32),
)


def step(*operands):
    vm = pl.BlockSpec(memory_space=pltpu.VMEM)
    hbm = pl.BlockSpec(memory_space=pl.ANY)
    return pl.pallas_call(
        kernel,
        name="step",
        out_shape=OUT,
        in_specs=[hbm] * 7,
        out_specs=(vm, vm, vm),
        scratch_shapes=SCRATCH,
        compiler_params=pltpu.CompilerParams(
            collective_id=0, has_side_effects=True, vmem_limit_bytes=60 * 2**20
        ),
    )(*operands)


def apply(scale, *operands):
    vm = pl.BlockSpec(memory_space=pltpu.VMEM)
    return pl.pallas_call(
        functools.partial(apply_kernel, scale),
        name="apply",
        out_shape=OUT,
        in_specs=[vm] * 6,
        out_specs=(vm, vm, vm),
        compiler_params=pltpu.CompilerParams(vmem_limit_bytes=60 * 2**20),
    )(*operands)


def body(tokens, cotangent, regions, rel_index, w_qkv, w_proj, bias_table, mom_qkv, mom_proj, mom_table):
    win, count, dim = tokens.shape
    devices = lax.axis_size(("gx", "gy", "gz"))
    tok = jnp.transpose(tokens, (1, 0, 2)).reshape(count * win, dim)
    cot = jnp.transpose(cotangent, (1, 0, 2)).reshape(count * win, dim)
    sums = step(tok, cot, regions, rel_index, w_qkv, w_proj, bias_table.T)
    out_qkv, out_proj, out_tab = apply(
        1.0 / (win * devices), *sums, mom_qkv.reshape(24, 128), mom_proj.reshape(8, 128), mom_table.T
    )
    return out_qkv.reshape(-1), out_proj.reshape(-1), out_tab.T


def solution(mesh):
    rows = P(("gx", "gy", "gz"))
    wide = P(("gx", "gy", "gz"), None, None)
    return jax.shard_map(
        body,
        mesh=mesh,
        in_specs=(wide, wide, P(("gx", "gy", "gz"), None), P(), P(), P(), P(), rows, rows, P()),
        out_specs=(rows, rows, P()),
        check_vma=False,
    )
```

```python
import functools

import jax
import jax.numpy as jnp
from jax import lax
from jax.experimental import pallas as pl
from jax.experimental.pallas import tpu as pltpu
from jax.sharding import PartitionSpec as P

MESH = pl.DeviceIdType.MESH
BF = jnp.bfloat16
F32 = jnp.float32
WIN = 16
TOK = 49
SEG = 64
TP = 56
D = 512
HEAD_DIM = 32
SCALE = HEAD_DIM ** -0.5
UNITS = 8
ALL = 4 * WIN // 2
GROUP = ALL // 4
ENTRIES = 176
CH = 256
CHUNKS = 8


def nt(a, b):
    return lax.dot_general(a, b, (((1,), (1,)), ((), ())), preferred_element_type=F32)


def nn(a, b):
    return jnp.dot(a, b, preferred_element_type=F32)


def iota(shape, dim):
    return lax.broadcasted_iota(jnp.int32, shape, dim)


def onehot(condition):
    return condition.astype(F32).astype(BF)


def aligned(start, size, to=128):
    return pl.ds(pl.multiple_of(start, to), size)


def small_tables(reg, rel, tab_t, bias, mask, pad, tabp, relt):
    low = iota((TP, 128), 1) < SEG
    pad[...] = jnp.zeros_like(pad)
    pad[0:TOK, 0:TOK] = rel[...].astype(F32)
    flipped = pad[...].T
    both = flipped[0:TP] + pltpu.roll(flipped, SEG, 1)[0:TP]
    index = both.astype(jnp.int32)
    relt[...] = both
    pad[...] = jnp.zeros_like(pad)
    pad[0:WIN, 0:TOK] = reg[...].astype(F32)
    regions = pad[0:WIN, :]
    regions = regions + pltpu.roll(regions, SEG, 1)
    columns = pad[...].T[0:TP]
    for w in range(WIN):
        key = jnp.broadcast_to(columns[:, w : w + 1], (TP, 128))
        mask[w] = jnp.where(key == regions[w : w + 1], 0.0, -100.0).astype(F32)
    tabp[...] = jnp.zeros_like(tabp)
    tabp[:, 0:169] = tab_t[...]
    first = jnp.bitwise_and(index, 127)
    beyond = index >= 128
    real = iota((TP, 128), 0) < TOK

    def looked(h):
        lo = jnp.broadcast_to(tabp[h : h + 1, 0:128], (TP, 128))
        hi = jnp.broadcast_to(tabp[h : h + 1, 128:256], (TP, 128))
        lo = jnp.take_along_axis(lo, first, axis=1, mode="promise_in_bounds")
        hi = jnp.take_along_axis(hi, first, axis=1, mode="promise_in_bounds")
        return jnp.where(beyond, hi, lo)

    for k in range(8):
        value = jnp.where(low, looked(2 * k), looked(2 * k + 1))
        bias[k // 2, :, (k % 2) * 128 : (k % 2 + 1) * 128] = jnp.where(real, value, -1e30)


def gather_windows(src, dst):
    row, col = iota((256, 256), 0), iota((256, 256), 1)
    pick = onehot((row % 16) * 16 + row // 16 == col)
    for part in range(3):
        out = nn(pick, src[part * 256 : (part + 1) * 256, :]).astype(BF)
        dst[:, part * 16 : (part + 1) * 16, :] = out.reshape(WIN, 16, D)
    out = nn(pick[:, 0:16], src[768:784, :]).astype(BF)
    dst[:, 48:64, :] = out.reshape(WIN, 16, D)


def project(wqkv, wproj, xp, cp, qkv, kvt, da, xpt):
    eye = onehot(iota((128, 128), 0) == iota((128, 128), 1))
    s = iota((128, 128), 0)
    wanted = (
        (s // 32) * 32
        + ((s // 4) % 2) * 16
        + ((s // 2) % 2) * 8
        + ((s // 8) % 2) * 4
        + ((s // 16) % 2) * 2
        + s % 2
    )
    strips = onehot(wanted == iota((128, 128), 1))

    def four_windows(c, carry):
        rows = aligned(c * 256, 256, 256)
        x = xp[pl.ds(c * 4, 4)].reshape(256, D)
        y = cp[pl.ds(c * 4, 4)].reshape(256, D)
        values = nn(x, wqkv[...]).astype(BF)
        qkv[rows, :] = values
        da[rows, :] = nt(y, wproj[...]).astype(BF)
        for b in range(4):
            xpt[b * 128 : (b + 1) * 128, rows] = nt(strips, x[:, b * 128 : (b + 1) * 128]).astype(BF)
            k = values[:, 512 + b * 128 : 512 + (b + 1) * 128]
            kvt[b * 128 : (b + 1) * 128, rows] = nt(eye, k).astype(BF)
            v = values[:, 1024 + b * 128 : 1024 + (b + 1) * 128]
            kvt[512 + b * 128 : 512 + (b + 1) * 128, rows] = nt(strips, v).astype(BF)
        return carry

    lax.fori_loop(0, 4, four_windows, 0)


class Attention:
    def __init__(self, qkv, kvt, da, bias, mask, keep, dk, dv, dqt, at, gb, wide, grads):
        self.qkv, self.kvt, self.da, self.bias, self.mask = qkv, kvt, da, bias, mask
        self.keep, self.dk, self.dv, self.dqt, self.at = keep, dk, dv, dqt, at
        self.gb, self.wide, self.grads = gb, wide, grads
        lane = iota((SEG, 256), 1) % 128
        self.heads = [onehot(lane // HEAD_DIM == h) for h in range(4)]
        self.zero = jnp.zeros((SEG, 128), BF)
        self.tail = jnp.zeros((SEG - TP, 256), F32)
        half = iota((128, 128), 1)
        self.left = onehot(half < SEG)
        self.right = onehot(half >= SEG)
        self.low = iota((32, 128), 1) < SEG

    def spread(self, a):
        a = jnp.concatenate([a[0:SEG], a[SEG:]], axis=1)
        return jnp.concatenate([a * head for head in self.heads], axis=0)

    def diagonal(self, a):
        upper = jnp.concatenate([a[0:SEG], self.zero], axis=1)
        lower = jnp.concatenate([self.zero, a[SEG:]], axis=1)
        return jnp.concatenate([upper, lower], axis=0)

    def stack(self, a, b):
        return jnp.concatenate([a, self.tail, b, self.tail], axis=0).astype(BF)

    def own(self, dst, pair, g, value):
        dst[aligned(pair * 128, SEG), aligned(g * 128, 128)] = value[0:SEG, 0:128].astype(BF)
        dst[aligned(pair * 128 + SEG, SEG, SEG), aligned(g * 128, 128)] = value[SEG:, 128:256].astype(BF)

    def across(self, dst, pair, g, turned, wide):
        lhs = jnp.concatenate([turned * self.left, turned * self.right], axis=0)
        full = nn(lhs, wide)
        for h in range(4):
            lanes = slice((h // 2) * 128, (h // 2 + 1) * 128)
            one = full[32 * h : 32 * h + 32, lanes]
            two = full[128 + 32 * h : 128 + 32 * h + 32, lanes]
            if h % 2:
                one = pltpu.roll(one, SEG, 1)
            else:
                two = pltpu.roll(two, SEG, 1)
            value = jnp.where(self.low, one, two).astype(BF)
            dst[aligned(g * 128 + 32 * h, 32, 32), aligned(pair * 128, 128)] = value

    def place(self, unit):
        return unit // (WIN // 2), unit % (WIN // 2)

    def forward12(self, u, unit):
        g, pair = self.place(unit)
        rows = aligned(pair * 128, 128)
        q_wide = self.spread(self.qkv[rows, aligned(g * 128, 128)])
        raw = nt(self.diagonal(self.qkv[rows, aligned(512 + g * 128, 128)]), q_wide)
        probs = []
        for i in range(2):
            scores = raw[i * SEG : i * SEG + TP] * SCALE + self.bias[g]
            scores = scores + jnp.concatenate([self.mask[2 * pair + i]] * 2, axis=1)
            e = jnp.exp(scores - jnp.max(scores, axis=0, keepdims=True))
            p = e * (1.0 / jnp.sum(e, axis=0, keepdims=True))
            self.keep[2 * unit + i] = p
            probs.append(p)
        self.wide[u] = self.stack(*probs)

    def forward3(self, u, unit):
        g, pair = self.place(unit)
        rows = aligned(pair * 128, 128)
        probs = self.wide[u]
        da_wide = self.spread(self.da[rows, aligned(g * 128, 128)])
        self.own(self.dv, pair, g, nn(probs, da_wide))
        self.across(self.at, pair, g, self.kvt[aligned(512 + g * 128, 128), rows], probs)

    def backward12(self, u, unit):
        g, pair = self.place(unit)
        rows = aligned(pair * 128, 128)
        da_wide = self.spread(self.da[rows, aligned(g * 128, 128)])
        raw = nt(self.diagonal(self.qkv[rows, aligned(1024 + g * 128, 128)]), da_wide)
        parts = []
        for i in range(2):
            p = self.keep[2 * unit + i]
            dp = raw[i * SEG : i * SEG + TP]
            parts.append(p * (dp - jnp.sum(p * dp, axis=0, keepdims=True)))
        total = parts[0] + parts[1]
        for k in range(2):
            block = aligned((2 * g + k) * TP, TP, 8)
            self.gb[block, :] = self.gb[block, :] + total[:, k * 128 : (k + 1) * 128]
        self.grads[unit] = self.stack(parts[0] * SCALE, parts[1] * SCALE)

    def backward_k(self, u, unit):
        g, pair = self.place(unit)
        rows = aligned(pair * 128, 128)
        q_wide = self.spread(self.qkv[rows, aligned(g * 128, 128)])
        self.own(self.dk, pair, g, nn(self.grads[unit], q_wide))

    def backward_q(self, u, unit):
        g, pair = self.place(unit)
        rows = aligned(pair * 128, 128)
        self.across(self.dqt, pair, g, self.kvt[aligned(g * 128, 128), rows], self.grads[unit])

    def stages(self, stages, units, t, which):
        for n in reversed(which):
            for u in range(units):
                stages[n](u, (t - n) * units + u)

    def run(self, stages, units, lo, hi):
        ahead = len(stages) - 1
        whole = tuple(range(len(stages)))
        lo, hi, steps = lo // units, hi // units, ALL // units
        if lo == 0:
            for t in range(ahead):
                self.stages(stages, units, t, whole[: t + 1])
        end = steps if hi == steps else hi + ahead

        def one(t, carry):
            self.stages(stages, units, t, whole)
            return carry

        if end - lo - ahead == 1:
            one(lo + ahead, 0)
        else:
            lax.fori_loop(lo + ahead, end, one, 0)
        if hi == steps:
            for t in range(ahead):
                self.stages(stages, units, steps + t, whole[t + 1 :])


def table_gradient(gb, relt):
    low = iota((8, 128), 1) < SEG
    entry = iota((ENTRIES, 128), 0).astype(F32)
    total = jnp.zeros((32, ENTRIES), F32)

    def line(j):
        if j >= TOK:
            return jnp.zeros((32, 128), BF), jnp.zeros((ENTRIES, 128), BF)
        hot = onehot(entry == jnp.broadcast_to(relt[j : j + 1, :], (ENTRIES, 128)))
        pairs = gb[pl.ds(j, 8, stride=TP), :]
        split = jnp.concatenate([jnp.where(low, pairs, 0.0), jnp.where(low, 0.0, pairs)], axis=0)
        upper = split.astype(BF)
        lower = (split - upper.astype(F32)).astype(BF)
        return jnp.concatenate([upper, lower], axis=0), hot

    for j in range(0, TOK, 2):
        a, b = line(j), line(j + 1)
        total = total + nt(
            jnp.concatenate([a[0], b[0]], axis=1), jnp.concatenate([a[1], b[1]], axis=1)
        )
    return total[0:16] + total[16:32]


class Exchange:
    def __init__(self, g, s1, ra, rb, a2, b2, ra2, rb2, zs, rz, tt, tr, send, recv):
        self.g, self.s1, self.ra, self.rb, self.a2, self.b2 = g, s1, ra, rb, a2, b2
        self.ra2, self.rb2, self.zs, self.rz, self.tt, self.tr = ra2, rb2, zs, rz, tt, tr
        self.send, self.recv, self.used = send, recv, 0
        gx, gy, gz = lax.axis_index("gx"), lax.axis_index("gy"), lax.axis_index("gz")
        x, z, core = lax.rem(gx, 4), gy, lax.rem(gz, 2)
        y = (gx // 4) * 2 + gz // 2

        def device(x, y, z, core):
            return ((y // 2) * 4 + x, z, lax.rem(y, 2) * 2 + core)

        def xor(a, b):
            out = 0
            for bit in (1, 2, 4):
                have = lax.rem(a // bit, 2)
                out = out + bit * ((1 - have) if b & bit else have)
            return out

        self.x, self.y, self.z, self.core = x, y, z, core
        self.partner = device(x, y, z, 1 - core)
        self.along_x = [(xor(x, d), device(xor(x, d), y, z, core)) for d in (1, 2, 3)]
        self.along_y = [(xor(y, d), device(x, xor(y, d), z, core)) for d in (1, 2, 3)]
        self.along_z = [(xor(z, d), device(x, y, xor(z, d), core)) for d in range(1, 8)]
        self.flight = {}

    def greet(self):
        self.peers = [self.partner] + [dev for _, dev in self.along_x + self.along_y + self.along_z]
        barrier = pltpu.get_barrier_semaphore()
        for peer in self.peers:
            pl.semaphore_signal(barrier, inc=1, device_id=peer, device_id_type=MESH)

    def greeted(self):
        pl.semaphore_wait(pltpu.get_barrier_semaphore(), len(self.peers))

    def start(self, key, src, dst, dev):
        n = self.used
        self.used += 1
        c = pltpu.make_async_remote_copy(
            src_ref=src, dst_ref=dst, send_sem=self.send.at[n], recv_sem=self.recv.at[n],
            device_id=dev, device_id_type=MESH,
        )
        c.start()
        self.flight.setdefault(key, []).append(c)

    def finish(self, key):
        for c in self.flight.pop(key):
            c.wait()

    def put(self, c, lo, value):
        lanes = slice(lo, lo + value.shape[1])
        for strip in range(16):
            y1, x, z2 = strip // 8, (strip // 2) % 4, strip % 2
            for core in range(2):
                for y0 in range(2):
                    r = strip * 32 + core * 16 + y0 * 8
                    self.g[c, core, z2, y1 * 2 + y0, x, :, lanes] = value[r : r + 8]

    def cores(self, c):
        self.start(("p0", c), self.g.at[c, 1 - self.core], self.s1.at[c], self.partner)

    def first(self, c):
        self.finish(("p0", c))
        for half in range(2):
            self.s1[c, half] = self.s1[c, half] + self.g[c, self.core, half]
        for n, (to, dev) in enumerate(self.along_x):
            self.start(("p1", c), self.s1.at[c, 0, :, to], self.ra.at[c, n], dev)
        for n, (to, dev) in enumerate(self.along_y):
            self.start(("p1", c), self.s1.at[c, 1, to], self.rb.at[c, n], dev)

    def second(self, lo, hi):
        for c in range(lo, hi):
            self.finish(("p1", c))
            self.a2[c] = self.s1[c, 0, :, self.x] + self.ra[c, 0] + self.ra[c, 1] + self.ra[c, 2]
            self.b2[c] = self.s1[c, 1, self.y] + self.rb[c, 0] + self.rb[c, 1] + self.rb[c, 2]
        span = pl.ds(lo, hi - lo)
        for n, (to, dev) in enumerate(self.along_y):
            self.start(("p2", lo), self.a2.at[span, to], self.ra2.at[n, span], dev)
        for n, (to, dev) in enumerate(self.along_x):
            self.start(("p2", lo), self.b2.at[span, to], self.rb2.at[n, span], dev)

    def third(self, lo, hi):
        self.finish(("p2", lo))
        for c in range(lo, hi):
            a = self.a2[c, self.y] + self.ra2[0, c] + self.ra2[1, c] + self.ra2[2, c]
            b = self.b2[c, self.x] + self.rb2[0, c] + self.rb2[1, c] + self.rb2[2, c]
            for k in range(4):
                self.zs[c, k] = a[2 * k : 2 * k + 2]
                self.zs[c, 4 + k] = b[2 * k : 2 * k + 2]
        span = pl.ds(lo, hi - lo)
        for n, (to, dev) in enumerate(self.along_z):
            self.start(("p3", lo), self.zs.at[span, to], self.rz.at[n, span], dev)

    def last(self, lo, hi):
        self.finish(("p3", lo))
        out = []
        for c in range(lo, hi):
            mine = self.zs[c, self.z]
            for n in range(7):
                mine = mine + self.rz[n, c]
            out.append(mine)
        return out

    def table_cores(self, value):
        self.tt[0] = jnp.zeros_like(self.tt[0])
        self.tt[0, 0, :, 0:ENTRIES] = value[0:8]
        self.tt[0, 1, :, 0:ENTRIES] = value[8:16]
        self.start("t0", self.tt.at[0, 1 - self.core], self.tr.at[0], self.partner)

    def table_axis(self, key, stage, first, count, own, peers):
        total = own
        if key is not None:
            self.finish(key)
            for n in range(count):
                total = total + self.tr[first + n]
        self.tt[stage, 0] = total
        for n, (_, dev) in enumerate(peers):
            self.start("t%d" % stage, self.tt.at[stage, 0], self.tr.at[first + count + n], dev)


def kernel(*refs):
    refs = list(refs)

    def take(n):
        out = refs[:n]
        del refs[:n]
        return out

    tok_hbm, cot_hbm, reg_hbm, rel_hbm, wqkv_hbm, wproj_hbm, tab_hbm = take(7)
    out_qkv, out_proj, out_tab = take(3)
    rel, reg, tab_t, tok, cot, wqkv, wproj, fetched = take(8)
    xp, cp, qkv, kvt, da, xpt = take(6)
    bias, mask, keep, dk, dv, dqt, at, gb, pad, tabp, relt, wide, grads = take(13)
    ex = Exchange(*refs)

    fetches = []
    moves = (
        (rel_hbm, rel), (reg_hbm, reg), (tab_hbm, tab_t),
        (tok_hbm, tok), (cot_hbm, cot), (wqkv_hbm, wqkv), (wproj_hbm, wproj),
    )
    for n, (src, dst) in enumerate(moves):
        fetch = pltpu.make_async_copy(src, dst, fetched.at[n])
        fetch.start()
        fetches.append(fetch)
    ex.greet()
    for fetch in fetches[:3]:
        fetch.wait()
    small_tables(reg, rel, tab_t, bias, mask, pad, tabp, relt)
    gb[...] = jnp.zeros_like(gb)
    fetches[3].wait()
    gather_windows(tok, xp)
    fetches[4].wait()
    gather_windows(cot, cp)
    fetches[5].wait()
    fetches[6].wait()
    project(wqkv, wproj, xp, cp, qkv, kvt, da, xpt)

    att = Attention(qkv, kvt, da, bias, mask, keep, dk, dv, dqt, at, gb, wide, grads)
    forward = (att.forward12, att.forward3), 4
    backward = (att.backward12,), 8
    to_keys = (att.backward_k,), 8
    to_queries = (att.backward_q,), 8

    def v_chunk(c):
        ex.put(c, 0, nn(xpt[...], dv[:, c * 256 : (c + 1) * 256]))
        ex.cores(c)

    def proj_chunk(c):
        y = cp[:, :, c * 256 : (c + 1) * 256].reshape(WIN * SEG, 256)
        ex.put(2 + c, 0, nn(at[...], y))
        ex.cores(2 + c)

    def k_chunk(c):
        ex.put(4 + 2 * c, 0, nn(xpt[...], dk[:, c * 256 : (c + 1) * 256]))
        ex.cores(4 + 2 * c)

    def q_chunk(c):
        ex.put(5 + 2 * c, 0, nt(xpt[...], dqt[c * 256 : (c + 1) * 256, :]))
        ex.cores(5 + 2 * c)

    half = 2 * GROUP
    def finish(lo, hi):
        for c, mine in zip(range(lo, hi), ex.last(lo, hi)):
            for r in range(2):
                for part in range(2):
                    value = mine[r : r + 1, part * 128 : (part + 1) * 128]
                    if 2 <= c < 4:
                        k = r * 4 + (c - 2) * 2 + part
                        out_proj[k : k + 1, :] = value
                    else:
                        col = (8, 10, 0, 0, 4, 0, 6, 2)[c] + part
                        k = r * 12 + col
                        out_qkv[k : k + 1, :] = value

    quarter = GROUP
    att.run(*forward, 0, half)
    ex.greeted()
    v_chunk(0)
    att.run(*forward, half, ALL)
    ex.first(0)
    v_chunk(1)
    proj_chunk(0)
    proj_chunk(1)
    att.run(*backward, 0, quarter)
    ex.first(1)
    ex.first(2)
    att.run(*backward, quarter, half)
    ex.first(3)
    att.run(*to_keys, 0, half)
    k_chunk(0)
    att.run(*to_queries, 0, half)
    q_chunk(0)
    att.run(*backward, half, half + quarter)
    ex.first(4)
    att.run(*backward, half + quarter, ALL)
    ex.first(5)
    ex.table_cores(table_gradient(gb, relt))
    ex.second(0, 3)
    att.run(*to_keys, half, ALL)
    own = ex.tt[0, ex.core]
    ex.finish("t0")
    ex.table_axis(None, 1, 0, 1, own + ex.tr[0], ex.along_x)
    k_chunk(1)
    att.run(*to_queries, half, half + quarter)
    ex.first(6)
    att.run(*to_queries, half + quarter, ALL)
    ex.table_axis("t1", 2, 1, 3, ex.tt[1, 0], ex.along_y)
    ex.third(0, 3)
    q_chunk(1)
    ex.second(3, 6)
    ex.first(7)
    ex.table_axis("t2", 3, 4, 3, ex.tt[2, 0], ex.along_z)
    ex.third(3, 6)
    finish(0, 3)
    ex.second(6, 8)
    ex.third(6, 8)
    finish(3, 6)
    ex.finish("t3")
    table = ex.tt[3, 0]
    for n in range(7):
        table = table + ex.tr[7 + n]
    ex.tt[4, 0] = table
    ex.start("t4", ex.tt.at[4, 0], ex.tr.at[14], ex.partner)
    ex.finish("t4")
    finish(6, 8)
    core = ex.core.astype(F32)
    other = ex.tr[14]
    even = table * (1.0 - core) + other * core
    odd = table * core + other * (1.0 - core)
    for k in range(8):
        out_tab[2 * k : 2 * k + 1, :] = even[k : k + 1, 0:169]
        out_tab[2 * k + 1 : 2 * k + 2, :] = odd[k : k + 1, 0:169]


def apply_kernel(scale, *refs):
    for total, momentum, out in zip(refs[0:3], refs[3:6], refs[6:9]):
        out[...] = 0.9 * momentum[...] + total[...] * scale


SCRATCH = [
    pltpu.VMEM((TOK, TOK), jnp.int32),
    pltpu.VMEM((WIN, TOK), jnp.int32),
    pltpu.VMEM((16, 169), F32),
    pltpu.VMEM((784, D), BF),
    pltpu.VMEM((784, D), BF),
    pltpu.VMEM((D, 3 * D), BF),
    pltpu.VMEM((D, D), BF),
    pltpu.SemaphoreType.DMA((7,)),
    pltpu.VMEM((WIN, SEG, D), BF),
    pltpu.VMEM((WIN, SEG, D), BF),
    pltpu.VMEM((1024, 3 * D), BF),
    pltpu.VMEM((1024, 1024), BF),
    pltpu.VMEM((1024, D), BF),
    pltpu.VMEM((D, 1024), BF),
    pltpu.VMEM((4, TP, 256), F32),
    pltpu.VMEM((WIN, TP, 128), F32),
    pltpu.VMEM((4 * WIN, TP, 256), F32),
    pltpu.VMEM((1024, D), BF),
    pltpu.VMEM((1024, D), BF),
    pltpu.VMEM((D, 1024), BF),
    pltpu.VMEM((D, 1024), BF),
    pltpu.VMEM((8 * TP, 128), F32),
    pltpu.VMEM((128, 128), F32),
    pltpu.VMEM((16, 256), F32),
    pltpu.VMEM((TP, 128), F32),
    pltpu.VMEM((UNITS, 128, 256), BF),
    pltpu.VMEM((2 * WIN, 128, 256), BF),
    pltpu.VMEM((CHUNKS, 2, 2, 4, 4, 8, CH), F32),
    pltpu.VMEM((CHUNKS, 2, 4, 4, 8, CH), F32),
    pltpu.VMEM((CHUNKS, 3, 4, 8, CH), F32),
    pltpu.VMEM((CHUNKS, 3, 4, 8, CH), F32),
    pltpu.VMEM((CHUNKS, 4, 8, CH), F32),
    pltpu.VMEM((CHUNKS, 4, 8, CH), F32),
    pltpu.VMEM((3, CHUNKS, 8, CH), F32),
    pltpu.VMEM((3, CHUNKS, 8, CH), F32),
    pltpu.VMEM((CHUNKS, 8, 2, CH), F32),
    pltpu.VMEM((7, CHUNKS, 2, CH), F32),
    pltpu.VMEM((5, 2, 8, CH), F32),
    pltpu.VMEM((15, 8, CH), F32),
    pltpu.SemaphoreType.DMA((120,)),
    pltpu.SemaphoreType.DMA((120,)),
]


OUT = (
    jax.ShapeDtypeStruct((24, 128), F32),
    jax.ShapeDtypeStruct((8, 128), F32),
    jax.ShapeDtypeStruct((16, 169), F32),
)


def step(*operands):
    vm = pl.BlockSpec(memory_space=pltpu.VMEM)
    hbm = pl.BlockSpec(memory_space=pl.ANY)
    return pl.pallas_call(
        kernel,
        name="step",
        out_shape=tuple(pltpu.VMEM(o.shape, o.dtype) for o in OUT),
        in_specs=[hbm] * 7,
        out_specs=(vm, vm, vm),
        scratch_shapes=SCRATCH,
        compiler_params=pltpu.CompilerParams(
            collective_id=0, has_side_effects=True, vmem_limit_bytes=60 * 2**20
        ),
    )(*operands)


def apply(scale, *operands):
    vm = pl.BlockSpec(memory_space=pltpu.VMEM)
    return pl.pallas_call(
        functools.partial(apply_kernel, scale),
        name="apply",
        out_shape=OUT,
        in_specs=[vm] * 6,
        out_specs=(vm, vm, vm),
        compiler_params=pltpu.CompilerParams(vmem_limit_bytes=2 * 2**20),
    )(*operands)


def body(tokens, cotangent, regions, rel_index, w_qkv, w_proj, bias_table, mom_qkv, mom_proj, mom_table):
    win, count, dim = tokens.shape
    devices = lax.axis_size(("gx", "gy", "gz"))
    tok = jnp.transpose(tokens, (1, 0, 2)).reshape(count * win, dim)
    cot = jnp.transpose(cotangent, (1, 0, 2)).reshape(count * win, dim)
    sums = step(tok, cot, regions, rel_index, w_qkv, w_proj, bias_table.T)
    out_qkv, out_proj, out_tab = apply(
        1.0 / (win * devices), *sums, mom_qkv.reshape(24, 128), mom_proj.reshape(8, 128), mom_table.T
    )
    return out_qkv.reshape(-1), out_proj.reshape(-1), out_tab.T


def solution(mesh):
    rows = P(("gx", "gy", "gz"))
    wide = P(("gx", "gy", "gz"), None, None)
    return jax.shard_map(
        body,
        mesh=mesh,
        in_specs=(wide, wide, P(("gx", "gy", "gz"), None), P(), P(), P(), P(), rows, rows, P()),
        out_specs=(rows, rows, P()),
        check_vma=False,
    )
```

```python
import functools

import jax
import jax.numpy as jnp
from jax import lax
from jax.experimental import pallas as pl
from jax.experimental.pallas import tpu as pltpu
from jax.sharding import PartitionSpec as P

MESH = pl.DeviceIdType.MESH
BF = jnp.bfloat16
F32 = jnp.float32
WIN = 16
TOK = 49
SEG = 64
TP = 56
D = 512
HEAD_DIM = 32
SCALE = HEAD_DIM ** -0.5
UNITS = 8
ALL = 4 * WIN // 2
GROUP = ALL // 4
ENTRIES = 176
CH = 256
CHUNKS = 8


def nt(a, b):
    return lax.dot_general(a, b, (((1,), (1,)), ((), ())), preferred_element_type=F32)


def nn(a, b):
    return jnp.dot(a, b, preferred_element_type=F32)


def iota(shape, dim):
    return lax.broadcasted_iota(jnp.int32, shape, dim)


def onehot(condition):
    return condition.astype(F32).astype(BF)


def aligned(start, size, to=128):
    return pl.ds(pl.multiple_of(start, to), size)


def small_tables(reg, rel, tab_t, bias, mask, pad, tabp, relt):
    low = iota((TP, 128), 1) < SEG
    pad[...] = jnp.zeros_like(pad)
    pad[0:TOK, 0:TOK] = rel[...].astype(F32)
    flipped = pad[...].T
    both = flipped[0:TP] + pltpu.roll(flipped, SEG, 1)[0:TP]
    index = both.astype(jnp.int32)
    relt[...] = both
    pad[...] = jnp.zeros_like(pad)
    pad[0:WIN, 0:TOK] = reg[...].astype(F32)
    regions = pad[0:WIN, :]
    regions = regions + pltpu.roll(regions, SEG, 1)
    columns = pad[...].T[0:TP]
    for w in range(WIN):
        key = jnp.broadcast_to(columns[:, w : w + 1], (TP, 128))
        mask[w] = jnp.where(key == regions[w : w + 1], 0.0, -100.0).astype(F32)
    tabp[...] = jnp.zeros_like(tabp)
    tabp[:, 0:169] = tab_t[...]
    first = jnp.bitwise_and(index, 127)
    beyond = index >= 128
    real = iota((TP, 128), 0) < TOK

    def looked(h):
        lo = jnp.broadcast_to(tabp[h : h + 1, 0:128], (TP, 128))
        hi = jnp.broadcast_to(tabp[h : h + 1, 128:256], (TP, 128))
        lo = jnp.take_along_axis(lo, first, axis=1, mode="promise_in_bounds")
        hi = jnp.take_along_axis(hi, first, axis=1, mode="promise_in_bounds")
        return jnp.where(beyond, hi, lo)

    for k in range(8):
        value = jnp.where(low, looked(2 * k), looked(2 * k + 1))
        bias[k // 2, :, (k % 2) * 128 : (k % 2 + 1) * 128] = jnp.where(real, value, -1e30)


def gather_windows(src, dst):
    row, col = iota((256, 256), 0), iota((256, 256), 1)
    pick = onehot((row % 16) * 16 + row // 16 == col)
    for part in range(3):
        out = nn(pick, src[part * 256 : (part + 1) * 256, :]).astype(BF)
        dst[:, part * 16 : (part + 1) * 16, :] = out.reshape(WIN, 16, D)
    out = nn(pick[:, 0:16], src[768:784, :]).astype(BF)
    dst[:, 48:64, :] = out.reshape(WIN, 16, D)


def project(wqkv, wproj, xp, cp, qkv, kvt, da, xpt):
    eye = onehot(iota((128, 128), 0) == iota((128, 128), 1))
    s = iota((128, 128), 0)
    wanted = (
        (s // 32) * 32
        + ((s // 4) % 2) * 16
        + ((s // 2) % 2) * 8
        + ((s // 8) % 2) * 4
        + ((s // 16) % 2) * 2
        + s % 2
    )
    strips = onehot(wanted == iota((128, 128), 1))

    def four_windows(c, carry):
        rows = aligned(c * 256, 256, 256)
        x = xp[pl.ds(c * 4, 4)].reshape(256, D)
        y = cp[pl.ds(c * 4, 4)].reshape(256, D)
        values = nn(x, wqkv[...]).astype(BF)
        qkv[rows, :] = values
        da[rows, :] = nt(y, wproj[...]).astype(BF)
        for b in range(4):
            xpt[b * 128 : (b + 1) * 128, rows] = nt(strips, x[:, b * 128 : (b + 1) * 128]).astype(BF)
            k = values[:, 512 + b * 128 : 512 + (b + 1) * 128]
            kvt[b * 128 : (b + 1) * 128, rows] = nt(eye, k).astype(BF)
            v = values[:, 1024 + b * 128 : 1024 + (b + 1) * 128]
            kvt[512 + b * 128 : 512 + (b + 1) * 128, rows] = nt(strips, v).astype(BF)
        return carry

    lax.fori_loop(0, 4, four_windows, 0)


class Attention:
    def __init__(self, qkv, kvt, da, bias, mask, keep, dk, dv, dqt, at, gb, wide, grads):
        self.qkv, self.kvt, self.da, self.bias, self.mask = qkv, kvt, da, bias, mask
        self.keep, self.dk, self.dv, self.dqt, self.at = keep, dk, dv, dqt, at
        self.gb, self.wide, self.grads = gb, wide, grads
        lane = iota((SEG, 256), 1) % 128
        self.heads = [onehot(lane // HEAD_DIM == h) for h in range(4)]
        self.zero = jnp.zeros((SEG, 128), BF)
        self.tail = jnp.zeros((SEG - TP, 256), F32)
        half = iota((128, 128), 1)
        self.left = onehot(half < SEG)
        self.right = onehot(half >= SEG)
        self.low = iota((32, 128), 1) < SEG

    def spread(self, a):
        a = jnp.concatenate([a[0:SEG], a[SEG:]], axis=1)
        return jnp.concatenate([a * head for head in self.heads], axis=0)

    def diagonal(self, a):
        upper = jnp.concatenate([a[0:SEG], self.zero], axis=1)
        lower = jnp.concatenate([self.zero, a[SEG:]], axis=1)
        return jnp.concatenate([upper, lower], axis=0)

    def stack(self, a, b):
        return jnp.concatenate([a, self.tail, b, self.tail], axis=0).astype(BF)

    def own(self, dst, pair, g, value):
        dst[aligned(pair * 128, SEG), aligned(g * 128, 128)] = value[0:SEG, 0:128].astype(BF)
        dst[aligned(pair * 128 + SEG, SEG, SEG), aligned(g * 128, 128)] = value[SEG:, 128:256].astype(BF)

    def across(self, dst, pair, g, turned, wide):
        lhs = jnp.concatenate([turned * self.left, turned * self.right], axis=0)
        full = nn(lhs, wide)
        for h in range(4):
            lanes = slice((h // 2) * 128, (h // 2 + 1) * 128)
            one = full[32 * h : 32 * h + 32, lanes]
            two = full[128 + 32 * h : 128 + 32 * h + 32, lanes]
            if h % 2:
                one = pltpu.roll(one, SEG, 1)
            else:
                two = pltpu.roll(two, SEG, 1)
            value = jnp.where(self.low, one, two).astype(BF)
            dst[aligned(g * 128 + 32 * h, 32, 32), aligned(pair * 128, 128)] = value

    def place(self, unit):
        return unit // (WIN // 2), unit % (WIN // 2)

    def forward12(self, u, unit):
        g, pair = self.place(unit)
        rows = aligned(pair * 128, 128)
        q_wide = self.spread(self.qkv[rows, aligned(g * 128, 128)])
        raw = nt(self.diagonal(self.qkv[rows, aligned(512 + g * 128, 128)]), q_wide)
        probs = []
        for i in range(2):
            scores = raw[i * SEG : i * SEG + TP] * SCALE + self.bias[g]
            scores = scores + jnp.concatenate([self.mask[2 * pair + i]] * 2, axis=1)
            e = jnp.exp(scores - jnp.max(scores, axis=0, keepdims=True))
            p = e * (1.0 / jnp.sum(e, axis=0, keepdims=True))
            self.keep[2 * unit + i] = p
            probs.append(p)
        self.wide[u] = self.stack(*probs)

    def forward3(self, u, unit):
        g, pair = self.place(unit)
        rows = aligned(pair * 128, 128)
        probs = self.wide[u]
        da_wide = self.spread(self.da[rows, aligned(g * 128, 128)])
        self.own(self.dv, pair, g, nn(probs, da_wide))
        self.across(self.at, pair, g, self.kvt[aligned(512 + g * 128, 128), rows], probs)

    def backward12(self, u, unit):
        g, pair = self.place(unit)
        rows = aligned(pair * 128, 128)
        da_wide = self.spread(self.da[rows, aligned(g * 128, 128)])
        raw = nt(self.diagonal(self.qkv[rows, aligned(1024 + g * 128, 128)]), da_wide)
        parts = []
        for i in range(2):
            p = self.keep[2 * unit + i]
            dp = raw[i * SEG : i * SEG + TP]
            parts.append(p * (dp - jnp.sum(p * dp, axis=0, keepdims=True)))
        total = parts[0] + parts[1]
        for k in range(2):
            block = aligned((2 * g + k) * TP, TP, 8)
            self.gb[block, :] = self.gb[block, :] + total[:, k * 128 : (k + 1) * 128]
        self.grads[unit] = self.stack(parts[0] * SCALE, parts[1] * SCALE)

    def backward_k(self, u, unit):
        g, pair = self.place(unit)
        rows = aligned(pair * 128, 128)
        q_wide = self.spread(self.qkv[rows, aligned(g * 128, 128)])
        self.own(self.dk, pair, g, nn(self.grads[unit], q_wide))

    def backward_q(self, u, unit):
        g, pair = self.place(unit)
        rows = aligned(pair * 128, 128)
        self.across(self.dqt, pair, g, self.kvt[aligned(g * 128, 128), rows], self.grads[unit])

    def stages(self, stages, units, t, which):
        for n in reversed(which):
            for u in range(units):
                stages[n](u, (t - n) * units + u)

    def run(self, stages, units, lo, hi):
        ahead = len(stages) - 1
        whole = tuple(range(len(stages)))
        lo, hi, steps = lo // units, hi // units, ALL // units
        if lo == 0:
            for t in range(ahead):
                self.stages(stages, units, t, whole[: t + 1])
        end = steps if hi == steps else hi + ahead

        def one(t, carry):
            self.stages(stages, units, t, whole)
            return carry

        if end - lo - ahead == 1:
            one(lo + ahead, 0)
        else:
            lax.fori_loop(lo + ahead, end, one, 0)
        if hi == steps:
            for t in range(ahead):
                self.stages(stages, units, steps + t, whole[t + 1 :])


def table_gradient(gb, relt):
    low = iota((8, 128), 1) < SEG
    entry = iota((ENTRIES, 128), 0).astype(F32)
    total = jnp.zeros((32, ENTRIES), F32)

    def line(j):
        if j >= TOK:
            return jnp.zeros((32, 128), BF), jnp.zeros((ENTRIES, 128), BF)
        hot = onehot(entry == jnp.broadcast_to(relt[j : j + 1, :], (ENTRIES, 128)))
        pairs = gb[pl.ds(j, 8, stride=TP), :]
        split = jnp.concatenate([jnp.where(low, pairs, 0.0), jnp.where(low, 0.0, pairs)], axis=0)
        upper = split.astype(BF)
        lower = (split - upper.astype(F32)).astype(BF)
        return jnp.concatenate([upper, lower], axis=0), hot

    for j in range(0, TOK, 2):
        a, b = line(j), line(j + 1)
        total = total + nt(
            jnp.concatenate([a[0], b[0]], axis=1), jnp.concatenate([a[1], b[1]], axis=1)
        )
    return total[0:16] + total[16:32]


class Exchange:
    def __init__(self, g, s1, ra, rb, a2, b2, ra2, rb2, zs, rz, tt, tr, send, recv):
        self.g, self.s1, self.ra, self.rb, self.a2, self.b2 = g, s1, ra, rb, a2, b2
        self.ra2, self.rb2, self.zs, self.rz, self.tt, self.tr = ra2, rb2, zs, rz, tt, tr
        self.send, self.recv, self.used = send, recv, 0
        gx, gy, gz = lax.axis_index("gx"), lax.axis_index("gy"), lax.axis_index("gz")
        x, z, core = lax.rem(gx, 4), gy, lax.rem(gz, 2)
        y = (gx // 4) * 2 + gz // 2

        def device(x, y, z, core):
            return ((y // 2) * 4 + x, z, lax.rem(y, 2) * 2 + core)

        def xor(a, b):
            out = 0
            for bit in (1, 2, 4):
                have = lax.rem(a // bit, 2)
                out = out + bit * ((1 - have) if b & bit else have)
            return out

        self.x, self.y, self.z, self.core = x, y, z, core
        self.partner = device(x, y, z, 1 - core)
        self.along_x = [(xor(x, d), device(xor(x, d), y, z, core)) for d in (1, 2, 3)]
        self.along_y = [(xor(y, d), device(x, xor(y, d), z, core)) for d in (1, 2, 3)]
        self.along_z = [(xor(z, d), device(x, y, xor(z, d), core)) for d in range(1, 8)]
        self.flight = {}

    def greet(self):
        self.peers = [self.partner] + [dev for _, dev in self.along_x + self.along_y + self.along_z]
        barrier = pltpu.get_barrier_semaphore()
        for peer in self.peers:
            pl.semaphore_signal(barrier, inc=1, device_id=peer, device_id_type=MESH)

    def greeted(self):
        pl.semaphore_wait(pltpu.get_barrier_semaphore(), len(self.peers))

    def start(self, key, src, dst, dev):
        n = self.used
        self.used += 1
        c = pltpu.make_async_remote_copy(
            src_ref=src, dst_ref=dst, send_sem=self.send.at[n], recv_sem=self.recv.at[n],
            device_id=dev, device_id_type=MESH,
        )
        c.start()
        self.flight.setdefault(key, []).append(c)

    def finish(self, key):
        for c in self.flight.pop(key):
            c.wait()

    def put(self, c, lo, value):
        lanes = slice(lo, lo + value.shape[1])
        for strip in range(16):
            y1, x, z2 = strip // 8, (strip // 2) % 4, strip % 2
            for core in range(2):
                for y0 in range(2):
                    r = strip * 32 + core * 16 + y0 * 8
                    self.g[c, core, z2, y1 * 2 + y0, x, :, lanes] = value[r : r + 8]

    def cores(self, c):
        self.start(("p0", c), self.g.at[c, 1 - self.core], self.s1.at[c], self.partner)

    def first(self, c):
        self.finish(("p0", c))
        for half in range(2):
            self.s1[c, half] = self.s1[c, half] + self.g[c, self.core, half]
        for n, (to, dev) in enumerate(self.along_x):
            self.start(("p1", c), self.s1.at[c, 0, :, to], self.ra.at[c, n], dev)
        for n, (to, dev) in enumerate(self.along_y):
            self.start(("p1", c), self.s1.at[c, 1, to], self.rb.at[c, n], dev)

    def second(self, lo, hi):
        for c in range(lo, hi):
            self.finish(("p1", c))
            self.a2[c] = self.s1[c, 0, :, self.x] + self.ra[c, 0] + self.ra[c, 1] + self.ra[c, 2]
            self.b2[c] = self.s1[c, 1, self.y] + self.rb[c, 0] + self.rb[c, 1] + self.rb[c, 2]
        span = pl.ds(lo, hi - lo)
        for n, (to, dev) in enumerate(self.along_y):
            self.start(("p2", lo), self.a2.at[span, to], self.ra2.at[n, span], dev)
        for n, (to, dev) in enumerate(self.along_x):
            self.start(("p2", lo), self.b2.at[span, to], self.rb2.at[n, span], dev)

    def third(self, lo, hi):
        self.finish(("p2", lo))
        for c in range(lo, hi):
            a = self.a2[c, self.y] + self.ra2[0, c] + self.ra2[1, c] + self.ra2[2, c]
            b = self.b2[c, self.x] + self.rb2[0, c] + self.rb2[1, c] + self.rb2[2, c]
            for k in range(4):
                self.zs[c, k] = a[2 * k : 2 * k + 2]
                self.zs[c, 4 + k] = b[2 * k : 2 * k + 2]
        span = pl.ds(lo, hi - lo)
        for n, (to, dev) in enumerate(self.along_z):
            self.start(("p3", lo), self.zs.at[span, to], self.rz.at[n, span], dev)

    def last(self, lo, hi):
        self.finish(("p3", lo))
        out = []
        for c in range(lo, hi):
            mine = self.zs[c, self.z]
            for n in range(7):
                mine = mine + self.rz[n, c]
            out.append(mine)
        return out

    def table_cores(self, value):
        self.tt[0] = jnp.zeros_like(self.tt[0])
        self.tt[0, 0, :, 0:ENTRIES] = value[0:8]
        self.tt[0, 1, :, 0:ENTRIES] = value[8:16]
        self.start("t0", self.tt.at[0, 1 - self.core], self.tr.at[0], self.partner)

    def table_axis(self, key, stage, first, count, own, peers):
        total = own
        if key is not None:
            self.finish(key)
            for n in range(count):
                total = total + self.tr[first + n]
        self.tt[stage, 0] = total
        for n, (_, dev) in enumerate(peers):
            self.start("t%d" % stage, self.tt.at[stage, 0], self.tr.at[first + count + n], dev)


def kernel(*refs):
    refs = list(refs)

    def take(n):
        out = refs[:n]
        del refs[:n]
        return out

    tok_hbm, cot_hbm, reg_hbm, rel_hbm, wqkv_hbm, wproj_hbm, tab_hbm = take(7)
    out_qkv, out_proj, out_tab = take(3)
    rel, reg, tab_t, tok, cot, wqkv, wproj, fetched = take(8)
    xp, cp, qkv, kvt, da, xpt = take(6)
    bias, mask, keep, dk, dv, dqt, at, gb, pad, tabp, relt, wide, grads = take(13)
    ex = Exchange(*refs)

    fetches = []
    moves = (
        (tok_hbm, tok), (rel_hbm, rel), (reg_hbm, reg), (tab_hbm, tab_t),
        (cot_hbm, cot), (wqkv_hbm, wqkv), (wproj_hbm, wproj),
    )
    for n, (src, dst) in enumerate(moves):
        fetch = pltpu.make_async_copy(src, dst, fetched.at[n])
        fetch.start()
        fetches.append(fetch)
    ex.greet()
    for fetch in fetches[:5]:
        fetch.wait()
    gather_windows(tok, xp)
    small_tables(reg, rel, tab_t, bias, mask, pad, tabp, relt)
    gb[...] = jnp.zeros_like(gb)
    gather_windows(cot, cp)
    fetches[5].wait()
    fetches[6].wait()
    project(wqkv, wproj, xp, cp, qkv, kvt, da, xpt)

    att = Attention(qkv, kvt, da, bias, mask, keep, dk, dv, dqt, at, gb, wide, grads)
    forward = (att.forward12, att.forward3), 4
    backward = (att.backward12,), 8
    to_keys = (att.backward_k,), 8
    to_queries = (att.backward_q,), 8

    def v_chunk(c):
        ex.put(c, 0, nn(xpt[...], dv[:, c * 256 : (c + 1) * 256]))
        ex.cores(c)

    def proj_chunk(c):
        y = cp[:, :, c * 256 : (c + 1) * 256].reshape(WIN * SEG, 256)
        ex.put(2 + c, 0, nn(at[...], y))
        ex.cores(2 + c)

    def k_chunk(c):
        ex.put(4 + 2 * c, 0, nn(xpt[...], dk[:, c * 256 : (c + 1) * 256]))
        ex.cores(4 + 2 * c)

    def q_chunk(c):
        ex.put(5 + 2 * c, 0, nt(xpt[...], dqt[c * 256 : (c + 1) * 256, :]))
        ex.cores(5 + 2 * c)

    half = 2 * GROUP
    def finish(lo, hi):
        for c, mine in zip(range(lo, hi), ex.last(lo, hi)):
            for r in range(2):
                for part in range(2):
                    value = mine[r : r + 1, part * 128 : (part + 1) * 128]
                    if 2 <= c < 4:
                        k = r * 4 + (c - 2) * 2 + part
                        out_proj[k : k + 1, :] = value
                    else:
                        col = (8, 10, 0, 0, 4, 0, 6, 2)[c] + part
                        k = r * 12 + col
                        out_qkv[k : k + 1, :] = value

    quarter = GROUP
    att.run(*forward, 0, half)
    ex.greeted()
    v_chunk(0)
    att.run(*forward, half, ALL)
    ex.first(0)
    v_chunk(1)
    proj_chunk(0)
    proj_chunk(1)
    att.run(*backward, 0, quarter)
    ex.first(1)
    att.run(*backward, quarter, half)
    ex.first(2)
    ex.first(3)
    att.run(*to_keys, 0, half)
    k_chunk(0)
    att.run(*to_queries, 0, half)
    q_chunk(0)
    att.run(*backward, half, half + quarter)
    ex.first(4)
    att.run(*backward, half + quarter, ALL)
    ex.table_cores(table_gradient(gb, relt))
    ex.first(5)
    ex.second(0, 3)
    att.run(*to_keys, half, ALL)
    own = ex.tt[0, ex.core]
    ex.finish("t0")
    ex.table_axis(None, 1, 0, 1, own + ex.tr[0], ex.along_x)
    k_chunk(1)
    att.run(*to_queries, half, ALL)
    q_chunk(1)
    ex.first(6)
    ex.first(7)
    ex.table_axis("t1", 2, 1, 3, ex.tt[1, 0], ex.along_y)
    ex.second(3, 6)
    ex.third(0, 3)
    ex.second(6, 7)
    ex.table_axis("t2", 3, 4, 3, ex.tt[2, 0], ex.along_z)
    ex.second(7, 8)
    ex.third(3, 6)
    ex.third(6, 7)
    ex.third(7, 8)
    finish(0, 3)
    ex.finish("t3")
    table = ex.tt[3, 0]
    for n in range(7):
        table = table + ex.tr[7 + n]
    ex.tt[4, 0] = table
    ex.start("t4", ex.tt.at[4, 0], ex.tr.at[14], ex.partner)
    finish(3, 6)
    finish(6, 7)
    ex.finish("t4")
    finish(7, 8)
    core = ex.core.astype(F32)
    other = ex.tr[14]
    even = table * (1.0 - core) + other * core
    odd = table * core + other * (1.0 - core)
    for k in range(8):
        out_tab[2 * k : 2 * k + 1, :] = even[k : k + 1, 0:169]
        out_tab[2 * k + 1 : 2 * k + 2, :] = odd[k : k + 1, 0:169]


def apply_kernel(scale, *refs):
    for total, momentum, out in zip(refs[0:3], refs[3:6], refs[6:9]):
        out[...] = 0.9 * momentum[...] + total[...] * scale


SCRATCH = [
    pltpu.VMEM((TOK, TOK), jnp.int32),
    pltpu.VMEM((WIN, TOK), jnp.int32),
    pltpu.VMEM((16, 169), F32),
    pltpu.VMEM((784, D), BF),
    pltpu.VMEM((784, D), BF),
    pltpu.VMEM((D, 3 * D), BF),
    pltpu.VMEM((D, D), BF),
    pltpu.SemaphoreType.DMA((7,)),
    pltpu.VMEM((WIN, SEG, D), BF),
    pltpu.VMEM((WIN, SEG, D), BF),
    pltpu.VMEM((1024, 3 * D), BF),
    pltpu.VMEM((1024, 1024), BF),
    pltpu.VMEM((1024, D), BF),
    pltpu.VMEM((D, 1024), BF),
    pltpu.VMEM((4, TP, 256), F32),
    pltpu.VMEM((WIN, TP, 128), F32),
    pltpu.VMEM((4 * WIN, TP, 256), F32),
    pltpu.VMEM((1024, D), BF),
    pltpu.VMEM((1024, D), BF),
    pltpu.VMEM((D, 1024), BF),
    pltpu.VMEM((D, 1024), BF),
    pltpu.VMEM((8 * TP, 128), F32),
    pltpu.VMEM((128, 128), F32),
    pltpu.VMEM((16, 256), F32),
    pltpu.VMEM((TP, 128), F32),
    pltpu.VMEM((UNITS, 128, 256), BF),
    pltpu.VMEM((2 * WIN, 128, 256), BF),
    pltpu.VMEM((CHUNKS, 2, 2, 4, 4, 8, CH), F32),
    pltpu.VMEM((CHUNKS, 2, 4, 4, 8, CH), F32),
    pltpu.VMEM((CHUNKS, 3, 4, 8, CH), F32),
    pltpu.VMEM((CHUNKS, 3, 4, 8, CH), F32),
    pltpu.VMEM((CHUNKS, 4, 8, CH), F32),
    pltpu.VMEM((CHUNKS, 4, 8, CH), F32),
    pltpu.VMEM((3, CHUNKS, 8, CH), F32),
    pltpu.VMEM((3, CHUNKS, 8, CH), F32),
    pltpu.VMEM((CHUNKS, 8, 2, CH), F32),
    pltpu.VMEM((7, CHUNKS, 2, CH), F32),
    pltpu.VMEM((5, 2, 8, CH), F32),
    pltpu.VMEM((15, 8, CH), F32),
    pltpu.SemaphoreType.DMA((128,)),
    pltpu.SemaphoreType.DMA((128,)),
]


OUT = (
    jax.ShapeDtypeStruct((24, 128), F32),
    jax.ShapeDtypeStruct((8, 128), F32),
    jax.ShapeDtypeStruct((16, 169), F32),
)


def step(*operands):
    vm = pl.BlockSpec(memory_space=pltpu.VMEM)
    hbm = pl.BlockSpec(memory_space=pl.ANY)
    return pl.pallas_call(
        kernel,
        name="step",
        out_shape=tuple(pltpu.VMEM(o.shape, o.dtype) for o in OUT),
        in_specs=[hbm] * 7,
        out_specs=(vm, vm, vm),
        scratch_shapes=SCRATCH,
        compiler_params=pltpu.CompilerParams(
            collective_id=0, has_side_effects=True, vmem_limit_bytes=60 * 2**20
        ),
    )(*operands)


def apply(scale, *operands):
    vm = pl.BlockSpec(memory_space=pltpu.VMEM)
    return pl.pallas_call(
        functools.partial(apply_kernel, scale),
        name="apply",
        out_shape=OUT,
        in_specs=[vm] * 6,
        out_specs=(vm, vm, vm),
        compiler_params=pltpu.CompilerParams(vmem_limit_bytes=2 * 2**20),
    )(*operands)


def body(tokens, cotangent, regions, rel_index, w_qkv, w_proj, bias_table, mom_qkv, mom_proj, mom_table):
    win, count, dim = tokens.shape
    devices = lax.axis_size(("gx", "gy", "gz"))
    tok = jnp.transpose(tokens, (1, 0, 2)).reshape(count * win, dim)
    cot = jnp.transpose(cotangent, (1, 0, 2)).reshape(count * win, dim)
    sums = step(tok, cot, regions, rel_index, w_qkv, w_proj, bias_table.T)
    out_qkv, out_proj, out_tab = apply(
        1.0 / (win * devices), *sums, mom_qkv.reshape(24, 128), mom_proj.reshape(8, 128), mom_table.T
    )
    return out_qkv.reshape(-1), out_proj.reshape(-1), out_tab.T


def solution(mesh):
    rows = P(("gx", "gy", "gz"))
    wide = P(("gx", "gy", "gz"), None, None)
    return jax.shard_map(
        body,
        mesh=mesh,
        in_specs=(wide, wide, P(("gx", "gy", "gz"), None), P(), P(), P(), P(), rows, rows, P()),
        out_specs=(rows, rows, P()),
        check_vma=False,
    )
```

```python
import functools

import jax
import jax.numpy as jnp
from jax import lax
from jax.experimental import pallas as pl
from jax.experimental.pallas import tpu as pltpu
from jax.sharding import PartitionSpec as P

MESH = pl.DeviceIdType.MESH
BF = jnp.bfloat16
F32 = jnp.float32
WIN = 16
TOK = 49
SEG = 64
TP = 56
D = 512
HEAD_DIM = 32
SCALE = HEAD_DIM ** -0.5
UNITS = 8
ALL = 4 * WIN // 2
GROUP = ALL // 4
ENTRIES = 176
CH = 256
CHUNKS = 8


def nt(a, b):
    return lax.dot_general(a, b, (((1,), (1,)), ((), ())), preferred_element_type=F32)


def nn(a, b):
    return jnp.dot(a, b, preferred_element_type=F32)


def iota(shape, dim):
    return lax.broadcasted_iota(jnp.int32, shape, dim)


def onehot(condition):
    return condition.astype(F32).astype(BF)


def aligned(start, size, to=128):
    return pl.ds(pl.multiple_of(start, to), size)


def small_tables(reg, rel, tab_t, bias, mask, pad, tabp, relt):
    low = iota((TP, 128), 1) < SEG
    pad[...] = jnp.zeros_like(pad)
    pad[0:TOK, 0:TOK] = rel[...].astype(F32)
    flipped = pad[...].T
    both = flipped[0:TP] + pltpu.roll(flipped, SEG, 1)[0:TP]
    index = both.astype(jnp.int32)
    relt[...] = both
    pad[...] = jnp.zeros_like(pad)
    pad[0:WIN, 0:TOK] = reg[...].astype(F32)
    regions = pad[0:WIN, :]
    regions = regions + pltpu.roll(regions, SEG, 1)
    columns = pad[...].T[0:TP]
    for w in range(WIN):
        key = jnp.broadcast_to(columns[:, w : w + 1], (TP, 128))
        mask[w] = jnp.where(key == regions[w : w + 1], 0.0, -100.0).astype(F32)
    tabp[...] = jnp.zeros_like(tabp)
    tabp[:, 0:169] = tab_t[...]
    first = jnp.bitwise_and(index, 127)
    beyond = index >= 128
    real = iota((TP, 128), 0) < TOK

    def looked(h):
        lo = jnp.broadcast_to(tabp[h : h + 1, 0:128], (TP, 128))
        hi = jnp.broadcast_to(tabp[h : h + 1, 128:256], (TP, 128))
        lo = jnp.take_along_axis(lo, first, axis=1, mode="promise_in_bounds")
        hi = jnp.take_along_axis(hi, first, axis=1, mode="promise_in_bounds")
        return jnp.where(beyond, hi, lo)

    for k in range(8):
        value = jnp.where(low, looked(2 * k), looked(2 * k + 1))
        bias[k // 2, :, (k % 2) * 128 : (k % 2 + 1) * 128] = jnp.where(real, value, -1e30)


def gather_windows(src, dst):
    row, col = iota((256, 256), 0), iota((256, 256), 1)
    pick = onehot((row % 16) * 16 + row // 16 == col)
    for part in range(3):
        out = nn(pick, src[part * 256 : (part + 1) * 256, :]).astype(BF)
        dst[:, part * 16 : (part + 1) * 16, :] = out.reshape(WIN, 16, D)
    out = nn(pick[:, 0:16], src[768:784, :]).astype(BF)
    dst[:, 48:64, :] = out.reshape(WIN, 16, D)


def project(wqkv, wproj, xp, cp, qkv, kvt, da, xpt):
    eye = onehot(iota((128, 128), 0) == iota((128, 128), 1))
    s = iota((128, 128), 0)
    wanted = (
        (s // 32) * 32
        + ((s // 4) % 2) * 16
        + ((s // 2) % 2) * 8
        + ((s // 8) % 2) * 4
        + ((s // 16) % 2) * 2
        + s % 2
    )
    strips = onehot(wanted == iota((128, 128), 1))

    def four_windows(c, carry):
        rows = aligned(c * 256, 256, 256)
        x = xp[pl.ds(c * 4, 4)].reshape(256, D)
        y = cp[pl.ds(c * 4, 4)].reshape(256, D)
        values = nn(x, wqkv[...]).astype(BF)
        qkv[rows, :] = values
        da[rows, :] = nt(y, wproj[...]).astype(BF)
        for b in range(4):
            xpt[b * 128 : (b + 1) * 128, rows] = nt(strips, x[:, b * 128 : (b + 1) * 128]).astype(BF)
            k = values[:, 512 + b * 128 : 512 + (b + 1) * 128]
            kvt[b * 128 : (b + 1) * 128, rows] = nt(eye, k).astype(BF)
            v = values[:, 1024 + b * 128 : 1024 + (b + 1) * 128]
            kvt[512 + b * 128 : 512 + (b + 1) * 128, rows] = nt(strips, v).astype(BF)
        return carry

    lax.fori_loop(0, 4, four_windows, 0)


class Attention:
    def __init__(self, qkv, kvt, da, bias, mask, keep, dk, dv, dqt, at, gb, wide, grads):
        self.qkv, self.kvt, self.da, self.bias, self.mask = qkv, kvt, da, bias, mask
        self.keep, self.dk, self.dv, self.dqt, self.at = keep, dk, dv, dqt, at
        self.gb, self.wide, self.grads = gb, wide, grads
        lane = iota((SEG, 256), 1) % 128
        self.heads = [onehot(lane // HEAD_DIM == h) for h in range(4)]
        self.zero = jnp.zeros((SEG, 128), BF)
        self.tail = jnp.zeros((SEG - TP, 256), F32)
        half = iota((128, 128), 1)
        self.left = onehot(half < SEG)
        self.right = onehot(half >= SEG)
        self.low = iota((32, 128), 1) < SEG

    def spread(self, a):
        a = jnp.concatenate([a[0:SEG], a[SEG:]], axis=1)
        return jnp.concatenate([a * head for head in self.heads], axis=0)

    def diagonal(self, a):
        upper = jnp.concatenate([a[0:SEG], self.zero], axis=1)
        lower = jnp.concatenate([self.zero, a[SEG:]], axis=1)
        return jnp.concatenate([upper, lower], axis=0)

    def stack(self, a, b):
        return jnp.concatenate([a, self.tail, b, self.tail], axis=0).astype(BF)

    def own(self, dst, pair, g, value):
        dst[aligned(pair * 128, SEG), aligned(g * 128, 128)] = value[0:SEG, 0:128].astype(BF)
        dst[aligned(pair * 128 + SEG, SEG, SEG), aligned(g * 128, 128)] = value[SEG:, 128:256].astype(BF)

    def across(self, dst, pair, g, turned, wide):
        lhs = jnp.concatenate([turned * self.left, turned * self.right], axis=0)
        full = nn(lhs, wide)
        for h in range(4):
            lanes = slice((h // 2) * 128, (h // 2 + 1) * 128)
            one = full[32 * h : 32 * h + 32, lanes]
            two = full[128 + 32 * h : 128 + 32 * h + 32, lanes]
            if h % 2:
                one = pltpu.roll(one, SEG, 1)
            else:
                two = pltpu.roll(two, SEG, 1)
            value = jnp.where(self.low, one, two).astype(BF)
            dst[aligned(g * 128 + 32 * h, 32, 32), aligned(pair * 128, 128)] = value

    def place(self, unit):
        return unit // (WIN // 2), unit % (WIN // 2)

    def forward12(self, u, unit):
        g, pair = self.place(unit)
        rows = aligned(pair * 128, 128)
        q_wide = self.spread(self.qkv[rows, aligned(g * 128, 128)])
        raw = nt(self.diagonal(self.qkv[rows, aligned(512 + g * 128, 128)]), q_wide)
        probs = []
        for i in range(2):
            scores = raw[i * SEG : i * SEG + TP] * SCALE + self.bias[g]
            scores = scores + jnp.concatenate([self.mask[2 * pair + i]] * 2, axis=1)
            e = jnp.exp(scores - jnp.max(scores, axis=0, keepdims=True))
            p = e * (1.0 / jnp.sum(e, axis=0, keepdims=True))
            self.keep[2 * unit + i] = p
            probs.append(p)
        self.wide[u] = self.stack(*probs)

    def forward3(self, u, unit):
        g, pair = self.place(unit)
        rows = aligned(pair * 128, 128)
        probs = self.wide[u]
        da_wide = self.spread(self.da[rows, aligned(g * 128, 128)])
        self.own(self.dv, pair, g, nn(probs, da_wide))
        self.across(self.at, pair, g, self.kvt[aligned(512 + g * 128, 128), rows], probs)

    def backward12(self, u, unit):
        g, pair = self.place(unit)
        rows = aligned(pair * 128, 128)
        da_wide = self.spread(self.da[rows, aligned(g * 128, 128)])
        raw = nt(self.diagonal(self.qkv[rows, aligned(1024 + g * 128, 128)]), da_wide)
        parts = []
        for i in range(2):
            p = self.keep[2 * unit + i]
            dp = raw[i * SEG : i * SEG + TP]
            parts.append(p * (dp - jnp.sum(p * dp, axis=0, keepdims=True)))
        total = parts[0] + parts[1]
        for k in range(2):
            block = aligned((2 * g + k) * TP, TP, 8)
            self.gb[block, :] = self.gb[block, :] + total[:, k * 128 : (k + 1) * 128]
        self.grads[unit] = self.stack(parts[0] * SCALE, parts[1] * SCALE)

    def backward_k(self, u, unit):
        g, pair = self.place(unit)
        rows = aligned(pair * 128, 128)
        q_wide = self.spread(self.qkv[rows, aligned(g * 128, 128)])
        self.own(self.dk, pair, g, nn(self.grads[unit], q_wide))

    def backward_q(self, u, unit):
        g, pair = self.place(unit)
        rows = aligned(pair * 128, 128)
        self.across(self.dqt, pair, g, self.kvt[aligned(g * 128, 128), rows], self.grads[unit])

    def stages(self, stages, units, t, which):
        for n in reversed(which):
            for u in range(units):
                stages[n](u, (t - n) * units + u)

    def run(self, stages, units, lo, hi):
        ahead = len(stages) - 1
        whole = tuple(range(len(stages)))
        lo, hi, steps = lo // units, hi // units, ALL // units
        if lo == 0:
            for t in range(ahead):
                self.stages(stages, units, t, whole[: t + 1])
        end = steps if hi == steps else hi + ahead

        def one(t, carry):
            self.stages(stages, units, t, whole)
            return carry

        if end - lo - ahead == 1:
            one(lo + ahead, 0)
        else:
            lax.fori_loop(lo + ahead, end, one, 0)
        if hi == steps:
            for t in range(ahead):
                self.stages(stages, units, steps + t, whole[t + 1 :])


def table_gradient(gb, relt):
    low = iota((8, 128), 1) < SEG
    entry = iota((ENTRIES, 128), 0).astype(F32)
    total = jnp.zeros((32, ENTRIES), F32)

    def line(j):
        if j >= TOK:
            return jnp.zeros((32, 128), BF), jnp.zeros((ENTRIES, 128), BF)
        hot = onehot(entry == jnp.broadcast_to(relt[j : j + 1, :], (ENTRIES, 128)))
        pairs = gb[pl.ds(j, 8, stride=TP), :]
        split = jnp.concatenate([jnp.where(low, pairs, 0.0), jnp.where(low, 0.0, pairs)], axis=0)
        upper = split.astype(BF)
        lower = (split - upper.astype(F32)).astype(BF)
        return jnp.concatenate([upper, lower], axis=0), hot

    for j in range(0, TOK, 2):
        a, b = line(j), line(j + 1)
        total = total + nt(
            jnp.concatenate([a[0], b[0]], axis=1), jnp.concatenate([a[1], b[1]], axis=1)
        )
    return total[0:16] + total[16:32]


class Exchange:
    def __init__(self, g, s1, ra, rb, a2, b2, ra2, rb2, zs, rz, tt, tr, send, recv):
        self.g, self.s1, self.ra, self.rb, self.a2, self.b2 = g, s1, ra, rb, a2, b2
        self.ra2, self.rb2, self.zs, self.rz, self.tt, self.tr = ra2, rb2, zs, rz, tt, tr
        self.send, self.recv, self.used = send, recv, 0
        gx, gy, gz = lax.axis_index("gx"), lax.axis_index("gy"), lax.axis_index("gz")
        x, z, core = lax.rem(gx, 4), gy, lax.rem(gz, 2)
        y = (gx // 4) * 2 + gz // 2

        def device(x, y, z, core):
            return ((y // 2) * 4 + x, z, lax.rem(y, 2) * 2 + core)

        def xor(a, b):
            out = 0
            for bit in (1, 2, 4):
                have = lax.rem(a // bit, 2)
                out = out + bit * ((1 - have) if b & bit else have)
            return out

        self.x, self.y, self.z, self.core = x, y, z, core
        self.partner = device(x, y, z, 1 - core)
        self.along_x = [(xor(x, d), device(xor(x, d), y, z, core)) for d in (1, 2, 3)]
        self.along_y = [(xor(y, d), device(x, xor(y, d), z, core)) for d in (1, 2, 3)]
        self.along_z = [(xor(z, d), device(x, y, xor(z, d), core)) for d in range(1, 8)]
        self.flight = {}

    def greet(self):
        self.peers = [self.partner] + [dev for _, dev in self.along_x + self.along_y + self.along_z]
        barrier = pltpu.get_barrier_semaphore()
        for peer in self.peers:
            pl.semaphore_signal(barrier, inc=1, device_id=peer, device_id_type=MESH)

    def greeted(self):
        pl.semaphore_wait(pltpu.get_barrier_semaphore(), len(self.peers))

    def start(self, key, src, dst, dev):
        n = self.used
        self.used += 1
        c = pltpu.make_async_remote_copy(
            src_ref=src, dst_ref=dst, send_sem=self.send.at[n], recv_sem=self.recv.at[n],
            device_id=dev, device_id_type=MESH,
        )
        c.start()
        self.flight.setdefault(key, []).append(c)

    def finish(self, key):
        for c in self.flight.pop(key):
            c.wait()

    def put(self, c, lo, value):
        lanes = slice(lo, lo + value.shape[1])
        for strip in range(16):
            y1, x, z2 = strip // 8, (strip // 2) % 4, strip % 2
            for core in range(2):
                for y0 in range(2):
                    r = strip * 32 + core * 16 + y0 * 8
                    self.g[c, core, z2, y1 * 2 + y0, x, :, lanes] = value[r : r + 8]

    def cores(self, c):
        self.start(("p0", c), self.g.at[c, 1 - self.core], self.s1.at[c], self.partner)

    def first(self, c):
        self.finish(("p0", c))
        for half in range(2):
            self.s1[c, half] = self.s1[c, half] + self.g[c, self.core, half]
        for n, (to, dev) in enumerate(self.along_x):
            self.start(("p1", c), self.s1.at[c, 0, :, to], self.ra.at[c, n], dev)
        for n, (to, dev) in enumerate(self.along_y):
            self.start(("p1", c), self.s1.at[c, 1, to], self.rb.at[c, n], dev)

    def second(self, lo, hi):
        for c in range(lo, hi):
            self.finish(("p1", c))
            self.a2[c] = self.s1[c, 0, :, self.x] + self.ra[c, 0] + self.ra[c, 1] + self.ra[c, 2]
            self.b2[c] = self.s1[c, 1, self.y] + self.rb[c, 0] + self.rb[c, 1] + self.rb[c, 2]
        span = pl.ds(lo, hi - lo)
        for n, (to, dev) in enumerate(self.along_y):
            self.start(("p2", lo), self.a2.at[span, to], self.ra2.at[n, span], dev)
        for n, (to, dev) in enumerate(self.along_x):
            self.start(("p2", lo), self.b2.at[span, to], self.rb2.at[n, span], dev)

    def third(self, lo, hi):
        self.finish(("p2", lo))
        for c in range(lo, hi):
            a = self.a2[c, self.y] + self.ra2[0, c] + self.ra2[1, c] + self.ra2[2, c]
            b = self.b2[c, self.x] + self.rb2[0, c] + self.rb2[1, c] + self.rb2[2, c]
            for k in range(4):
                self.zs[c, k] = a[2 * k : 2 * k + 2]
                self.zs[c, 4 + k] = b[2 * k : 2 * k + 2]
        span = pl.ds(lo, hi - lo)
        for n, (to, dev) in enumerate(self.along_z):
            self.start(("p3", lo), self.zs.at[span, to], self.rz.at[n, span], dev)

    def last(self, lo, hi):
        self.finish(("p3", lo))
        out = []
        for c in range(lo, hi):
            mine = self.zs[c, self.z]
            for n in range(7):
                mine = mine + self.rz[n, c]
            out.append(mine)
        return out

    def table_cores(self, value):
        self.tt[0] = jnp.zeros_like(self.tt[0])
        self.tt[0, 0, :, 0:ENTRIES] = value[0:8]
        self.tt[0, 1, :, 0:ENTRIES] = value[8:16]
        self.start("t0", self.tt.at[0, 1 - self.core], self.tr.at[0], self.partner)

    def table_axis(self, key, stage, first, count, own, peers):
        total = own
        if key is not None:
            self.finish(key)
            for n in range(count):
                total = total + self.tr[first + n]
        self.tt[stage, 0] = total
        for n, (_, dev) in enumerate(peers):
            self.start("t%d" % stage, self.tt.at[stage, 0], self.tr.at[first + count + n], dev)


def kernel(*refs):
    refs = list(refs)

    def take(n):
        out = refs[:n]
        del refs[:n]
        return out

    tok_hbm, cot_hbm, reg_hbm, rel_hbm, wqkv_hbm, wproj_hbm, tab_hbm = take(7)
    out_qkv, out_proj, out_tab = take(3)
    rel, reg, tab_t, tok, cot, wqkv, wproj, fetched = take(8)
    xp, cp, qkv, kvt, da, xpt = take(6)
    bias, mask, keep, dk, dv, dqt, at, gb, pad, tabp, relt, wide, grads = take(13)
    ex = Exchange(*refs)

    fetches = []
    moves = (
        (tok_hbm, tok), (rel_hbm, rel), (reg_hbm, reg), (tab_hbm, tab_t),
        (cot_hbm, cot), (wqkv_hbm, wqkv), (wproj_hbm, wproj),
    )
    for n, (src, dst) in enumerate(moves):
        fetch = pltpu.make_async_copy(src, dst, fetched.at[n])
        fetch.start()
        fetches.append(fetch)
    ex.greet()
    for fetch in fetches[:5]:
        fetch.wait()
    gather_windows(tok, xp)
    small_tables(reg, rel, tab_t, bias, mask, pad, tabp, relt)
    gb[...] = jnp.zeros_like(gb)
    gather_windows(cot, cp)
    fetches[5].wait()
    fetches[6].wait()
    project(wqkv, wproj, xp, cp, qkv, kvt, da, xpt)

    att = Attention(qkv, kvt, da, bias, mask, keep, dk, dv, dqt, at, gb, wide, grads)
    forward = (att.forward12, att.forward3), 4
    backward = (att.backward12,), 8
    to_keys = (att.backward_k,), 8
    to_queries = (att.backward_q,), 8

    def v_chunk(c):
        ex.put(c, 0, nn(xpt[...], dv[:, c * 256 : (c + 1) * 256]))
        ex.cores(c)

    def proj_chunk(c):
        y = cp[:, :, c * 256 : (c + 1) * 256].reshape(WIN * SEG, 256)
        ex.put(2 + c, 0, nn(at[...], y))
        ex.cores(2 + c)

    def k_chunk(c):
        ex.put(4 + 2 * c, 0, nn(xpt[...], dk[:, c * 256 : (c + 1) * 256]))
        ex.cores(4 + 2 * c)

    def q_chunk(c):
        ex.put(5 + 2 * c, 0, nt(xpt[...], dqt[c * 256 : (c + 1) * 256, :]))
        ex.cores(5 + 2 * c)

    half = 2 * GROUP
    def finish(lo, hi):
        for c, mine in zip(range(lo, hi), ex.last(lo, hi)):
            for r in range(2):
                for part in range(2):
                    value = mine[r : r + 1, part * 128 : (part + 1) * 128]
                    if 2 <= c < 4:
                        k = r * 4 + (c - 2) * 2 + part
                        out_proj[k : k + 1, :] = value
                    else:
                        col = (8, 10, 0, 0, 4, 0, 6, 2)[c] + part
                        k = r * 12 + col
                        out_qkv[k : k + 1, :] = value

    quarter = GROUP
    att.run(*forward, 0, half)
    ex.greeted()
    v_chunk(0)
    att.run(*backward, 0, quarter)
    att.run(*backward, quarter, half)
    ex.first(0)
    att.run(*to_keys, 0, half)
    k_chunk(0)
    att.run(*to_queries, 0, half)
    q_chunk(0)
    ex.first(4)
    att.run(*forward, half, ALL)
    ex.first(5)
    v_chunk(1)
    proj_chunk(0)
    proj_chunk(1)
    att.run(*backward, half, half + quarter)
    ex.first(1)
    ex.second(4, 6)
    att.run(*backward, half + quarter, ALL)
    ex.first(2)
    ex.first(3)
    ex.table_cores(table_gradient(gb, relt))
    ex.third(4, 6)
    att.run(*to_keys, half, ALL)
    own = ex.tt[0, ex.core]
    ex.finish("t0")
    ex.table_axis(None, 1, 0, 1, own + ex.tr[0], ex.along_x)
    k_chunk(1)
    att.run(*to_queries, half, ALL)
    q_chunk(1)
    ex.first(6)
    ex.first(7)
    ex.table_axis("t1", 2, 1, 3, ex.tt[1, 0], ex.along_y)
    ex.second(0, 4)
    ex.second(6, 7)
    ex.table_axis("t2", 3, 4, 3, ex.tt[2, 0], ex.along_z)
    ex.second(7, 8)
    ex.third(0, 4)
    ex.third(6, 7)
    ex.third(7, 8)
    finish(4, 6)
    ex.finish("t3")
    table = ex.tt[3, 0]
    for n in range(7):
        table = table + ex.tr[7 + n]
    ex.tt[4, 0] = table
    ex.start("t4", ex.tt.at[4, 0], ex.tr.at[14], ex.partner)
    finish(0, 4)
    finish(6, 7)
    ex.finish("t4")
    finish(7, 8)
    core = ex.core.astype(F32)
    other = ex.tr[14]
    even = table * (1.0 - core) + other * core
    odd = table * core + other * (1.0 - core)
    for k in range(8):
        out_tab[2 * k : 2 * k + 1, :] = even[k : k + 1, 0:169]
        out_tab[2 * k + 1 : 2 * k + 2, :] = odd[k : k + 1, 0:169]


def apply_kernel(scale, *refs):
    for total, momentum, out in zip(refs[0:3], refs[3:6], refs[6:9]):
        out[...] = 0.9 * momentum[...] + total[...] * scale


SCRATCH = [
    pltpu.VMEM((TOK, TOK), jnp.int32),
    pltpu.VMEM((WIN, TOK), jnp.int32),
    pltpu.VMEM((16, 169), F32),
    pltpu.VMEM((784, D), BF),
    pltpu.VMEM((784, D), BF),
    pltpu.VMEM((D, 3 * D), BF),
    pltpu.VMEM((D, D), BF),
    pltpu.SemaphoreType.DMA((7,)),
    pltpu.VMEM((WIN, SEG, D), BF),
    pltpu.VMEM((WIN, SEG, D), BF),
    pltpu.VMEM((1024, 3 * D), BF),
    pltpu.VMEM((1024, 1024), BF),
    pltpu.VMEM((1024, D), BF),
    pltpu.VMEM((D, 1024), BF),
    pltpu.VMEM((4, TP, 256), F32),
    pltpu.VMEM((WIN, TP, 128), F32),
    pltpu.VMEM((4 * WIN, TP, 256), F32),
    pltpu.VMEM((1024, D), BF),
    pltpu.VMEM((1024, D), BF),
    pltpu.VMEM((D, 1024), BF),
    pltpu.VMEM((D, 1024), BF),
    pltpu.VMEM((8 * TP, 128), F32),
    pltpu.VMEM((128, 128), F32),
    pltpu.VMEM((16, 256), F32),
    pltpu.VMEM((TP, 128), F32),
    pltpu.VMEM((UNITS, 128, 256), BF),
    pltpu.VMEM((2 * WIN, 128, 256), BF),
    pltpu.VMEM((CHUNKS, 2, 2, 4, 4, 8, CH), F32),
    pltpu.VMEM((CHUNKS, 2, 4, 4, 8, CH), F32),
    pltpu.VMEM((CHUNKS, 3, 4, 8, CH), F32),
    pltpu.VMEM((CHUNKS, 3, 4, 8, CH), F32),
    pltpu.VMEM((CHUNKS, 4, 8, CH), F32),
    pltpu.VMEM((CHUNKS, 4, 8, CH), F32),
    pltpu.VMEM((3, CHUNKS, 8, CH), F32),
    pltpu.VMEM((3, CHUNKS, 8, CH), F32),
    pltpu.VMEM((CHUNKS, 8, 2, CH), F32),
    pltpu.VMEM((7, CHUNKS, 2, CH), F32),
    pltpu.VMEM((5, 2, 8, CH), F32),
    pltpu.VMEM((15, 8, CH), F32),
    pltpu.SemaphoreType.DMA((128,)),
    pltpu.SemaphoreType.DMA((128,)),
]


OUT = (
    jax.ShapeDtypeStruct((24, 128), F32),
    jax.ShapeDtypeStruct((8, 128), F32),
    jax.ShapeDtypeStruct((16, 169), F32),
)


def step(*operands):
    vm = pl.BlockSpec(memory_space=pltpu.VMEM)
    hbm = pl.BlockSpec(memory_space=pl.ANY)
    return pl.pallas_call(
        kernel,
        name="step",
        out_shape=tuple(pltpu.VMEM(o.shape, o.dtype) for o in OUT),
        in_specs=[hbm] * 7,
        out_specs=(vm, vm, vm),
        scratch_shapes=SCRATCH,
        compiler_params=pltpu.CompilerParams(
            collective_id=0, has_side_effects=True, vmem_limit_bytes=60 * 2**20
        ),
    )(*operands)


def apply(scale, *operands):
    vm = pl.BlockSpec(memory_space=pltpu.VMEM)
    return pl.pallas_call(
        functools.partial(apply_kernel, scale),
        name="apply",
        out_shape=OUT,
        in_specs=[vm] * 6,
        out_specs=(vm, vm, vm),
        compiler_params=pltpu.CompilerParams(vmem_limit_bytes=2 * 2**20),
    )(*operands)


def body(tokens, cotangent, regions, rel_index, w_qkv, w_proj, bias_table, mom_qkv, mom_proj, mom_table):
    win, count, dim = tokens.shape
    devices = lax.axis_size(("gx", "gy", "gz"))
    tok = jnp.transpose(tokens, (1, 0, 2)).reshape(count * win, dim)
    cot = jnp.transpose(cotangent, (1, 0, 2)).reshape(count * win, dim)
    sums = step(tok, cot, regions, rel_index, w_qkv, w_proj, bias_table.T)
    out_qkv, out_proj, out_tab = apply(
        1.0 / (win * devices), *sums, mom_qkv.reshape(24, 128), mom_proj.reshape(8, 128), mom_table.T
    )
    return out_qkv.reshape(-1), out_proj.reshape(-1), out_tab.T


def solution(mesh):
    rows = P(("gx", "gy", "gz"))
    wide = P(("gx", "gy", "gz"), None, None)
    return jax.shard_map(
        body,
        mesh=mesh,
        in_specs=(wide, wide, P(("gx", "gy", "gz"), None), P(), P(), P(), P(), rows, rows, P()),
        out_specs=(rows, rows, P()),
        check_vma=False,
    )
```
